32 devices in a mesh: gx: 4 (over y, x), gy: 8 (over z, core).
Axes of the slice: x: 2, y: 2, z: 4, core: 2. Of those that a mesh axis runs over, the one named last changes fastest.
Arguments:
- velocity: float32 [3, 128, 64, 128], P(None, 'gx', 'gy'), may hold values from -6 to 6
- stress: float32 [6, 128, 64, 128], P(None, 'gx', 'gy'), may hold values from -6 to 6
- lame_first: float32 [128, 64, 128], P('gx', 'gy'), may hold values from 0.5 to 2
- modulus: float32 [128, 64, 128], P('gx', 'gy'), may hold values from 0.5 to 2
- buoyancy: float32 [128, 64, 128], P('gx', 'gy'), may hold values from 0.5 to 2
- zone: int32 [128, 64, 128], P('gx', 'gy'), may hold values from 0 to 7
- eligible: int32 [128, 64, 128], P('gx', 'gy'), may hold values 0 or 1
- cohesion: float32 [8], replicated, may hold values from 0.2 to 2
- friction: float32 [8], replicated, may hold values from 0.1 to 0.6
- source_cell: int32 [16], replicated, may hold values from 0 to 1048575
- source_moment: float32 [6, 16], replicated, may hold values from -15 to 15
Outputs:
- velocity_out: float32 [3, 128, 64, 128], P(None, 'gx', 'gy')
- stress_out: float32 [6, 128, 64, 128], P(None, 'gx', 'gy')
The draws below stay inside these ranges and needn't reach their ends.
All inputs are finite; a program needn't handle non-finite values. No bound on the sum of `eligible` on one device may be relied on, other than what follows from the above.
Results may differ from the reference program's by a relative error of at most 0.00011.
Values sent between devices are 32-bit elements; how exact they have to be, the bound alone decides.
No kernel may reach another device: no remote copies, remote signals or barrier semaphores. Data moves between devices by JAX's collectives and lax.ppermute only.
A program may use at most 64 MiB of HBM per device.

```python
import math
import jax
import jax.numpy as jnp
from jax import lax

NZ = 128
STEPS = 2
NZONES = 8
NSRC = 16
NX = 128
NY = 64


def with_ends(values, stream_key, low, largest):
    longest = values.shape.index(max(values.shape))
    spots = []
    for shift in (0, 1):
        where = [jax.random.randint(jax.random.fold_in(stream_key, axis), (), 0, length) for axis, length in enumerate(values.shape)]
        where[longest] = (where[longest] + shift) % values.shape[longest]
        spots.append(tuple(where))
    return values.at[spots[0]].set(low).at[spots[1]].set(largest)


def levels(stream_key, shape, cuts, smallest, high):
    def one(position, parts):
        steps = jax.random.uniform(jax.random.fold_in(jax.random.fold_in(stream_key, 6), position), (parts,), jnp.float32, smallest / len(cuts), high / len(cuts))
        return jnp.repeat(jnp.exp(steps), shape[position] // parts).reshape((-1,) + (1,) * (len(shape) - position - 1))

    level = one(*cuts[0])
    for cut in cuts[1:]:
        level = level * one(*cut)
    return level


def centred(key, extent, deviation, most, pieces=(), dtype=jnp.bfloat16):
    array = jax.random.normal(key, extent, jnp.float32) * deviation
    if len(pieces) > 0:
        array = levels(key, extent, pieces, -0.22, 0.18) * array
    return jnp.clip(array, min=-most, max=most).astype(dtype)


def setup_inputs(seed: int = 0) -> dict:
    seeds = jax.random.split(jax.random.key(seed), 12)
    return {
        "velocity": centred(seeds[0], (3, NX, NY, NZ), 1.0, 6.0, ((1, 4), (2, 8)), jnp.float32),
        "stress": centred(seeds[1], (6, NX, NY, NZ), 1.0, 6.0, ((1, 4), (2, 8)), jnp.float32),
        "lame_first": jnp.clip(jnp.exp(math.log(2.0) - 1.3862944 * jax.random.uniform(seeds[2], (NX, NY, NZ), jnp.float32) ** levels(seeds[2], (NX, NY, NZ), ((0, 4), (1, 8)), -0.2, 0.2)), 0.5, 2.0),
        "modulus": jnp.clip(jnp.exp(math.log(2.0) - 1.3862944 * jax.random.uniform(seeds[3], (NX, NY, NZ), jnp.float32) ** levels(seeds[3], (NX, NY, NZ), ((0, 4), (1, 8)), -0.2, 0.2)), 0.5, 2.0),
        "buoyancy": jnp.clip(jnp.exp(math.log(2.0) - 1.3862944 * jax.random.uniform(seeds[4], (NX, NY, NZ), jnp.float32) ** levels(seeds[4], (NX, NY, NZ), ((0, 4), (1, 8)), -0.2, 0.2)), 0.5, 2.0),
        "zone": with_ends(jax.random.randint(seeds[5], (NX, NY, NZ), 0, NZONES), jax.random.fold_in(seeds[5], 1), 0, NZONES - 1).astype(jnp.int32),
        "eligible": with_ends((jax.random.randint(seeds[6], (NX, NY, NZ), 0, 2) < 1).astype(jnp.int32), jax.random.fold_in(seeds[6], 1), 0, 1),
        "cohesion": jnp.clip(jnp.exp(jax.random.uniform(seeds[7], (NZONES,), jnp.float32, math.log(0.2), math.log(2.0))), 0.2, 2.0),
        "friction": jnp.clip(jax.random.uniform(seeds[8], (NZONES,), jnp.float32, 0.1, 0.6), 0.1, 0.6),
        "source_cell": with_ends(jax.random.randint(seeds[9], (NSRC,), 0, NX * NY * NZ), jax.random.fold_in(seeds[9], 1), 0, (NX * NY * NZ) - 1).astype(jnp.int32),
        "source_moment": centred(seeds[10], (6, NSRC), 3.0, 15.0, (), jnp.float32),
    }


time_step = 0.1
near_weight = 9.0 / 8.0
far_weight = 1.0 / 24.0
shear_floor = 0.25

def crop(padded, axis, offset):
    result = padded
    for dim in range(3):
        begin = offset if dim == axis else 2
        length = padded.shape[dim] - 4
        result = lax.slice_in_dim(result, begin, begin + length, axis=dim)
    return result

def derivative(padded, axis, forward):
    if forward:
        return near_weight * (crop(padded, axis, 3) - crop(padded, axis, 2)) - far_weight * (crop(padded, axis, 4) - crop(padded, axis, 1))
    return near_weight * (crop(padded, axis, 2) - crop(padded, axis, 1)) - far_weight * (crop(padded, axis, 3) - crop(padded, axis, 0))

def velocity_update(stress_pad, velocity, buoyancy):
    force_x = derivative(stress_pad[0], 0, True) + derivative(stress_pad[3], 1, False) + derivative(stress_pad[4], 2, False)
    force_y = derivative(stress_pad[3], 0, False) + derivative(stress_pad[1], 1, True) + derivative(stress_pad[5], 2, False)
    force_z = derivative(stress_pad[4], 0, False) + derivative(stress_pad[5], 1, False) + derivative(stress_pad[2], 2, True)
    forces = jnp.stack([force_x, force_y, force_z])
    return velocity + time_step * buoyancy[None] * forces

def stress_update(flow_pad, stress, lame_first, modulus):
    strain_x = derivative(flow_pad[0], 0, False)
    strain_y = derivative(flow_pad[1], 1, False)
    strain_z = derivative(flow_pad[2], 2, False)
    dilation = strain_x + strain_y + strain_z
    shear_xy = derivative(flow_pad[0], 1, True) + derivative(flow_pad[1], 0, True)
    shear_xz = derivative(flow_pad[0], 2, True) + derivative(flow_pad[2], 0, True)
    shear_yz = derivative(flow_pad[1], 2, True) + derivative(flow_pad[2], 1, True)
    rates = jnp.stack([lame_first * dilation + 2.0 * modulus * strain_x, lame_first * dilation + 2.0 * modulus * strain_y, lame_first * dilation + 2.0 * modulus * strain_z, modulus * shear_xy, modulus * shear_xz, modulus * shear_yz])
    return stress + time_step * rates

def plastic(stress, cell_cohesion, cell_friction, eligible):
    pressure = (stress[0] + stress[1] + stress[2]) / 3.0
    dev_x = stress[0] - pressure
    dev_y = stress[1] - pressure
    dev_z = stress[2] - pressure
    second = 0.5 * (dev_x * dev_x + dev_y * dev_y + dev_z * dev_z) + stress[3] * stress[3] + stress[4] * stress[4] + stress[5] * stress[5]
    strength = jnp.maximum(cell_cohesion * jnp.sqrt(1.0 - cell_friction * cell_friction) - pressure * cell_friction, 0.0)
    ratio = jnp.minimum(1.0, strength / jnp.maximum(jnp.sqrt(second), shear_floor))
    factor = jnp.where(eligible == 1, ratio, 1.0)
    return jnp.stack([pressure + factor * dev_x, pressure + factor * dev_y, pressure + factor * dev_z, factor * stress[3], factor * stress[4], factor * stress[5]])

def pad_space(field, width):
    return jnp.pad(field, ((0, 0), (width, width), (width, width), (width, width)))

def reference(velocity, stress, lame_first, modulus, buoyancy, zone, eligible, cohesion, friction, source_cell, source_moment):
    cell_cohesion = cohesion[zone]
    cell_friction = friction[zone]
    plane = NY * NZ
    src_x = (source_cell // plane).astype(jnp.int32)
    src_y = (source_cell // NZ % NY).astype(jnp.int32)
    src_z = (source_cell % NZ).astype(jnp.int32)
    injection = jnp.zeros_like(stress).at[:, src_x, src_y, src_z].add(time_step * source_moment)
    for step in range(STEPS):
        velocity = velocity_update(pad_space(stress, 2), velocity, buoyancy)
        stress = stress_update(pad_space(velocity, 2), stress, lame_first, modulus)
        stress = stress + injection
        stress = plastic(stress, cell_cohesion, cell_friction, eligible)
    return (velocity, stress)
```

```python
import jax
import jax.numpy as jnp
from jax import lax
from jax.experimental import pallas as pl
from jax.experimental.pallas import tpu as pltpu
from jax.sharding import PartitionSpec as P

STEPS = 2

time_step = 0.1
near_weight = 9.0 / 8.0
far_weight = 1.0 / 24.0
shear_floor = 0.25

XX, YY, ZZ, XY, XZ, YZ = range(6)

LOW_Y = ((XX, 1), (XY, 3), (XZ, 1), (YY, 3), (YZ, 3), (ZZ, 1))
HIGH_Y = ((XX, 2), (XY, 3), (XZ, 2), (YY, 3), (YZ, 3), (ZZ, 2))
LOW_X = ((XX, 3), (XY, 3), (XZ, 3), (YY, 1), (YZ, 1), (ZZ, 1))
HIGH_X = ((XX, 3), (XY, 3), (XZ, 3), (YY, 2), (YZ, 2), (ZZ, 2))
LOW_FLOW_Y = ((0, 1), (1, 2), (2, 1))
HIGH_FLOW_Y = ((0, 2), (1, 1), (2, 2))
LOW_FLOW_X = ((0, 2), (1, 1), (2, 1))
HIGH_FLOW_X = ((0, 1), (1, 2), (2, 2))

PAD_X = 4
RIM = 8


class Shape:
    def __init__(self, rows_x, rows_y, depth):
        self.rows_x, self.rows_y, self.depth = rows_x, rows_y, depth
        self.pitch = rows_y + RIM
        self.rows = (rows_x + 2 * PAD_X + 1) * self.pitch

    def row(self, x, y):
        return (x + PAD_X) * self.pitch + RIM + y


def entries(spec):
    return [(c, k) for c, depth in spec for k in range(depth)]


def y_rows(low, high, rows_y):
    up = [(c, rows_y - 1 - k) for c, k in entries(low)]
    down = [(c, k) for c, k in entries(high)]
    return up, down


def got_y(low, high, rows_y):
    below = [(c, -1 - k) for c, k in entries(low)]
    above = [(c, rows_y + k) for c, k in entries(high)]
    return below, above


def pack_y(shape, pairs, out):
    for slot, (ref, y) in enumerate(pairs):
        for x in range(0, shape.rows_x, 8):
            out[slot, pl.ds(x, 8), :] = ref[pl.ds(shape.row(x, y), 8, stride=shape.pitch), :]


def unpack_y(shape, pairs, got):
    for slot, (ref, y) in enumerate(pairs):
        for x in range(0, shape.rows_x, 8):
            ref[pl.ds(shape.row(x, y), 8, stride=shape.pitch), :] = got[slot, pl.ds(x, 8), :]


def pack_x(shape, whole, inner, out):
    sub = lax.broadcasted_iota(jnp.int32, (8, shape.depth), 0)
    slot = 0
    for ref, x, rim in whole:
        for t in range(0, shape.rows_y, 8):
            out[slot] = ref[pl.ds(shape.row(x, t), 8), :]
            slot += 1
        if rim:
            after = ref[pl.ds(shape.row(x + 1, -RIM), 8), :]
            before = ref[pl.ds(shape.row(x, -RIM), 8), :]
            out[slot] = jnp.where(sub < 4, after, before)
            slot += 1
    return slot


def unpack_x(shape, whole, got):
    slot = 0
    for ref, x, rim in whole:
        for t in range(0, shape.rows_y, 8):
            ref[pl.ds(shape.row(x, t), 8), :] = got[slot]
            slot += 1
        if rim:
            ref[pl.ds(shape.row(x + 1, -RIM), 4), :] = got[slot, 0:4, :]
            ref[pl.ds(shape.row(x, -4), 4), :] = got[slot, 4:8, :]
            slot += 1


def x_slots(spec, rows_y, rim):
    count = 0
    for c, depth in spec:
        count += depth * (rows_y // 8 + (1 if rim and c != ZZ else 0))
    return count


def x_list(stress, flow, buoyancy, spec, flow_spec, place):
    whole = [(stress.at[c], place(k), c != ZZ) for c, k in entries(spec)]
    if flow is not None:
        whole += [(flow.at[c], place(k), False) for c, k in entries(flow_spec)]
        whole += [(buoyancy, place(k), False) for k in range(2)]
    return whole


def y_list(stress, flow, buoyancy, rows, flow_rows, rim_rows):
    pairs = [(stress.at[c], y) for c, y in rows]
    if flow is not None:
        pairs += [(flow.at[c], y) for c, y in flow_rows]
        pairs += [(buoyancy, y) for y in rim_rows]
    return pairs


def send_y(shape, stress, flow, buoyancy, first, second):
    rows_y = shape.rows_y
    up, down = y_rows(LOW_Y, HIGH_Y, rows_y)
    flow_up, flow_down = y_rows(LOW_FLOW_Y, HIGH_FLOW_Y, rows_y)
    up = y_list(stress, flow, buoyancy, up, flow_up, (rows_y - 1, rows_y - 2))
    down = y_list(stress, flow, buoyancy, down, flow_down, (0, 1))
    odd = lax.axis_index("gy") % 2

    @pl.when(odd == 0)
    def _():
        pack_y(shape, up, first)
        pack_y(shape, down, second)

    @pl.when(odd == 1)
    def _():
        pack_y(shape, down, first)
        pack_y(shape, up, second)


def receive_y(shape, stress, flow, buoyancy, first, second):
    rows_y = shape.rows_y
    below, above = got_y(LOW_Y, HIGH_Y, rows_y)
    flow_below, flow_above = got_y(LOW_FLOW_Y, HIGH_FLOW_Y, rows_y)
    below = y_list(stress, flow, buoyancy, below, flow_below, (-1, -2))
    above = y_list(stress, flow, buoyancy, above, flow_above, (rows_y, rows_y + 1))
    odd = lax.axis_index("gy") % 2

    @pl.when(odd == 0)
    def _():
        unpack_y(shape, above, first)
        unpack_y(shape, below, second)

    @pl.when(odd == 1)
    def _():
        unpack_y(shape, below, first)
        unpack_y(shape, above, second)


def send_x(shape, stress, flow, buoyancy, first, second):
    last = shape.rows_x - 1
    up = x_list(stress, flow, buoyancy, LOW_X, LOW_FLOW_X, lambda k: last - k)
    down = x_list(stress, flow, buoyancy, HIGH_X, HIGH_FLOW_X, lambda k: k)
    odd = lax.axis_index("gx") % 2

    @pl.when(odd == 0)
    def _():
        pack_x(shape, up, None, first)
        pack_x(shape, down, None, second)

    @pl.when(odd == 1)
    def _():
        pack_x(shape, down, None, first)
        pack_x(shape, up, None, second)


def receive_x(shape, stress, flow, buoyancy, first, second):
    below = x_list(stress, flow, buoyancy, LOW_X, LOW_FLOW_X, lambda k: -1 - k)
    above = x_list(stress, flow, buoyancy, HIGH_X, HIGH_FLOW_X, lambda k: shape.rows_x + k)
    odd = lax.axis_index("gx") % 2

    @pl.when(odd == 0)
    def _():
        unpack_x(shape, above, first)
        unpack_x(shape, below, second)

    @pl.when(odd == 1)
    def _():
        unpack_x(shape, below, first)
        unpack_x(shape, above, second)


class Lanes:
    def __init__(self, depth):
        self.depth = depth
        lane = lax.broadcasted_iota(jnp.int32, (8, depth), 1)
        zero = jnp.zeros((8, depth), jnp.float32)
        near = jnp.full((8, depth), near_weight, jnp.float32)
        far = jnp.full((8, depth), far_weight, jnp.float32)
        self.f_up = jnp.where(lane < depth - 1, near, zero)
        self.f_up2 = jnp.where(lane < depth - 2, far, zero)
        self.f_down = jnp.where(lane > 0, far, zero)
        self.b_down = jnp.where(lane > 0, near, zero)
        self.b_down2 = jnp.where(lane > 1, far, zero)
        self.b_up = jnp.where(lane < depth - 1, far, zero)

    def forward(self, f):
        up, up2, down = (pltpu.roll(f, s % self.depth, 1) for s in (-1, -2, 1))
        return (self.f_up * up - near_weight * f) - (self.f_up2 * up2 - self.f_down * down)

    def backward(self, f):
        up, down, down2 = (pltpu.roll(f, s % self.depth, 1) for s in (-1, 1, 2))
        return (near_weight * f - self.b_down * down) - (self.b_up * up - self.b_down2 * down2)


def forward(ref, row, step):
    a, b, c, d = (ref[pl.ds(row + k * step, 8), :] for k in (-1, 0, 1, 2))
    return near_weight * (c - b) - far_weight * (d - a)


def backward(ref, row, step):
    a, b, c, d = (ref[pl.ds(row + k * step, 8), :] for k in (-2, -1, 0, 1))
    return near_weight * (c - b) - far_weight * (d - a)


def tile(ref, row):
    return ref[pl.ds(row, 8), :]


def update_velocity(shape, stress, flow, buoyancy):
    lanes = Lanes(shape.depth)
    sx, sy = shape.pitch, 1
    xx, yy, zz, xy, xz, yz = (stress.at[c] for c in range(6))

    def layer(i, carry):
        base = pl.multiple_of(i * shape.pitch, 8)
        for t in range(0, shape.pitch, 8):
            row = base + t
            scale = time_step * tile(buoyancy, row)
            force_x = forward(xx, row, sx) + backward(xy, row, sy) + lanes.backward(tile(xz, row))
            flow[0, pl.ds(row, 8), :] += scale * force_x
            force_y = backward(xy, row, sx) + forward(yy, row, sy) + lanes.backward(tile(yz, row))
            flow[1, pl.ds(row, 8), :] += scale * force_y
            force_z = backward(xz, row, sx) + backward(yz, row, sy) + lanes.forward(tile(zz, row))
            flow[2, pl.ds(row, 8), :] += scale * force_z
        return carry

    lax.fori_loop(PAD_X - 2, PAD_X + shape.rows_x + 2, layer, 0)


def inject(shape, stress, source_cell, source_moment):
    rows_x, rows_y, depth = shape.rows_x, shape.rows_y, shape.depth
    total_y = rows_y * lax.axis_size("gy")
    start_x = lax.axis_index("gx") * rows_x
    start_y = lax.axis_index("gy") * rows_y
    sub = lax.broadcasted_iota(jnp.int32, (8, depth), 0)
    lane = lax.broadcasted_iota(jnp.int32, (8, depth), 1)
    for s in range(source_cell.shape[0]):
        cell = source_cell[s]
        x = cell // (total_y * depth) - start_x
        y = cell // depth % total_y - start_y
        z = cell % depth

        @pl.when((x >= 0) & (x < rows_x) & (y >= 0) & (y < rows_y))
        def _(x=x, y=y, z=z, s=s):
            row = pl.multiple_of((x + PAD_X) * shape.pitch + RIM + y // 8 * 8, 8)
            here = (sub == y % 8) & (lane == z)
            for c in range(6):
                amount = time_step * source_moment[c, s]
                stress[c, pl.ds(row, 8), :] += jnp.where(here, amount, 0.0)


def update_stress(shape, stress, flow, rock):
    lanes = Lanes(shape.depth)
    sx, sy = shape.pitch, 1
    vx, vy, vz = (flow.at[c] for c in range(3))

    def layer(i, carry):
        for t in range(0, shape.rows_y, 8):
            row = pl.multiple_of((i + PAD_X) * shape.pitch + RIM + t, 8)
            own = pl.multiple_of(i * shape.rows_y + t, 8)
            first = time_step * rock[0, pl.ds(own, 8), :]
            shear = time_step * rock[1, pl.ds(own, 8), :]
            strain_x = backward(vx, row, sx)
            strain_y = backward(vy, row, sy)
            here_z = tile(vz, row)
            strain_z = lanes.backward(here_z)
            volume = first * (strain_x + strain_y + strain_z)
            twice = 2.0 * shear
            xx = tile(stress.at[XX], row) + (volume + twice * strain_x)
            yy = tile(stress.at[YY], row) + (volume + twice * strain_y)
            zz = tile(stress.at[ZZ], row) + (volume + twice * strain_z)
            xy = tile(stress.at[XY], row) + shear * (forward(vx, row, sy) + forward(vy, row, sx))
            xz = tile(stress.at[XZ], row) + shear * (
                lanes.forward(tile(vx, row)) + forward(vz, row, sx)
            )
            yz = tile(stress.at[YZ], row) + shear * (
                lanes.forward(tile(vy, row)) + forward(vz, row, sy)
            )
            pressure = (xx + yy + zz) * (1.0 / 3.0)
            dx, dy, dz = xx - pressure, yy - pressure, zz - pressure
            second = 0.5 * (dx * dx + dy * dy + dz * dz) + xy * xy + xz * xz + yz * yz
            strength = jnp.maximum(
                rock[2, pl.ds(own, 8), :] - pressure * rock[3, pl.ds(own, 8), :], 0.0
            )
            ratio = strength * lax.rsqrt(jnp.maximum(second, shear_floor * shear_floor))
            factor = jnp.where(rock[4, pl.ds(own, 8), :] > 0.5, jnp.minimum(ratio, 1.0), 1.0)
            stress[XX, pl.ds(row, 8), :] = pressure + factor * dx
            stress[YY, pl.ds(row, 8), :] = pressure + factor * dy
            stress[ZZ, pl.ds(row, 8), :] = pressure + factor * dz
            stress[XY, pl.ds(row, 8), :] = factor * xy
            stress[XZ, pl.ds(row, 8), :] = factor * xz
            stress[YZ, pl.ds(row, 8), :] = factor * yz
        return carry

    lax.fori_loop(0, shape.rows_x, layer, 0)


def own_cells(shape, ref):
    lead = ref.shape[:-2]
    view = ref.reshape(*lead, shape.rows_x + 2 * PAD_X + 1, shape.pitch, shape.depth)
    return view.at[
        (slice(None),) * len(lead) + (pl.ds(PAD_X, shape.rows_x), pl.ds(RIM, shape.rows_y))
    ]


def vmem(shape):
    return pltpu.VMEM(shape, jnp.float32)


in_vmem = pl.BlockSpec(memory_space=pltpu.VMEM)
in_smem = pl.BlockSpec(memory_space=pltpu.SMEM)
in_hbm = pl.BlockSpec(memory_space=pl.ANY)


def call(body, ins, in_specs, out_shape, out_specs, name, flops, aliases=None, scratch=()):
    ins = [
        pltpu.with_memory_space_constraint(x, pltpu.VMEM) if s is in_vmem else x
        for x, s in zip(ins, in_specs)
    ]
    return pl.pallas_call(
        body,
        in_specs=in_specs,
        out_shape=out_shape,
        out_specs=out_specs,
        input_output_aliases=aliases or {},
        scratch_shapes=scratch,
        name=name,
        cost_estimate=pl.CostEstimate(flops=flops, bytes_accessed=1000000, transcendentals=0),
        compiler_params=pltpu.CompilerParams(vmem_limit_bytes=16 * 1024 * 1024),
    )(*ins)


def swaps(axis, first, second):
    count = lax.axis_size(axis)
    got = []
    for start, block in ((0, first), (1, second)):
        pairs = []
        for low in range(start, count - 1, 2):
            pairs += [(low, low + 1), (low + 1, low)]
        got.append(lax.ppermute(block, axis, pairs))
    return got


def on_device(
    velocity,
    stress,
    lame_first,
    modulus,
    buoyancy,
    zone,
    eligible,
    cohesion,
    friction,
    source_cell,
    source_moment,
):
    shape = Shape(*zone.shape)
    rows_x, rows_y, depth = zone.shape
    whole_s, whole_v = vmem((6, shape.rows, depth)), vmem((3, shape.rows, depth))
    whole_b = vmem((shape.rows, depth))
    stress_rows = max(len(entries(LOW_Y)), len(entries(HIGH_Y)))
    all_rows = stress_rows + 5 + 2
    stress_slots = max(x_slots(LOW_X, rows_y, True), x_slots(HIGH_X, rows_y, True))
    flow_slots = (max(x_slots(LOW_FLOW_X, rows_y, False), x_slots(HIGH_FLOW_X, rows_y, False))
                  + 2 * (rows_y // 8))

    def buffers(axis, first_round):
        if axis == "y":
            return vmem((all_rows if first_round else stress_rows, rows_x, depth))
        return vmem((stress_slots + (flow_slots if first_round else 0), 8, depth))

    def load(v_in, s_in, b_in, s, v, b, first, second, sems):
        copies = [
            pltpu.make_async_copy(s_in, own_cells(shape, s), sems.at[0]),
            pltpu.make_async_copy(v_in, own_cells(shape, v), sems.at[1]),
            pltpu.make_async_copy(b_in, own_cells(shape, b), sems.at[2]),
        ]
        for c in copies:
            c.start()
        for c in copies:
            c.wait()
        send_y(shape, s, v, b, first, second)

    s, v, b, first, second = call(
        load,
        [velocity, stress, buoyancy],
        [in_hbm] * 3,
        [whole_s, whole_v, whole_b, buffers("y", True), buffers("y", True)],
        [in_vmem] * 5,
        "load",
        1000000,
        scratch=[pltpu.SemaphoreType.DMA((3,))],
    )

    def prepare(lame_in, shear_in, zone_in, eligible_in, cohesion, friction, rock, zones, able, sems):
        flat = rock.reshape(5, rows_x, rows_y, depth)
        copies = [
            pltpu.make_async_copy(zone_in, zones, sems.at[0]),
            pltpu.make_async_copy(eligible_in, able, sems.at[1]),
            pltpu.make_async_copy(lame_in, flat.at[0], sems.at[2]),
            pltpu.make_async_copy(shear_in, flat.at[1], sems.at[3]),
        ]
        for c in copies:
            c.start()
        copies[0].wait()
        copies[1].wait()

        def layer(i, carry):
            for t in range(0, rows_y, 8):
                own = pl.multiple_of(i * rows_y + t, 8)
                which = zones[i, pl.ds(t, 8), :]
                hold = jnp.full((8, depth), cohesion[0], jnp.float32)
                rub = jnp.full((8, depth), friction[0], jnp.float32)
                for k in range(1, cohesion.shape[0]):
                    hit = which == k
                    hold = jnp.where(hit, cohesion[k], hold)
                    rub = jnp.where(hit, friction[k], rub)
                rock[2, pl.ds(own, 8), :] = hold * jnp.sqrt(1.0 - rub * rub)
                rock[3, pl.ds(own, 8), :] = rub
                rock[4, pl.ds(own, 8), :] = jnp.where(able[i, pl.ds(t, 8), :] == 1, 1.0, 0.0)
            return carry

        lax.fori_loop(0, rows_x, layer, 0)
        copies[2].wait()
        copies[3].wait()

    rock = call(
        prepare,
        [lame_first, modulus, zone, eligible, cohesion, friction],
        [in_hbm] * 4 + [in_smem] * 2,
        vmem((5, rows_x * rows_y, depth)),
        in_vmem,
        "prepare",
        1000000,
        scratch=[
            pltpu.VMEM((rows_x, rows_y, depth), jnp.int32),
            pltpu.VMEM((rows_x, rows_y, depth), jnp.int32),
            pltpu.SemaphoreType.DMA((4,)),
        ],
    )

    for step in range(STEPS):
        begin, end = step == 0, step == STEPS - 1
        first, second = swaps("gy", first, second)

        if begin:

            def turn(s_in, v_in, b_in, got_a, got_b, s, v, b, out_a, out_b):
                receive_y(shape, s, v, b, got_a, got_b)
                send_x(shape, s, v, b, out_a, out_b)

            s, v, b, first, second = call(
                turn,
                [s, v, b, first, second],
                [in_vmem] * 5,
                [whole_s, whole_v, whole_b, buffers("x", True), buffers("x", True)],
                [in_vmem] * 5,
                "turn_first",
                1000000,
                aliases={0: 0, 1: 1, 2: 2},
            )
        else:

            def turn(s_in, got_a, got_b, s, out_a, out_b):
                receive_y(shape, s, None, None, got_a, got_b)
                send_x(shape, s, None, None, out_a, out_b)

            s, first, second = call(
                turn,
                [s, first, second],
                [in_vmem] * 3,
                [whole_s, buffers("x", False), buffers("x", False)],
                [in_vmem] * 3,
                "turn",
                1000000,
                aliases={0: 0},
            )
        first, second = swaps("gx", first, second)

        if not end:

            def advance(s_in, v_in, b_in, rock, got_a, got_b, cell, moment, s, v, b, out_a, out_b):
                fields = (s, v, b) if begin else (s, None, None)
                receive_x(shape, *fields, got_a, got_b)
                update_velocity(shape, s, v, b)
                inject(shape, s, cell, moment)
                update_stress(shape, s, v, rock)
                send_y(shape, s, None, None, out_a, out_b)

            s, v, b, first, second = call(
                advance,
                [s, v, b, rock, first, second, source_cell, source_moment],
                [in_vmem] * 6 + [in_smem] * 2,
                [whole_s, whole_v, whole_b, buffers("y", False), buffers("y", False)],
                [in_vmem] * 5,
                "advance",
                10000000,
                aliases={0: 0, 1: 1, 2: 2},
            )
        else:

            def finish(s_in, v_in, b, rock, got_a, got_b, cell, moment, s, v, v_out, s_out, sems):
                receive_x(shape, s, None, None, got_a, got_b)
                update_velocity(shape, s, v, b)
                out_v = pltpu.make_async_copy(own_cells(shape, v), v_out, sems.at[0])
                out_v.start()
                inject(shape, s, cell, moment)
                update_stress(shape, s, v, rock)
                out_s = pltpu.make_async_copy(own_cells(shape, s), s_out, sems.at[1])
                out_s.start()
                out_v.wait()
                out_s.wait()

            _, _, velocity, stress = call(
                finish,
                [s, v, b, rock, first, second, source_cell, source_moment],
                [in_vmem] * 6 + [in_smem] * 2,
                [
                    whole_s,
                    whole_v,
                    jax.ShapeDtypeStruct(velocity.shape, jnp.float32),
                    jax.ShapeDtypeStruct(stress.shape, jnp.float32),
                ],
                [in_vmem, in_vmem, in_hbm, in_hbm],
                "finish",
                10000000,
                aliases={0: 0, 1: 1},
                scratch=[pltpu.SemaphoreType.DMA((2,))],
            )
    return (velocity, stress)


def solution(mesh):
    placed = (
        P(None, "gx", "gy", None),
        P(None, "gx", "gy", None),
        P("gx", "gy", None),
        P("gx", "gy", None),
        P("gx", "gy", None),
        P("gx", "gy", None),
        P("gx", "gy", None),
        P(),
        P(),
        P(),
        P(),
    )
    return jax.shard_map(
        on_device,
        mesh=mesh,
        in_specs=placed,
        out_specs=(P(None, "gx", "gy", None), P(None, "gx", "gy", None)),
        check_vma=False,
    )
```

```python
import jax
import jax.numpy as jnp
from jax import lax
from jax.experimental import pallas as pl
from jax.experimental.pallas import tpu as pltpu
from jax.sharding import PartitionSpec as P

STEPS = 2

time_step = 0.1
near_weight = 9.0 / 8.0
far_weight = 1.0 / 24.0
shear_floor = 0.25

XX, YY, ZZ, XY, XZ, YZ = range(6)

LOW_Y = ((XX, 1), (XY, 3), (XZ, 1), (YY, 3), (YZ, 3), (ZZ, 1))
HIGH_Y = ((XX, 2), (XY, 3), (XZ, 2), (YY, 3), (YZ, 3), (ZZ, 2))
LOW_X = ((XX, 3), (XY, 3), (XZ, 3), (YY, 1), (YZ, 1), (ZZ, 1))
HIGH_X = ((XX, 3), (XY, 3), (XZ, 3), (YY, 2), (YZ, 2), (ZZ, 2))
LOW_FLOW_Y = ((0, 1), (1, 2), (2, 1))
HIGH_FLOW_Y = ((0, 2), (1, 1), (2, 2))
LOW_FLOW_X = ((0, 2), (1, 1), (2, 1))
HIGH_FLOW_X = ((0, 1), (1, 2), (2, 2))

PAD_X = 4
RIM = 8


class Shape:
    def __init__(self, rows_x, rows_y, depth):
        self.rows_x, self.rows_y, self.depth = rows_x, rows_y, depth
        self.pitch = rows_y + RIM
        self.rows = (rows_x + 2 * PAD_X + 1) * self.pitch

    def row(self, x, y):
        return (x + PAD_X) * self.pitch + RIM + y


def entries(spec):
    return [(c, k) for c, depth in spec for k in range(depth)]


def y_rows(low, high, rows_y):
    up = [(c, rows_y - 1 - k) for c, k in entries(low)]
    down = [(c, k) for c, k in entries(high)]
    return up, down


def got_y(low, high, rows_y):
    below = [(c, -1 - k) for c, k in entries(low)]
    above = [(c, rows_y + k) for c, k in entries(high)]
    return below, above


def pack_y(shape, pairs, out):
    for slot, (ref, y) in enumerate(pairs):
        for x in range(0, shape.rows_x, 8):
            out[slot, pl.ds(x, 8), :] = ref[pl.ds(shape.row(x, y), 8, stride=shape.pitch), :]


def unpack_y(shape, pairs, got):
    for slot, (ref, y) in enumerate(pairs):
        for x in range(0, shape.rows_x, 8):
            ref[pl.ds(shape.row(x, y), 8, stride=shape.pitch), :] = got[slot, pl.ds(x, 8), :]


def pack_x(shape, whole, inner, out):
    sub = lax.broadcasted_iota(jnp.int32, (8, shape.depth), 0)
    slot = 0
    for ref, x, rim in whole:
        for t in range(0, shape.rows_y, 8):
            out[slot] = ref[pl.ds(shape.row(x, t), 8), :]
            slot += 1
        if rim:
            after = ref[pl.ds(shape.row(x + 1, -RIM), 8), :]
            before = ref[pl.ds(shape.row(x, -RIM), 8), :]
            out[slot] = jnp.where(sub < 4, after, before)
            slot += 1
    return slot


def unpack_x(shape, whole, got):
    slot = 0
    for ref, x, rim in whole:
        for t in range(0, shape.rows_y, 8):
            ref[pl.ds(shape.row(x, t), 8), :] = got[slot]
            slot += 1
        if rim:
            ref[pl.ds(shape.row(x + 1, -RIM), 4), :] = got[slot, 0:4, :]
            ref[pl.ds(shape.row(x, -4), 4), :] = got[slot, 4:8, :]
            slot += 1


def x_slots(spec, rows_y, rim):
    count = 0
    for c, depth in spec:
        count += depth * (rows_y // 8 + (1 if rim and c != ZZ else 0))
    return count


def x_list(stress, flow, buoyancy, spec, flow_spec, place):
    whole = [(stress.at[c], place(k), c != ZZ) for c, k in entries(spec)]
    if flow is not None:
        whole += [(flow.at[c], place(k), False) for c, k in entries(flow_spec)]
        whole += [(buoyancy, place(k), False) for k in range(2)]
    return whole


def y_list(stress, flow, buoyancy, rows, flow_rows, rim_rows):
    pairs = [(stress.at[c], y) for c, y in rows]
    if flow is not None:
        pairs += [(flow.at[c], y) for c, y in flow_rows]
        pairs += [(buoyancy, y) for y in rim_rows]
    return pairs


def send_y(shape, stress, flow, buoyancy, first, second):
    rows_y = shape.rows_y
    up, down = y_rows(LOW_Y, HIGH_Y, rows_y)
    flow_up, flow_down = y_rows(LOW_FLOW_Y, HIGH_FLOW_Y, rows_y)
    up = y_list(stress, flow, buoyancy, up, flow_up, (rows_y - 1, rows_y - 2))
    down = y_list(stress, flow, buoyancy, down, flow_down, (0, 1))
    odd = lax.axis_index("gy") % 2

    @pl.when(odd == 0)
    def _():
        pack_y(shape, up, first)
        pack_y(shape, down, second)

    @pl.when(odd == 1)
    def _():
        pack_y(shape, down, first)
        pack_y(shape, up, second)


def receive_y(shape, stress, flow, buoyancy, first, second):
    rows_y = shape.rows_y
    below, above = got_y(LOW_Y, HIGH_Y, rows_y)
    flow_below, flow_above = got_y(LOW_FLOW_Y, HIGH_FLOW_Y, rows_y)
    below = y_list(stress, flow, buoyancy, below, flow_below, (-1, -2))
    above = y_list(stress, flow, buoyancy, above, flow_above, (rows_y, rows_y + 1))
    odd = lax.axis_index("gy") % 2

    @pl.when(odd == 0)
    def _():
        unpack_y(shape, above, first)
        unpack_y(shape, below, second)

    @pl.when(odd == 1)
    def _():
        unpack_y(shape, below, first)
        unpack_y(shape, above, second)


def send_x(shape, stress, flow, buoyancy, first, second):
    last = shape.rows_x - 1
    up = x_list(stress, flow, buoyancy, LOW_X, LOW_FLOW_X, lambda k: last - k)
    down = x_list(stress, flow, buoyancy, HIGH_X, HIGH_FLOW_X, lambda k: k)
    odd = lax.axis_index("gx") % 2

    @pl.when(odd == 0)
    def _():
        pack_x(shape, up, None, first)
        pack_x(shape, down, None, second)

    @pl.when(odd == 1)
    def _():
        pack_x(shape, down, None, first)
        pack_x(shape, up, None, second)


def receive_x(shape, stress, flow, buoyancy, first, second):
    below = x_list(stress, flow, buoyancy, LOW_X, LOW_FLOW_X, lambda k: -1 - k)
    above = x_list(stress, flow, buoyancy, HIGH_X, HIGH_FLOW_X, lambda k: shape.rows_x + k)
    odd = lax.axis_index("gx") % 2

    @pl.when(odd == 0)
    def _():
        unpack_x(shape, above, first)
        unpack_x(shape, below, second)

    @pl.when(odd == 1)
    def _():
        unpack_x(shape, below, first)
        unpack_x(shape, above, second)


class Lanes:
    def __init__(self, depth):
        self.depth = depth
        lane = lax.broadcasted_iota(jnp.int32, (8, depth), 1)
        zero = jnp.zeros((8, depth), jnp.float32)
        near = jnp.full((8, depth), near_weight, jnp.float32)
        far = jnp.full((8, depth), far_weight, jnp.float32)
        self.f_up = jnp.where(lane < depth - 1, near, zero)
        self.f_up2 = jnp.where(lane < depth - 2, far, zero)
        self.f_down = jnp.where(lane > 0, far, zero)
        self.b_down = jnp.where(lane > 0, near, zero)
        self.b_down2 = jnp.where(lane > 1, far, zero)
        self.b_up = jnp.where(lane < depth - 1, far, zero)

    def forward(self, f):
        up, up2, down = (pltpu.roll(f, s % self.depth, 1) for s in (-1, -2, 1))
        return (self.f_up * up - near_weight * f) - (self.f_up2 * up2 - self.f_down * down)

    def backward(self, f):
        up, down, down2 = (pltpu.roll(f, s % self.depth, 1) for s in (-1, 1, 2))
        return (near_weight * f - self.b_down * down) - (self.b_up * up - self.b_down2 * down2)


def forward(ref, row, step):
    a, b, c, d = (ref[pl.ds(row + k * step, 8), :] for k in (-1, 0, 1, 2))
    return near_weight * (c - b) - far_weight * (d - a)


def backward(ref, row, step):
    a, b, c, d = (ref[pl.ds(row + k * step, 8), :] for k in (-2, -1, 0, 1))
    return near_weight * (c - b) - far_weight * (d - a)


def tile(ref, row):
    return ref[pl.ds(row, 8), :]


def push_velocity(shape, lanes, stress, flow, buoyancy, row, along="xyz"):
    sx, sy = shape.pitch, 1
    xx, yy, zz, xy, xz, yz = (stress.at[c] for c in range(6))
    parts = {
        "x": lambda: (forward(xx, row, sx), backward(xy, row, sx), backward(xz, row, sx)),
        "y": lambda: (backward(xy, row, sy), forward(yy, row, sy), backward(yz, row, sy)),
        "z": lambda: (
            lanes.backward(tile(xz, row)),
            lanes.backward(tile(yz, row)),
            lanes.forward(tile(zz, row)),
        ),
    }
    force = parts[along[0]]()
    for axis in along[1:]:
        force = [f + g for f, g in zip(force, parts[axis]())]
    scale = time_step * tile(buoyancy, row)
    for c in range(3):
        flow[c, pl.ds(row, 8), :] += scale * force[c]


def layers(first, stop, body, unroll):
    def run(x, carry):
        body(x)
        return carry

    lax.fori_loop(first, stop, run, 0, unroll=unroll)


def aligned(shape, x, y):
    return pl.multiple_of((x + PAD_X) * shape.pitch + RIM + y, 8)


def inject(shape, stress, source_cell, source_moment, wanted):
    rows_x, rows_y, depth = shape.rows_x, shape.rows_y, shape.depth
    total_y = rows_y * lax.axis_size("gy")
    start_x = lax.axis_index("gx") * rows_x
    start_y = lax.axis_index("gy") * rows_y
    sub = lax.broadcasted_iota(jnp.int32, (8, depth), 0)
    lane = lax.broadcasted_iota(jnp.int32, (8, depth), 1)
    for s in range(source_cell.shape[0]):
        cell = source_cell[s]
        line = lax.div(cell, depth)
        x = lax.div(line, total_y) - start_x
        y = lax.rem(line, total_y) - start_y
        z = lax.rem(cell, depth)

        @pl.when(wanted(x) & (y >= 0) & (y < rows_y))
        def _(x=x, y=y, z=z, s=s):
            band = lax.div(y, 8) * 8
            row = aligned(shape, x, band)
            here = (sub == y - band) & (lane == z)
            for c in range(6):
                amount = time_step * source_moment[c, s]
                stress[c, pl.ds(row, 8), :] += jnp.where(here, amount, 0.0)


def push_stress(shape, lanes, stress, flow, rock, x):
    sx, sy = shape.pitch, 1
    vx, vy, vz = (flow.at[c] for c in range(3))

    for t in range(0, shape.rows_y, 8):
        row = aligned(shape, x, t)
        own = pl.multiple_of(x * shape.rows_y + t, 8)
        first = time_step * rock[0, pl.ds(own, 8), :]
        shear = time_step * rock[1, pl.ds(own, 8), :]
        strain_x = backward(vx, row, sx)
        strain_y = backward(vy, row, sy)
        here_z = tile(vz, row)
        strain_z = lanes.backward(here_z)
        volume = first * (strain_x + strain_y + strain_z)
        twice = 2.0 * shear
        xx = tile(stress.at[XX], row) + (volume + twice * strain_x)
        yy = tile(stress.at[YY], row) + (volume + twice * strain_y)
        zz = tile(stress.at[ZZ], row) + (volume + twice * strain_z)
        xy = tile(stress.at[XY], row) + shear * (forward(vx, row, sy) + forward(vy, row, sx))
        xz = tile(stress.at[XZ], row) + shear * (
            lanes.forward(tile(vx, row)) + forward(vz, row, sx)
        )
        yz = tile(stress.at[YZ], row) + shear * (
            lanes.forward(tile(vy, row)) + forward(vz, row, sy)
        )
        pressure = (xx + yy + zz) * (1.0 / 3.0)
        dx, dy, dz = xx - pressure, yy - pressure, zz - pressure
        second = 0.5 * (dx * dx + dy * dy + dz * dz) + xy * xy + xz * xz + yz * yz
        strength = jnp.maximum(
            rock[2, pl.ds(own, 8), :] - pressure * rock[3, pl.ds(own, 8), :], 0.0
        )
        ratio = strength * lax.rsqrt(jnp.maximum(second, shear_floor * shear_floor))
        factor = jnp.where(rock[4, pl.ds(own, 8), :] > 0.5, jnp.minimum(ratio, 1.0), 1.0)
        stress[XX, pl.ds(row, 8), :] = pressure + factor * dx
        stress[YY, pl.ds(row, 8), :] = pressure + factor * dy
        stress[ZZ, pl.ds(row, 8), :] = pressure + factor * dz
        stress[XY, pl.ds(row, 8), :] = factor * xy
        stress[XZ, pl.ds(row, 8), :] = factor * xz
        stress[YZ, pl.ds(row, 8), :] = factor * yz


def own_cells(shape, ref, first=0, count=None):
    lead = ref.shape[:-2]
    view = ref.reshape(*lead, shape.rows_x + 2 * PAD_X + 1, shape.pitch, shape.depth)
    count = shape.rows_x - first if count is None else count
    return view.at[
        (slice(None),) * len(lead) + (pl.ds(PAD_X + first, count), pl.ds(RIM, shape.rows_y))
    ]


def run_copies(pairs, sems):
    copies = [pltpu.make_async_copy(a, b, sems.at[i]) for i, (a, b) in enumerate(pairs)]
    for c in copies:
        c.start()
    for c in copies:
        c.wait()


def vmem(shape):
    return pltpu.VMEM(shape, jnp.float32)


in_vmem = pl.BlockSpec(memory_space=pltpu.VMEM)
in_smem = pl.BlockSpec(memory_space=pltpu.SMEM)
in_hbm = pl.BlockSpec(memory_space=pltpu.HBM)


def call(body, ins, in_specs, out_shape, out_specs, name, flops, aliases=None, scratch=()):
    space = {id(in_vmem): pltpu.VMEM, id(in_hbm): pltpu.HBM}
    ins = [
        pltpu.with_memory_space_constraint(x, space[id(s)]) if id(s) in space else x
        for x, s in zip(ins, in_specs)
    ]
    return pl.pallas_call(
        body,
        in_specs=in_specs,
        out_shape=out_shape,
        out_specs=out_specs,
        input_output_aliases=aliases or {},
        scratch_shapes=scratch,
        name=name,
        cost_estimate=pl.CostEstimate(flops=flops, bytes_accessed=1000000, transcendentals=0),
        compiler_params=pltpu.CompilerParams(vmem_limit_bytes=16 * 1024 * 1024),
    )(*ins)


def swaps(axis, first, second):
    count = lax.axis_size(axis)
    got = []
    for start, block in ((0, first), (1, second)):
        pairs = []
        for low in range(start, count - 1, 2):
            pairs += [(low, low + 1), (low + 1, low)]
        got.append(lax.ppermute(block, axis, pairs))
    return got


def on_device(
    velocity,
    stress,
    lame_first,
    modulus,
    buoyancy,
    zone,
    eligible,
    cohesion,
    friction,
    source_cell,
    source_moment,
):
    shape = Shape(*zone.shape)
    rows_x, rows_y, depth = zone.shape
    whole_s, whole_v = vmem((6, shape.rows, depth)), vmem((3, shape.rows, depth))
    whole_b = vmem((shape.rows, depth))
    stress_rows = max(len(entries(LOW_Y)), len(entries(HIGH_Y)))
    all_rows = stress_rows + 5 + 2
    stress_slots = max(x_slots(LOW_X, rows_y, True), x_slots(HIGH_X, rows_y, True))
    flow_slots = (max(x_slots(LOW_FLOW_X, rows_y, False), x_slots(HIGH_FLOW_X, rows_y, False))
                  + 2 * (rows_y // 8))

    def buffers(axis, first_round):
        if axis == "y":
            return vmem((all_rows if first_round else stress_rows, rows_x, depth))
        return vmem((stress_slots + (flow_slots if first_round else 0), 8, depth))

    inner = (2, rows_x - 2)
    deep = (4, rows_x - 4)
    bands = range(0, rows_y, 8)

    def load(v_in, s_in, b_in, s, v, b, first, second, sems):
        own = [own_cells(shape, ref) for ref in (s, v, b)]
        run_copies(list(zip((s_in, v_in, b_in), own)), sems)
        send_y(shape, s, v, b, first, second)

    s, v, b, first, second = call(
        load,
        [velocity, stress, buoyancy],
        [in_hbm] * 3,
        [whole_s, whole_v, whole_b, buffers("y", True), buffers("y", True)],
        [in_vmem] * 5,
        "load",
        1000000,
        scratch=[pltpu.SemaphoreType.DMA((3,))],
    )

    def across(s, v, b):
        lanes = Lanes(depth)

        def layer(x):
            for t in bands:
                push_velocity(shape, lanes, s, v, b, aligned(shape, x, t), "xz")

        layers(*inner, layer, 4)

    def prepare(
        v_in, s, b, lame_in, shear_in, zone_in, able_in, cohesion, friction, v, rock, zones, able, sems
    ):
        flat = rock.reshape(5, rows_x, rows_y, depth)
        pairs = ((zone_in, zones), (able_in, able), (lame_in, flat.at[0]), (shear_in, flat.at[1]))
        copies = [pltpu.make_async_copy(a, c, sems.at[i]) for i, (a, c) in enumerate(pairs)]
        for c in copies:
            c.start()
        across(s, v, b)
        for c in copies:
            c.wait()

        def layer(x):
            for t in bands:
                own = pl.multiple_of(x * rows_y + t, 8)
                which = zones[x, pl.ds(t, 8), :]
                hold = jnp.full((8, depth), cohesion[0], jnp.float32)
                rub = jnp.full((8, depth), friction[0], jnp.float32)
                for k in range(1, cohesion.shape[0]):
                    hit = which == k
                    hold = jnp.where(hit, cohesion[k], hold)
                    rub = jnp.where(hit, friction[k], rub)
                rock[2, pl.ds(own, 8), :] = hold * jnp.sqrt(1.0 - rub * rub)
                rock[3, pl.ds(own, 8), :] = rub
                rock[4, pl.ds(own, 8), :] = jnp.where(able[x, pl.ds(t, 8), :] == 1, 1.0, 0.0)

        layers(0, rows_x, layer, 4)

    def plain(v_in, s, b, v):
        across(s, v, b)

    def middle(s, v, b, rock, cell, moment):
        lanes = Lanes(depth)

        def layer(x):
            for t in bands:
                push_velocity(shape, lanes, s, v, b, aligned(shape, x, t), "y")
            push_velocity(shape, lanes, s, v, b, aligned(shape, x, -RIM), "xyz")

        for t in bands:
            push_velocity(shape, lanes, s, v, b, aligned(shape, inner[0], t), "y")
        layers(inner[0] + 1, inner[1], layer, 4)
        inject(shape, s, cell, moment, lambda x: (x >= deep[0]) & (x < deep[1]))
        layers(*deep, lambda x: push_stress(shape, lanes, s, v, rock, x), 4)

    def outer(s, v, b, rock, cell, moment, ready=None):
        lanes = Lanes(depth)
        for low in (-2, inner[1]):
            for x in range(low, low + 4):
                for t in bands:
                    push_velocity(shape, lanes, s, v, b, aligned(shape, x, t), "xyz")
        for low in (0, inner[1]):
            for x in range(low, low + 3):
                push_velocity(shape, lanes, s, v, b, aligned(shape, x, -RIM), "xyz")
        if ready is not None:
            ready()
        rows = lambda x: (x >= 0) & (x < rows_x) & ((x < deep[0]) | (x >= deep[1]))
        inject(shape, s, cell, moment, rows)
        for low in (0, deep[1]):
            for x in range(low, low + 4):
                push_stress(shape, lanes, s, v, rock, x)

    cells = [source_cell, source_moment]
    out_shapes = [
        pltpu.HBM(velocity.shape, jnp.float32),
        pltpu.HBM(stress.shape, jnp.float32),
    ]
    for step in range(STEPS):
        begin, end = step == 0, step == STEPS - 1
        first, second = swaps("gy", first, second)

        if begin:
            v, rock = call(
                prepare,
                [v, s, b, lame_first, modulus, zone, eligible, cohesion, friction],
                [in_vmem] * 3 + [in_hbm] * 4 + [in_smem] * 2,
                [whole_v, vmem((5, rows_x * rows_y, depth))],
                [in_vmem] * 2,
                "prepare",
                10000000,
                aliases={0: 0},
                scratch=[
                    pltpu.VMEM((rows_x, rows_y, depth), jnp.int32),
                    pltpu.VMEM((rows_x, rows_y, depth), jnp.int32),
                    pltpu.SemaphoreType.DMA((4,)),
                ],
            )

            def turn(s_in, v_in, b_in, got_a, got_b, s, v, b, out_a, out_b):
                receive_y(shape, s, v, b, got_a, got_b)
                send_x(shape, s, v, b, out_a, out_b)

            s, v, b, first, second = call(
                turn,
                [s, v, b, first, second],
                [in_vmem] * 5,
                [whole_s, whole_v, whole_b, buffers("x", True), buffers("x", True)],
                [in_vmem] * 5,
                "turn_first",
                1000000,
                aliases={0: 0, 1: 1, 2: 2},
            )
        else:
            v = call(plain, [v, s, b], [in_vmem] * 3, whole_v, in_vmem, "plain", 10000000, {0: 0})

            def turn(s_in, got_a, got_b, s, out_a, out_b):
                receive_y(shape, s, None, None, got_a, got_b)
                send_x(shape, s, None, None, out_a, out_b)

            s, first, second = call(
                turn,
                [s, first, second],
                [in_vmem] * 3,
                [whole_s, buffers("x", False), buffers("x", False)],
                [in_vmem] * 3,
                "turn",
                1000000,
                aliases={0: 0},
            )
        first, second = swaps("gx", first, second)

        if not end:

            def interior(s_in, v_in, b, rock, cell, moment, s, v):
                middle(s, v, b, rock, cell, moment)

            s, v = call(
                interior,
                [s, v, b, rock] + cells,
                [in_vmem] * 4 + [in_smem] * 2,
                [whole_s, whole_v],
                [in_vmem] * 2,
                "interior",
                10000000,
                aliases={0: 0, 1: 1},
            )

            def border(s_in, v_in, b_in, rock, got_a, got_b, cell, moment, s, v, b, out_a, out_b):
                receive_x(shape, *((s, v, b) if begin else (s, None, None)), got_a, got_b)
                outer(s, v, b, rock, cell, moment)
                send_y(shape, s, None, None, out_a, out_b)

            s, v, b, first, second = call(
                border,
                [s, v, b, rock, first, second] + cells,
                [in_vmem] * 6 + [in_smem] * 2,
                [whole_s, whole_v, whole_b, buffers("y", False), buffers("y", False)],
                [in_vmem] * 5,
                "border",
                10000000,
                aliases={0: 0, 1: 1, 2: 2},
            )
        else:

            def interior(s_in, v_in, b, rock, cell, moment, s, v, v_out, s_out, sems):
                middle(s, v, b, rock, cell, moment)
                pairs = []
                for ref, out, (low, high) in ((v, v_out, inner), (s, s_out, deep)):
                    part = out.at[:, pl.ds(low, high - low)]
                    pairs.append((own_cells(shape, ref, low, high - low), part))
                run_copies(pairs, sems)

            s, v, v_out, s_out = call(
                interior,
                [s, v, b, rock] + cells,
                [in_vmem] * 4 + [in_smem] * 2,
                [whole_s, whole_v] + out_shapes,
                [in_vmem] * 2 + [in_hbm] * 2,
                "interior_last",
                10000000,
                aliases={0: 0, 1: 1},
                scratch=[pltpu.SemaphoreType.DMA((2,))],
            )

            def border(
                s_in, v_in, b, rock, got_a, got_b, cell, moment, v_old, s_old, s, v, v_out, s_out, sems
            ):
                def copies(ref, out, low, high, at):
                    spans = ((0, low), (high, rows_x - high))
                    return [
                        pltpu.make_async_copy(
                            own_cells(shape, ref, x, n), out.at[:, pl.ds(x, n)], sems.at[at + i]
                        )
                        for i, (x, n) in enumerate(spans)
                    ]

                v_copies = copies(v, v_out, *inner, 0)
                s_copies = copies(s, s_out, *deep, 2)
                receive_x(shape, s, None, None, got_a, got_b)
                outer(s, v, b, rock, cell, moment, lambda: [c.start() for c in v_copies])
                for c in s_copies:
                    c.start()
                for c in v_copies + s_copies:
                    c.wait()

            _, _, velocity, stress = call(
                border,
                [s, v, b, rock, first, second] + cells + [v_out, s_out],
                [in_vmem] * 6 + [in_smem] * 2 + [in_hbm] * 2,
                [whole_s, whole_v] + out_shapes,
                [in_vmem, in_vmem, in_hbm, in_hbm],
                "border_last",
                10000000,
                aliases={0: 0, 1: 1, 8: 2, 9: 3},
                scratch=[pltpu.SemaphoreType.DMA((4,))],
            )
    return (velocity, stress)


def solution(mesh):
    placed = (
        P(None, "gx", "gy", None),
        P(None, "gx", "gy", None),
        P("gx", "gy", None),
        P("gx", "gy", None),
        P("gx", "gy", None),
        P("gx", "gy", None),
        P("gx", "gy", None),
        P(),
        P(),
        P(),
        P(),
    )
    return jax.shard_map(
        on_device,
        mesh=mesh,
        in_specs=placed,
        out_specs=(P(None, "gx", "gy", None), P(None, "gx", "gy", None)),
        check_vma=False,
    )
```

```python
import jax
import jax.numpy as jnp
from jax import lax
from jax.experimental import pallas as pl
from jax.experimental.pallas import tpu as pltpu
from jax.sharding import PartitionSpec as P

STEPS = 2

time_step = 0.1
near_weight = 9.0 / 8.0
far_weight = 1.0 / 24.0
shear_floor = 0.25

XX, YY, ZZ, XY, XZ, YZ = range(6)

LOW_Y = ((XY, 2), (YY, 1), (YZ, 2))
HIGH_Y = ((XY, 1), (YY, 2), (YZ, 1))
LOW_X = ((XX, 1), (XY, 2), (XZ, 2))
HIGH_X = ((XX, 2), (XY, 1), (XZ, 1))
LOW_FLOW_Y = ((0, 1), (1, 2), (2, 1))
HIGH_FLOW_Y = ((0, 2), (1, 1), (2, 2))
LOW_FLOW_X = ((0, 2), (1, 1), (2, 1))
HIGH_FLOW_X = ((0, 1), (1, 2), (2, 2))
DRIVES = (XX, XY, XZ)

PAD_X = 4
RIM = 8


class Shape:
    def __init__(self, rows_x, rows_y, depth):
        self.rows_x, self.rows_y, self.depth = rows_x, rows_y, depth
        self.pitch = rows_y + RIM
        self.rows = (rows_x + 2 * PAD_X + 1) * self.pitch

    def row(self, x, y):
        return (x + PAD_X) * self.pitch + RIM + y


def entries(spec):
    return [(c, k) for c, depth in spec for k in range(depth)]


def pack_y(shape, pairs, out):
    for slot, (ref, y) in enumerate(pairs):
        for x in range(0, shape.rows_x, 8):
            out[slot, pl.ds(x, 8), :] = ref[pl.ds(shape.row(x, y), 8, stride=shape.pitch), :]


def unpack_y(shape, pairs, got):
    for slot, (ref, y) in enumerate(pairs):
        for x in range(0, shape.rows_x, 8):
            ref[pl.ds(shape.row(x, y), 8, stride=shape.pitch), :] = got[slot, pl.ds(x, 8), :]


def y_list(fields, spec, flow_spec, place):
    halo, flow, buoyancy = fields
    pairs = [(halo[c], place(k)) for c, k in entries(spec)]
    pairs += [(flow.at[c], place(k)) for c, k in entries(flow_spec)]
    if buoyancy is not None:
        pairs += [(buoyancy, place(k)) for k in range(2)]
    return pairs


def edge_layers(shape):
    return (0, 1, shape.rows_x - 2, shape.rows_x - 1)


def pack_corner(shape, stress, flow_spec, place, out):
    for i, x in enumerate(edge_layers(shape)):
        for j, (c, k) in enumerate(entries(flow_spec)):
            row = shape.row(x, place(k))
            out[pl.ds(8 * i + j, 1), :] = stress[DRIVES[c], pl.ds(row, 1), :]


def by_parity(axis, body, first, second):
    odd = lax.axis_index(axis) % 2

    @pl.when(odd == 0)
    def _():
        body(second, first)

    @pl.when(odd == 1)
    def _():
        body(first, second)


def send_y(shape, stress, flow, buoyancy, first, second):
    fields = ({c: stress.at[c] for c in range(6)}, flow, buoyancy)
    top = lambda k: shape.rows_y - 1 - k
    bottom = lambda k: k

    def body(below, above):
        last = above.shape[0] - 1
        pack_y(shape, y_list(fields, LOW_Y, LOW_FLOW_Y, top), above)
        pack_corner(shape, stress, LOW_FLOW_Y, top, above.at[last])
        pack_y(shape, y_list(fields, HIGH_Y, HIGH_FLOW_Y, bottom), below)
        pack_corner(shape, stress, HIGH_FLOW_Y, bottom, below.at[last])

    by_parity("gy", body, first, second)


def receive_y(shape, halo, flow, buoyancy, first, second):
    fields = ({c: halo.at[i] for i, c in enumerate((XY, YY, YZ))}, flow, buoyancy)

    def body(below, above):
        unpack_y(shape, y_list(fields, LOW_Y, LOW_FLOW_Y, lambda k: -1 - k), below)
        unpack_y(shape, y_list(fields, HIGH_Y, HIGH_FLOW_Y, lambda k: shape.rows_y + k), above)

    by_parity("gy", body, first, second)


def x_count(shape, first_round):
    bands = shape.rows_y // 8
    most = max(
        len(entries(spec)) * (bands + 1) + len(entries(flow_spec)) * bands
        for spec, flow_spec in ((LOW_X, LOW_FLOW_X), (HIGH_X, HIGH_FLOW_X))
    )
    return most + (2 * bands if first_round else 0)


def y_count(first_round):
    most = max(
        len(entries(spec)) + len(entries(flow_spec))
        for spec, flow_spec in ((LOW_Y, LOW_FLOW_Y), (HIGH_Y, HIGH_FLOW_Y))
    )
    return most + 1 + (2 if first_round else 0)


def x_slots(shape, spec, flow_spec, first_round):
    bands = range(0, shape.rows_y, 8)
    keys = [("s", c, k, t) for c, k in entries(spec) for t in bands]
    keys += [("v", c, k, t) for c, k in entries(flow_spec) for t in bands]
    keys += [("rim", c, k) for c, k in entries(spec)]
    if first_round:
        keys += [("b", 0, k, t) for k in range(2) for t in bands]
    return {key: i for i, key in enumerate(keys)}


def send_x(shape, stress, flow, buoyancy, got_first, got_second, first, second):
    arrays = {"s": stress, "v": flow, "b": buoyancy}
    layer_at = {x: i for i, x in enumerate(edge_layers(shape))}

    def with_corners(got_below, got_above):
        def fill(out, spec, flow_spec, place):
            slots = x_slots(shape, spec, flow_spec, buoyancy is not None)
            for (kind, c, k, *t), slot in slots.items():
                if kind == "rim":
                    for got, rims, at in (
                        (got_above, HIGH_FLOW_Y, lambda d: d),
                        (got_below, LOW_FLOW_Y, lambda d: 7 - d),
                    ):
                        for j, (which, depth) in enumerate(entries(rims)):
                            if DRIVES[which] == c:
                                row = 8 * layer_at[place(k)] + j
                                corner = got[got.shape[0] - 1, pl.ds(row, 1), :]
                                out[slot, pl.ds(at(depth), 1), :] = corner
                else:
                    ref = arrays[kind] if kind == "b" else arrays[kind].at[c]
                    out[slot] = tile(ref, shape.row(place(k), t[0]))

        def body(below, above):
            fill(above, LOW_X, LOW_FLOW_X, lambda k: shape.rows_x - 1 - k)
            fill(below, HIGH_X, HIGH_FLOW_X, lambda k: k)

        by_parity("gx", body, first, second)

    by_parity("gy", with_corners, got_first, got_second)


NEAR, FAR = near_weight, far_weight
UP = {1: NEAR, 0: -NEAR, 2: -FAR, -1: FAR}
DOWN = {0: NEAR, -1: -NEAR, 1: -FAR, -2: FAR}


def crossing(c, x, sources):
    total = None
    for step, weight in (UP if c == 0 else DOWN).items():
        if x + step in sources:
            term = weight * sources[x + step]()
            total = term if total is None else total + term
    return total


def receive_x(shape, stress, flow, buoyancy, first_round, first, second):
    rows_x = shape.rows_x
    sub = lax.broadcasted_iota(jnp.int32, (8, shape.depth), 0)

    def body(below, above):
        sides = (
            (below, x_slots(shape, LOW_X, LOW_FLOW_X, first_round), lambda k: -1 - k),
            (above, x_slots(shape, HIGH_X, HIGH_FLOW_X, first_round), lambda k: rows_x + k),
        )
        came = {}
        for got, slots, place in sides:
            for (kind, c, k, *t), slot in slots.items():
                if kind == "b":
                    buoyancy[pl.ds(shape.row(place(k), t[0]), 8), :] = got[slot]
                else:
                    came[(kind, c, place(k), *t)] = (got, slot)

        def arrived(kind, c, *t):
            return {
                key[2]: (lambda got=got, slot=slot: got[slot])
                for key, (got, slot) in came.items()
                if key[:2] == (kind, c) and key[3:] == t
            }

        for t in range(0, shape.rows_y, 8):
            for c in range(3):
                halo = arrived("s", DRIVES[c], t)
                own = {
                    x: (lambda x=x: tile(stress.at[DRIVES[c]], shape.row(x, t)))
                    for x in edge_layers(shape)
                }
                rim = arrived("v", c, t)
                for x in edge_layers(shape):
                    force = crossing(c, x, halo)
                    if force is not None:
                        row = shape.row(x, t)
                        flow[c, pl.ds(row, 8), :] += time_step * tile(buoyancy, row) * force
                for x, value in rim.items():
                    row = shape.row(x, t)
                    force = crossing(c, x, own)
                    flow[c, pl.ds(row, 8), :] = value() + time_step * tile(buoyancy, row) * force
        for c in range(3):
            halo = arrived("rim", DRIVES[c])
            forces = {x: crossing(c, x, halo) for x in edge_layers(shape)}
            for x in sorted({x + d for x in edge_layers(shape) for d in (0, 1)}):
                high, low = forces.get(x - 1), forces.get(x)
                if high is None and low is None:
                    continue
                zero = jnp.zeros((8, shape.depth), jnp.float32)
                force = jnp.where(
                    sub < 4, zero if high is None else high, zero if low is None else low
                )
                row = shape.row(x, -RIM)
                flow[c, pl.ds(row, 8), :] += time_step * tile(buoyancy, row) * force

    by_parity("gx", body, first, second)


class Lanes:
    def __init__(self, depth):
        self.depth = depth
        lane = lax.broadcasted_iota(jnp.int32, (8, depth), 1)
        zero = jnp.zeros((8, depth), jnp.float32)
        near = jnp.full((8, depth), near_weight, jnp.float32)
        far = jnp.full((8, depth), far_weight, jnp.float32)
        self.f_up = jnp.where(lane < depth - 1, near, zero)
        self.f_up2 = jnp.where(lane < depth - 2, far, zero)
        self.f_down = jnp.where(lane > 0, far, zero)
        self.b_down = jnp.where(lane > 0, near, zero)
        self.b_down2 = jnp.where(lane > 1, far, zero)
        self.b_up = jnp.where(lane < depth - 1, far, zero)

    def forward(self, f):
        up, up2, down = (pltpu.roll(f, s % self.depth, 1) for s in (-1, -2, 1))
        return (self.f_up * up - near_weight * f) - (self.f_up2 * up2 - self.f_down * down)

    def backward(self, f):
        up, down, down2 = (pltpu.roll(f, s % self.depth, 1) for s in (-1, 1, 2))
        return (near_weight * f - self.b_down * down) - (self.b_up * up - self.b_down2 * down2)


def forward(ref, row, step):
    a, b, c, d = (ref[pl.ds(row + k * step, 8), :] for k in (-1, 0, 1, 2))
    return near_weight * (c - b) - far_weight * (d - a)


def backward(ref, row, step):
    a, b, c, d = (ref[pl.ds(row + k * step, 8), :] for k in (-2, -1, 0, 1))
    return near_weight * (c - b) - far_weight * (d - a)


def tile(ref, row):
    return ref[pl.ds(row, 8), :]


def push_velocity(shape, lanes, stress, flow, buoyancy, row, along="xyz"):
    sx, sy = shape.pitch, 1
    xx, yy, zz, xy, xz, yz = (stress.at[c] for c in range(6))
    parts = {
        "x": lambda: (forward(xx, row, sx), backward(xy, row, sx), backward(xz, row, sx)),
        "y": lambda: (backward(xy, row, sy), forward(yy, row, sy), backward(yz, row, sy)),
        "z": lambda: (
            lanes.backward(tile(xz, row)),
            lanes.backward(tile(yz, row)),
            lanes.forward(tile(zz, row)),
        ),
    }
    force = parts[along[0]]()
    for axis in along[1:]:
        force = [f + g for f, g in zip(force, parts[axis]())]
    scale = time_step * tile(buoyancy, row)
    for c in range(3):
        flow[c, pl.ds(row, 8), :] += scale * force[c]


def push_across_y(halves, flow, buoyancy, row):
    xy, yy, yz = halves
    force = (backward(xy, row, 1), forward(yy, row, 1), backward(yz, row, 1))
    scale = time_step * tile(buoyancy, row)
    for c in range(3):
        flow[c, pl.ds(row, 8), :] += scale * force[c]


def layers(first, stop, body, unroll):
    def run(x, carry):
        body(x)
        return carry

    lax.fori_loop(first, stop, run, 0, unroll=unroll)


def aligned(shape, x, y):
    return pl.multiple_of((x + PAD_X) * shape.pitch + RIM + y, 8)


def inject(shape, stress, source_cell, source_moment, wanted):
    rows_x, rows_y, depth = shape.rows_x, shape.rows_y, shape.depth
    total_y = rows_y * lax.axis_size("gy")
    start_x = lax.axis_index("gx") * rows_x
    start_y = lax.axis_index("gy") * rows_y
    sub = lax.broadcasted_iota(jnp.int32, (8, depth), 0)
    lane = lax.broadcasted_iota(jnp.int32, (8, depth), 1)
    for s in range(source_cell.shape[0]):
        cell = source_cell[s]
        line = lax.div(cell, depth)
        x = lax.div(line, total_y) - start_x
        y = lax.rem(line, total_y) - start_y
        z = lax.rem(cell, depth)

        @pl.when(wanted(x) & (y >= 0) & (y < rows_y))
        def _(x=x, y=y, z=z, s=s):
            band = lax.div(y, 8) * 8
            row = aligned(shape, x, band)
            here = (sub == y - band) & (lane == z)
            for c in range(6):
                amount = time_step * source_moment[c, s]
                stress[c, pl.ds(row, 8), :] += jnp.where(here, amount, 0.0)


def push_stress(shape, lanes, stress, flow, rock, x):
    sx, sy = shape.pitch, 1
    vx, vy, vz = (flow.at[c] for c in range(3))

    for t in range(0, shape.rows_y, 8):
        row = aligned(shape, x, t)
        own = pl.multiple_of(x * shape.rows_y + t, 8)
        first = time_step * rock[0, pl.ds(own, 8), :]
        shear = time_step * rock[1, pl.ds(own, 8), :]
        strain_x = backward(vx, row, sx)
        strain_y = backward(vy, row, sy)
        here_z = tile(vz, row)
        strain_z = lanes.backward(here_z)
        volume = first * (strain_x + strain_y + strain_z)
        twice = 2.0 * shear
        xx = tile(stress.at[XX], row) + (volume + twice * strain_x)
        yy = tile(stress.at[YY], row) + (volume + twice * strain_y)
        zz = tile(stress.at[ZZ], row) + (volume + twice * strain_z)
        xy = tile(stress.at[XY], row) + shear * (forward(vx, row, sy) + forward(vy, row, sx))
        xz = tile(stress.at[XZ], row) + shear * (
            lanes.forward(tile(vx, row)) + forward(vz, row, sx)
        )
        yz = tile(stress.at[YZ], row) + shear * (
            lanes.forward(tile(vy, row)) + forward(vz, row, sy)
        )
        pressure = (xx + yy + zz) * (1.0 / 3.0)
        dx, dy, dz = xx - pressure, yy - pressure, zz - pressure
        second = 0.5 * (dx * dx + dy * dy + dz * dz) + xy * xy + xz * xz + yz * yz
        strength = jnp.maximum(
            rock[2, pl.ds(own, 8), :] - pressure * rock[3, pl.ds(own, 8), :], 0.0
        )
        ratio = strength * lax.rsqrt(jnp.maximum(second, shear_floor * shear_floor))
        factor = jnp.where(rock[4, pl.ds(own, 8), :] > 0.5, jnp.minimum(ratio, 1.0), 1.0)
        stress[XX, pl.ds(row, 8), :] = pressure + factor * dx
        stress[YY, pl.ds(row, 8), :] = pressure + factor * dy
        stress[ZZ, pl.ds(row, 8), :] = pressure + factor * dz
        stress[XY, pl.ds(row, 8), :] = factor * xy
        stress[XZ, pl.ds(row, 8), :] = factor * xz
        stress[YZ, pl.ds(row, 8), :] = factor * yz


def own_cells(shape, ref, first=0, count=None):
    lead = ref.shape[:-2]
    view = ref.reshape(*lead, shape.rows_x + 2 * PAD_X + 1, shape.pitch, shape.depth)
    count = shape.rows_x - first if count is None else count
    return view.at[
        (slice(None),) * len(lead) + (pl.ds(PAD_X + first, count), pl.ds(RIM, shape.rows_y))
    ]


def run_copies(pairs, sems):
    copies = [pltpu.make_async_copy(a, b, sems.at[i]) for i, (a, b) in enumerate(pairs)]
    for c in copies:
        c.start()
    for c in copies:
        c.wait()


def vmem(shape):
    return pltpu.VMEM(shape, jnp.float32)


in_vmem = pl.BlockSpec(memory_space=pltpu.VMEM)
in_smem = pl.BlockSpec(memory_space=pltpu.SMEM)
in_hbm = pl.BlockSpec(memory_space=pltpu.HBM)


def call(body, ins, in_specs, out_shape, out_specs, name, flops, aliases=None, scratch=()):
    space = {id(in_vmem): pltpu.VMEM, id(in_hbm): pltpu.HBM}
    ins = [
        pltpu.with_memory_space_constraint(x, space[id(s)]) if id(s) in space else x
        for x, s in zip(ins, in_specs)
    ]
    return pl.pallas_call(
        body,
        in_specs=in_specs,
        out_shape=out_shape,
        out_specs=out_specs,
        input_output_aliases=aliases or {},
        scratch_shapes=scratch,
        name=name,
        cost_estimate=pl.CostEstimate(flops=flops, bytes_accessed=1000000, transcendentals=0),
        compiler_params=pltpu.CompilerParams(vmem_limit_bytes=16 * 1024 * 1024),
    )(*ins)


def swaps(axis, first, second):
    count = lax.axis_size(axis)
    got = []
    for start, block in ((0, first), (1, second)):
        pairs = []
        for low in range(start, count - 1, 2):
            pairs += [(low, low + 1), (low + 1, low)]
        got.append(lax.ppermute(block, axis, pairs))
    return got


def on_device(
    velocity,
    stress,
    lame_first,
    modulus,
    buoyancy,
    zone,
    eligible,
    cohesion,
    friction,
    source_cell,
    source_moment,
):
    shape = Shape(*zone.shape)
    rows_x, rows_y, depth = zone.shape
    whole_s, whole_v = vmem((6, shape.rows, depth)), vmem((3, shape.rows, depth))
    whole_b, whole_h = vmem((shape.rows, depth)), vmem((3, shape.rows, depth))
    y_buffers = {first: vmem((y_count(first), rows_x, depth)) for first in (True, False)}
    x_buffers = {first: vmem((x_count(shape, first), 8, depth)) for first in (True, False)}

    inner = (2, rows_x - 2)
    deep = (4, rows_x - 4)
    next_inner = (6, rows_x - 6)
    bands = range(0, rows_y, 8)

    def own_forces(lanes, s, v, b, x):
        for t in bands:
            push_velocity(shape, lanes, s, v, b, aligned(shape, x, t))

    def load(v_in, s_in, b_in, s, v, b, h, first, second, sems):
        groups = []
        for g, x in enumerate(range(0, rows_x, 8)):
            group = []
            for i, (source, ref) in enumerate(((s_in, s), (v_in, v), (b_in, b))):
                part = source.at[:, pl.ds(x, 8)] if i < 2 else source.at[pl.ds(x, 8)]
                place = own_cells(shape, ref, x, 8)
                group.append(pltpu.make_async_copy(part, place, sems.at[g, i]))
                group[-1].start()
            groups.append(group)
        zero = jnp.zeros((8, depth), jnp.float32)
        for x in range(0, rows_x + 1):
            for c in (XY, YY, YZ):
                s[c, pl.ds(shape.row(x, -RIM), 8), :] = zero
        for x in range(0, rows_x):
            for t in bands:
                for c in range(3):
                    h[c, pl.ds(shape.row(x, t), 8), :] = zero
        for x in (-2, -1, rows_x, rows_x + 1):
            for t in bands:
                for c in range(6):
                    s[c, pl.ds(shape.row(x, t), 8), :] = zero
        lanes = Lanes(depth)
        done = 0
        for g, group in enumerate(groups):
            for copy in group:
                copy.wait()
            stop = rows_x if g == len(groups) - 1 else 8 * g + 6
            layers(done, stop, lambda x: own_forces(lanes, s, v, b, x), stop - done)
            done = stop
        send_y(shape, s, v, b, first, second)

    s, v, b, h, first, second = call(
        load,
        [velocity, stress, buoyancy],
        [in_hbm] * 3,
        [whole_s, whole_v, whole_b, whole_h, y_buffers[True], y_buffers[True]],
        [in_vmem] * 6,
        "load",
        10000000,
        scratch=[pltpu.SemaphoreType.DMA((rows_x // 8, 3))],
    )

    def prepare(after, lame_in, shear_in, zone_in, able_in, cohesion, friction, rock, zones, able, sems):
        flat = rock.reshape(5, rows_x, rows_y, depth)
        pairs = ((zone_in, zones), (able_in, able), (lame_in, flat.at[0]), (shear_in, flat.at[1]))
        run_copies(pairs, sems)

        def layer(x):
            for t in bands:
                own = pl.multiple_of(x * rows_y + t, 8)
                which = zones[x, pl.ds(t, 8), :]
                hold = jnp.full((8, depth), cohesion[0], jnp.float32)
                rub = jnp.full((8, depth), friction[0], jnp.float32)
                for k in range(1, cohesion.shape[0]):
                    hit = which == k
                    hold = jnp.where(hit, cohesion[k], hold)
                    rub = jnp.where(hit, friction[k], rub)
                rock[2, pl.ds(own, 8), :] = hold * jnp.sqrt(1.0 - rub * rub)
                rock[3, pl.ds(own, 8), :] = rub
                rock[4, pl.ds(own, 8), :] = jnp.where(able[x, pl.ds(t, 8), :] == 1, 1.0, 0.0)

        layers(0, rows_x, layer, 4)

    rock = call(
        prepare,
        [b, lame_first, modulus, zone, eligible, cohesion, friction],
        [in_vmem] + [in_hbm] * 4 + [in_smem] * 2,
        vmem((5, rows_x * rows_y, depth)),
        in_vmem,
        "prepare",
        10000000,
        scratch=[
            pltpu.VMEM((rows_x, rows_y, depth), jnp.int32),
            pltpu.VMEM((rows_x, rows_y, depth), jnp.int32),
            pltpu.SemaphoreType.DMA((4,)),
        ],
    )

    def middle(s, v, b, h, rock, cell, moment):
        lanes = Lanes(depth)
        halves = [h.at[c] for c in range(3)]
        own = [s.at[c] for c in (XY, YY, YZ)]

        def layer(x):
            for t in bands:
                push_across_y(halves, v, b, aligned(shape, x, t))

        layers(*inner, layer, 4)
        layers(0, rows_x + 1, lambda x: push_across_y(own, v, b, aligned(shape, x, -RIM)), 3)
        inject(shape, s, cell, moment, lambda x: (x >= deep[0]) & (x < deep[1]))
        layers(*deep, lambda x: push_stress(shape, lanes, s, v, rock, x), 4)

    def outer(s, v, b, rock, cell, moment):
        lanes = Lanes(depth)
        rows = lambda x: (x >= 0) & (x < rows_x) & ((x < deep[0]) | (x >= deep[1]))
        inject(shape, s, cell, moment, rows)
        for low in (0, deep[1]):
            for x in range(low, low + 4):
                push_stress(shape, lanes, s, v, rock, x)

    cells = [source_cell, source_moment]
    out_shapes = [
        pltpu.HBM(velocity.shape, jnp.float32),
        pltpu.HBM(stress.shape, jnp.float32),
    ]
    for step in range(STEPS):
        begin, end = step == 0, step == STEPS - 1
        first, second = swaps("gy", first, second)

        if begin:

            def turn(s, v_in, b_in, h_in, got_a, got_b, v, b, h, out_a, out_b):
                receive_y(shape, h, v, b, got_a, got_b)
                for x in edge_layers(shape):
                    for t in bands:
                        push_across_y([h.at[c] for c in range(3)], v, b, shape.row(x, t))
                send_x(shape, s, v, b, got_a, got_b, out_a, out_b)

            v, b, h, first, second = call(
                turn,
                [s, v, b, h, first, second],
                [in_vmem] * 6,
                [whole_v, whole_b, whole_h, x_buffers[True], x_buffers[True]],
                [in_vmem] * 5,
                "turn_first",
                1000000,
                aliases={1: 0, 2: 1, 3: 2},
            )
        else:

            def turn(s, v_in, b, h_in, got_a, got_b, v, h, out_a, out_b):
                receive_y(shape, h, v, None, got_a, got_b)
                for x in edge_layers(shape):
                    for t in bands:
                        push_across_y([h.at[c] for c in range(3)], v, b, shape.row(x, t))
                send_x(shape, s, v, None, got_a, got_b, out_a, out_b)

            v, h, first, second = call(
                turn,
                [s, v, b, h, first, second],
                [in_vmem] * 6,
                [whole_v, whole_h, x_buffers[False], x_buffers[False]],
                [in_vmem] * 4,
                "turn",
                1000000,
                aliases={1: 0, 3: 1},
            )
        first, second = swaps("gx", first, second)

        if not end:

            def interior(s_in, v_in, b, h, rock, cell, moment, s, v):
                middle(s, v, b, h, rock, cell, moment)
                lanes = Lanes(depth)
                layers(*next_inner, lambda x: own_forces(lanes, s, v, b, x), 4)

            s, v = call(
                interior,
                [s, v, b, h, rock] + cells,
                [in_vmem] * 5 + [in_smem] * 2,
                [whole_s, whole_v],
                [in_vmem] * 2,
                "interior",
                10000000,
                aliases={0: 0, 1: 1},
            )

            def border(s_in, v_in, b_in, rock, got_a, got_b, cell, moment, s, v, b, out_a, out_b):
                receive_x(shape, s, v, b, begin, got_a, got_b)
                outer(s, v, b, rock, cell, moment)
                lanes = Lanes(depth)
                for low in (0, next_inner[1]):
                    for x in range(low, low + next_inner[0]):
                        own_forces(lanes, s, v, b, x)
                send_y(shape, s, v, None, out_a, out_b)

            s, v, b, first, second = call(
                border,
                [s, v, b, rock, first, second] + cells,
                [in_vmem] * 6 + [in_smem] * 2,
                [whole_s, whole_v, whole_b, y_buffers[False], y_buffers[False]],
                [in_vmem] * 5,
                "border",
                10000000,
                aliases={0: 0, 1: 1, 2: 2},
            )
        else:

            def interior(s_in, v_in, b, h, rock, cell, moment, s, v, v_out, s_out, sems):
                middle(s, v, b, h, rock, cell, moment)
                pairs = []
                for ref, out, (low, high) in ((v, v_out, inner), (s, s_out, deep)):
                    part = out.at[:, pl.ds(low, high - low)]
                    pairs.append((own_cells(shape, ref, low, high - low), part))
                run_copies(pairs, sems)

            s, v, v_out, s_out = call(
                interior,
                [s, v, b, h, rock] + cells,
                [in_vmem] * 5 + [in_smem] * 2,
                [whole_s, whole_v] + out_shapes,
                [in_vmem] * 2 + [in_hbm] * 2,
                "interior_last",
                10000000,
                aliases={0: 0, 1: 1},
                scratch=[pltpu.SemaphoreType.DMA((2,))],
            )

            def border(
                s_in, v_in, b, rock, got_a, got_b, cell, moment, v_old, s_old, s, v, v_out, s_out, sems
            ):
                def copies(ref, out, low, high, at):
                    spans = ((0, low), (high, rows_x - high))
                    return [
                        pltpu.make_async_copy(
                            own_cells(shape, ref, x, n), out.at[:, pl.ds(x, n)], sems.at[at + i]
                        )
                        for i, (x, n) in enumerate(spans)
                    ]

                v_copies = copies(v, v_out, *inner, 0)
                s_copies = copies(s, s_out, *deep, 2)
                receive_x(shape, s, v, b, begin, got_a, got_b)
                for c in v_copies:
                    c.start()
                outer(s, v, b, rock, cell, moment)
                for c in s_copies:
                    c.start()
                for c in v_copies + s_copies:
                    c.wait()

            _, _, velocity, stress = call(
                border,
                [s, v, b, rock, first, second] + cells + [v_out, s_out],
                [in_vmem] * 6 + [in_smem] * 2 + [in_hbm] * 2,
                [whole_s, whole_v] + out_shapes,
                [in_vmem, in_vmem, in_hbm, in_hbm],
                "border_last",
                10000000,
                aliases={0: 0, 1: 1, 8: 2, 9: 3},
                scratch=[pltpu.SemaphoreType.DMA((4,))],
            )
    return (velocity, stress)


def solution(mesh):
    placed = (
        P(None, "gx", "gy", None),
        P(None, "gx", "gy", None),
        P("gx", "gy", None),
        P("gx", "gy", None),
        P("gx", "gy", None),
        P("gx", "gy", None),
        P("gx", "gy", None),
        P(),
        P(),
        P(),
        P(),
    )
    return jax.shard_map(
        on_device,
        mesh=mesh,
        in_specs=placed,
        out_specs=(P(None, "gx", "gy", None), P(None, "gx", "gy", None)),
        check_vma=False,
    )
```

```python
import jax
import jax.numpy as jnp
from jax import lax
from jax.experimental import pallas as pl
from jax.experimental.pallas import tpu as pltpu
from jax.sharding import PartitionSpec as P


time_step = 0.1
near_weight = 9.0 / 8.0
far_weight = 1.0 / 24.0
shear_floor = 0.25

XX, YY, ZZ, XY, XZ, YZ = range(6)

LOW_Y = ((XY, 2), (YY, 1), (YZ, 2))
HIGH_Y = ((XY, 1), (YY, 2), (YZ, 1))
LOW_X = ((XX, 1), (XY, 2), (XZ, 2))
HIGH_X = ((XX, 2), (XY, 1), (XZ, 1))
LOW_FLOW_Y = ((0, 1), (1, 2), (2, 1))
HIGH_FLOW_Y = ((0, 2), (1, 1), (2, 2))
BESIDE = 3
LOW_DEEP_X = ((0, 5), (1, 4), (2, 4))
HIGH_DEEP_X = ((0, 4), (1, 5), (2, 5))
DRIVES = (XX, XY, XZ)

PAD_X = 8
RIM = 8


class Shape:
    def __init__(self, rows_x, rows_y, depth):
        self.rows_x, self.rows_y, self.depth = rows_x, rows_y, depth
        self.pitch = rows_y + RIM
        self.rows = (rows_x + 2 * PAD_X + 1) * self.pitch

    def row(self, x, y):
        return (x + PAD_X) * self.pitch + RIM + y


def entries(spec):
    return [(c, k) for c, depth in spec for k in range(depth)]


def pack_y(shape, pairs, out):
    for slot, (ref, y) in enumerate(pairs):
        for x in range(0, shape.rows_x, 8):
            out[slot, pl.ds(x, 8), :] = ref[pl.ds(shape.row(x, y), 8, stride=shape.pitch), :]


def unpack_y(shape, pairs, got):
    for slot, (ref, y) in enumerate(pairs):
        for x in range(0, shape.rows_x, 8):
            ref[pl.ds(shape.row(x, y), 8, stride=shape.pitch), :] = got[slot, pl.ds(x, 8), :]


def y_list(fields, spec, flow_spec, place):
    halo, flow, buoyancy = fields
    pairs = [(halo[c], place(k)) for c, k in entries(spec)]
    pairs += [(flow.at[c], place(k)) for c, k in entries(flow_spec)]
    if buoyancy is not None:
        pairs += [(buoyancy, place(k)) for k in range(2)]
    return pairs


def edge_layers(shape):
    return (0, 1, shape.rows_x - 2, shape.rows_x - 1)


def beside_layers(shape):
    return (-2, -1, shape.rows_x, shape.rows_x + 1)


def pack_singles(shape, stress, layers_x, rows, out):
    for i, x in enumerate(layers_x):
        for j, (c, y) in enumerate(rows):
            out[pl.ds(8 * i + j, 1), :] = stress[c, pl.ds(shape.row(x, y), 1), :]


def by_parity(axis, body, *swapped):
    odd = lax.axis_index(axis) % 2

    @pl.when(odd == 0)
    def _():
        body(*[r for first, second in swapped for r in (second, first)])

    @pl.when(odd == 1)
    def _():
        body(*[r for first, second in swapped for r in (first, second)])


def send_y(shape, stress, flow, buoyancy, first, second):
    fields = ({c: stress.at[c] for c in range(6)}, flow, buoyancy)

    def fill(out, spec, flow_spec, place):
        pack_y(shape, y_list(fields, spec, flow_spec, place), out)
        if buoyancy is None:
            layers_x, rows = beside_layers(shape), [(c, place(k)) for c, k in entries(spec)]
        else:
            layers_x = edge_layers(shape)
            rows = [(DRIVES[c], place(k)) for c, k in entries(flow_spec)]
        pack_singles(shape, stress, layers_x, rows, out.at[out.shape[0] - 1])

    def body(below, above):
        fill(above, LOW_Y, LOW_FLOW_Y, lambda k: shape.rows_y - 1 - k)
        fill(below, HIGH_Y, HIGH_FLOW_Y, lambda k: k)

    by_parity("gy", body, (first, second))


def receive_y(shape, halo, flow, buoyancy, first, second):
    halves = {c: halo.at[i] for i, c in enumerate((XY, YY, YZ))}
    fields = (halves, flow, buoyancy)

    def take(got, spec, flow_spec, place):
        unpack_y(shape, y_list(fields, spec, flow_spec, place), got)
        if buoyancy is None:
            for i, x in enumerate(beside_layers(shape)):
                for j, (c, k) in enumerate(entries(spec)):
                    single = got[got.shape[0] - 1, pl.ds(8 * i + j, 1), :]
                    halves[c][pl.ds(shape.row(x, place(k)), 1), :] = single

    def body(below, above):
        take(below, LOW_Y, LOW_FLOW_Y, lambda k: -1 - k)
        take(above, HIGH_Y, HIGH_FLOW_Y, lambda k: shape.rows_y + k)

    by_parity("gy", body, (first, second))


def y_count(first_round):
    most = max(
        len(entries(spec)) + len(entries(flow_spec))
        for spec, flow_spec in ((LOW_Y, LOW_FLOW_Y), (HIGH_Y, HIGH_FLOW_Y))
    )
    return most + 1 + (2 if first_round else 0)


def x_slots(shape, side):
    spec, flow_spec = ((LOW_X, LOW_DEEP_X), (HIGH_X, HIGH_DEEP_X))[side]
    bands = range(0, shape.rows_y, 8)
    keys = [("v", c, k, t) for c, k in entries(flow_spec) for t in bands]
    keys += [("v", c, k, "rim") for c in range(3) for k in range(BESIDE)]
    keys += [("b", 0, k, "rim") for k in range(2)]
    keys += [("s", c, k, "rim") for c, k in entries(spec)]
    return {key: i for i, key in enumerate(keys)}


def x_count(shape):
    return max(len(x_slots(shape, side)) for side in (0, 1))


def early_slots(shape):
    bands = range(0, shape.rows_y, 8)
    keys = [("s", c, k, t) for c in range(6) for k in range(BESIDE) for t in bands]
    keys += [("r", c, k, t) for c in range(4) for k in range(BESIDE) for t in bands]
    keys += [("b", 0, k, t) for k in range(2) for t in bands]
    return {key: i for i, key in enumerate(keys)}


def send_early(shape, stress, buoyancy, raw, first, second):
    def fill(out, side, place):
        for (kind, c, k, t), slot in early_slots(shape).items():
            x = place(k)
            if kind == "r":
                at = x - (shape.rows_x - BESIDE if side == 0 else 0)
                out[slot] = raw(c, side, at, t)
            else:
                out[slot] = tile(stress.at[c] if kind == "s" else buoyancy, shape.row(x, t))

    def body(below, above):
        fill(above, 0, lambda k: shape.rows_x - 1 - k)
        fill(below, 1, lambda k: k)

    by_parity("gx", body, (first, second))


def receive_early(shape, stress, buoyancy, rock, cohesion, friction, first, second):
    slots = early_slots(shape)

    def take(got, place):
        for (kind, c, k, t), slot in slots.items():
            x = place(k)
            if kind == "s":
                stress[c, pl.ds(shape.row(x, t), 8), :] = got[slot]
            elif kind == "b":
                buoyancy[pl.ds(shape.row(x, t), 8), :] = got[slot]
            elif c == 0:
                raw = [got[slots["r", i, k, t]] for i in range(4)]
                fill_rock(shape, rock, x, t, cohesion, friction, *raw[2:])
                for i in range(2):
                    rock[i, pl.ds((x + BESIDE) * shape.rows_y + t, 8), :] = raw[i]

    def body(below, above):
        take(below, lambda k: -1 - k)
        take(above, lambda k: shape.rows_x + k)

    by_parity("gx", body, (first, second))


def fill_rock(shape, rock, x, t, cohesion, friction, which, able):
    hold = jnp.full((8, shape.depth), cohesion[0], jnp.float32)
    rub = jnp.full((8, shape.depth), friction[0], jnp.float32)
    for k in range(1, cohesion.shape[0]):
        hit = which == k
        hold = jnp.where(hit, cohesion[k], hold)
        rub = jnp.where(hit, friction[k], rub)
    own = pl.multiple_of((x + BESIDE) * shape.rows_y + t, 8)
    rock[2, pl.ds(own, 8), :] = hold * jnp.sqrt(1.0 - rub * rub)
    rock[3, pl.ds(own, 8), :] = rub
    rock[4, pl.ds(own, 8), :] = jnp.where(able == 1, 1.0, 0.0)


def rim_tile(shape, ref, x, sub):
    after, before = tile(ref, shape.row(x + 1, -RIM)), tile(ref, shape.row(x, -RIM))
    return jnp.where(sub < 4, after, before)


def send_x(shape, flow, buoyancy, got_first, got_second, first, second):
    layer_at = {x: i for i, x in enumerate(edge_layers(shape))}
    sub = lax.broadcasted_iota(jnp.int32, (8, shape.depth), 0)

    def fill(out, side, place, got_below, got_above):
        for (kind, c, k, t), slot in x_slots(shape, side).items():
            x = place(k)
            if kind == "s" and t == "rim":
                for got, rims, at in (
                    (got_above, HIGH_FLOW_Y, lambda d: d),
                    (got_below, LOW_FLOW_Y, lambda d: 7 - d),
                ):
                    for j, (which, depth) in enumerate(entries(rims)):
                        if DRIVES[which] == c:
                            single = got[got.shape[0] - 1, pl.ds(8 * layer_at[x] + j, 1), :]
                            out[slot, pl.ds(at(depth), 1), :] = single
            else:
                ref = flow.at[c] if kind == "v" else buoyancy
                if t == "rim":
                    out[slot] = rim_tile(shape, ref, x, sub)
                else:
                    out[slot] = tile(ref, shape.row(x, t))

    def with_corners(got_below, got_above):
        def body(below, above):
            fill(above, 0, lambda k: shape.rows_x - 1 - k, got_below, got_above)
            fill(below, 1, lambda k: k, got_below, got_above)

        by_parity("gx", body, (first, second))

    by_parity("gy", with_corners, (got_first, got_second))


NEAR, FAR = near_weight, far_weight
UP = {1: NEAR, 0: -NEAR, 2: -FAR, -1: FAR}
DOWN = {0: NEAR, -1: -NEAR, 1: -FAR, -2: FAR}


def crossing(c, x, sources):
    total = None
    for step, weight in (UP if c == 0 else DOWN).items():
        if x + step in sources:
            term = weight * sources[x + step]()
            total = term if total is None else total + term
    return total


def receive_x(shape, stress, flow, buoyancy, got, sent):
    rows_x, depth = shape.rows_x, shape.depth
    sub = lax.broadcasted_iota(jnp.int32, (8, depth), 0)
    zero = jnp.zeros((8, depth), jnp.float32)

    def add(c, row, force):
        flow[c, pl.ds(row, 8), :] += time_step * tile(buoyancy, row) * force

    def body(below, above, sent_below, sent_above):
        def read(sides):
            return {
                (kind, c, place(k), t): (ref, slot)
                for ref, side, place in sides
                for (kind, c, k, t), slot in x_slots(shape, side).items()
            }

        came = read(((below, 0, lambda k: -1 - k), (above, 1, lambda k: rows_x + k)))
        went = read(((sent_above, 0, lambda k: rows_x - 1 - k), (sent_below, 1, lambda k: k)))

        def rims(of, c):
            return {
                x: (lambda ref=ref, slot=slot: ref[slot])
                for (kind, which, x, t), (ref, slot) in of.items()
                if (kind, which, t) == ("s", DRIVES[c], "rim")
            }

        for (kind, c, x, t), (ref, slot) in came.items():
            if t != "rim":
                flow[c, pl.ds(shape.row(x, t), 8), :] = ref[slot]
        for t in range(0, shape.rows_y, 8):
            for c in range(3):
                there = {
                    x: (lambda x=x: tile(stress.at[DRIVES[c]], shape.row(x, t)))
                    for x in edge_layers(shape) + beside_layers(shape)
                }
                inside = {x: there[x] for x in edge_layers(shape)}
                outside = {x: there[x] for x in beside_layers(shape)}
                for targets, sources in ((inside, outside), (outside, inside)):
                    for x in targets:
                        force = crossing(c, x, sources)
                        if force is not None:
                            add(c, shape.row(x, t), force)
        for c in range(3):
            halo, own = rims(came, c), rims(went, c)
            forces = {x: crossing(c, x, halo) for x in edge_layers(shape)}
            for x in sorted({x + d for x in edge_layers(shape) for d in (0, 1)}):
                high, low = forces.get(x - 1), forces.get(x)
                if high is None and low is None:
                    continue
                high, low = (zero if f is None else f for f in (high, low))
                add(c, shape.row(x, -RIM), jnp.where(sub < 4, high, low))
            for x in [d for k in range(BESIDE) for d in (-1 - k, rows_x + k)]:
                ref, slot = came["v", c, x, "rim"]
                value = ref[slot]
                force = crossing(c, x, own)
                if force is not None:
                    ref, slot = came["b", 0, x, "rim"]
                    value = value + time_step * ref[slot] * force
                flow[c, pl.ds(shape.row(x + 1, -RIM), 4), :] = value[0:4]
                flow[c, pl.ds(shape.row(x, -4), 4), :] = value[4:8]

    by_parity("gx", body, got, sent)


class Lanes:
    def __init__(self, depth):
        self.depth = depth
        lane = lax.broadcasted_iota(jnp.int32, (8, depth), 1)
        zero = jnp.zeros((8, depth), jnp.float32)
        near = jnp.full((8, depth), near_weight, jnp.float32)
        far = jnp.full((8, depth), far_weight, jnp.float32)
        self.f_up = jnp.where(lane < depth - 1, near, zero)
        self.f_up2 = jnp.where(lane < depth - 2, far, zero)
        self.f_down = jnp.where(lane > 0, far, zero)
        self.b_down = jnp.where(lane > 0, near, zero)
        self.b_down2 = jnp.where(lane > 1, far, zero)
        self.b_up = jnp.where(lane < depth - 1, far, zero)

    def forward(self, f):
        up, up2, down = (pltpu.roll(f, s % self.depth, 1) for s in (-1, -2, 1))
        return (self.f_up * up - near_weight * f) - (self.f_up2 * up2 - self.f_down * down)

    def backward(self, f):
        up, down, down2 = (pltpu.roll(f, s % self.depth, 1) for s in (-1, 1, 2))
        return (near_weight * f - self.b_down * down) - (self.b_up * up - self.b_down2 * down2)


def forward(ref, row, step):
    a, b, c, d = (ref[pl.ds(row + k * step, 8), :] for k in (-1, 0, 1, 2))
    return near_weight * (c - b) - far_weight * (d - a)


def backward(ref, row, step):
    a, b, c, d = (ref[pl.ds(row + k * step, 8), :] for k in (-2, -1, 0, 1))
    return near_weight * (c - b) - far_weight * (d - a)


def tile(ref, row):
    return ref[pl.ds(row, 8), :]


def push_velocity(shape, lanes, stress, flow, buoyancy, row, along="xyz"):
    sx, sy = shape.pitch, 1
    xx, yy, zz, xy, xz, yz = (stress.at[c] for c in range(6))
    parts = {
        "x": lambda: (forward(xx, row, sx), backward(xy, row, sx), backward(xz, row, sx)),
        "y": lambda: (backward(xy, row, sy), forward(yy, row, sy), backward(yz, row, sy)),
        "z": lambda: (
            lanes.backward(tile(xz, row)),
            lanes.backward(tile(yz, row)),
            lanes.forward(tile(zz, row)),
        ),
    }
    force = parts[along[0]]()
    for axis in along[1:]:
        force = [f + g for f, g in zip(force, parts[axis]())]
    scale = time_step * tile(buoyancy, row)
    for c in range(3):
        flow[c, pl.ds(row, 8), :] += scale * force[c]


def push_across_y(halves, flow, buoyancy, row):
    xy, yy, yz = halves
    force = (backward(xy, row, 1), forward(yy, row, 1), backward(yz, row, 1))
    scale = time_step * tile(buoyancy, row)
    for c in range(3):
        flow[c, pl.ds(row, 8), :] += scale * force[c]


def layers(first, stop, body, unroll):
    def run(x, carry):
        body(x)
        return carry

    lax.fori_loop(first, stop, run, 0, unroll=unroll)


def aligned(shape, x, y):
    return pl.multiple_of((x + PAD_X) * shape.pitch + RIM + y, 8)


def inject(shape, stress, source_cell, source_moment, wanted):
    rows_x, rows_y, depth = shape.rows_x, shape.rows_y, shape.depth
    total_y = rows_y * lax.axis_size("gy")
    start_x = lax.axis_index("gx") * rows_x
    start_y = lax.axis_index("gy") * rows_y
    sub = lax.broadcasted_iota(jnp.int32, (8, depth), 0)
    lane = lax.broadcasted_iota(jnp.int32, (8, depth), 1)
    for s in range(source_cell.shape[0]):
        cell = source_cell[s]
        line = lax.div(cell, depth)
        x = lax.div(line, total_y) - start_x
        y = lax.rem(line, total_y) - start_y
        z = lax.rem(cell, depth)

        @pl.when(wanted(x) & (y >= 0) & (y < rows_y))
        def _(x=x, y=y, z=z, s=s):
            band = lax.div(y, 8) * 8
            row = aligned(shape, x, band)
            here = (sub == y - band) & (lane == z)
            for c in range(6):
                amount = time_step * source_moment[c, s]
                stress[c, pl.ds(row, 8), :] += jnp.where(here, amount, 0.0)


def push_stress(shape, lanes, stress, flow, rock, x):
    sx, sy = shape.pitch, 1
    vx, vy, vz = (flow.at[c] for c in range(3))

    for t in range(0, shape.rows_y, 8):
        row = aligned(shape, x, t)
        own = pl.multiple_of((x + BESIDE) * shape.rows_y + t, 8)
        first = time_step * rock[0, pl.ds(own, 8), :]
        shear = time_step * rock[1, pl.ds(own, 8), :]
        strain_x = backward(vx, row, sx)
        strain_y = backward(vy, row, sy)
        here_z = tile(vz, row)
        strain_z = lanes.backward(here_z)
        volume = first * (strain_x + strain_y + strain_z)
        twice = 2.0 * shear
        xx = tile(stress.at[XX], row) + (volume + twice * strain_x)
        yy = tile(stress.at[YY], row) + (volume + twice * strain_y)
        zz = tile(stress.at[ZZ], row) + (volume + twice * strain_z)
        xy = tile(stress.at[XY], row) + shear * (forward(vx, row, sy) + forward(vy, row, sx))
        xz = tile(stress.at[XZ], row) + shear * (
            lanes.forward(tile(vx, row)) + forward(vz, row, sx)
        )
        yz = tile(stress.at[YZ], row) + shear * (
            lanes.forward(tile(vy, row)) + forward(vz, row, sy)
        )
        pressure = (xx + yy + zz) * (1.0 / 3.0)
        dx, dy, dz = xx - pressure, yy - pressure, zz - pressure
        second = 0.5 * (dx * dx + dy * dy + dz * dz) + xy * xy + xz * xz + yz * yz
        strength = jnp.maximum(
            rock[2, pl.ds(own, 8), :] - pressure * rock[3, pl.ds(own, 8), :], 0.0
        )
        ratio = strength * lax.rsqrt(jnp.maximum(second, shear_floor * shear_floor))
        factor = jnp.where(rock[4, pl.ds(own, 8), :] > 0.5, jnp.minimum(ratio, 1.0), 1.0)
        stress[XX, pl.ds(row, 8), :] = pressure + factor * dx
        stress[YY, pl.ds(row, 8), :] = pressure + factor * dy
        stress[ZZ, pl.ds(row, 8), :] = pressure + factor * dz
        stress[XY, pl.ds(row, 8), :] = factor * xy
        stress[XZ, pl.ds(row, 8), :] = factor * xz
        stress[YZ, pl.ds(row, 8), :] = factor * yz


def own_cells(shape, ref, first=0, count=None):
    lead = ref.shape[:-2]
    view = ref.reshape(*lead, shape.rows_x + 2 * PAD_X + 1, shape.pitch, shape.depth)
    count = shape.rows_x - first if count is None else count
    return view.at[
        (slice(None),) * len(lead) + (pl.ds(PAD_X + first, count), pl.ds(RIM, shape.rows_y))
    ]


def run_copies(pairs, sems):
    copies = [pltpu.make_async_copy(a, b, sems.at[i]) for i, (a, b) in enumerate(pairs)]
    for c in copies:
        c.start()
    for c in copies:
        c.wait()


def vmem(shape):
    return pltpu.VMEM(shape, jnp.float32)


in_vmem = pl.BlockSpec(memory_space=pltpu.VMEM)
in_smem = pl.BlockSpec(memory_space=pltpu.SMEM)
in_hbm = pl.BlockSpec(memory_space=pltpu.HBM)


def call(body, ins, in_specs, out_shape, out_specs, flops, aliases=None, scratch=()):
    space = {id(in_vmem): pltpu.VMEM, id(in_hbm): pltpu.HBM}
    ins = [
        pltpu.with_memory_space_constraint(x, space[id(s)]) if id(s) in space else x
        for x, s in zip(ins, in_specs)
    ]
    return pl.pallas_call(
        body,
        in_specs=in_specs,
        out_shape=out_shape,
        out_specs=out_specs,
        input_output_aliases=aliases or {},
        scratch_shapes=scratch,
        cost_estimate=pl.CostEstimate(flops=flops, bytes_accessed=1000000, transcendentals=0),
        compiler_params=pltpu.CompilerParams(vmem_limit_bytes=16 * 1024 * 1024),
    )(*ins)


def swaps(axis, first, second):
    count = lax.axis_size(axis)
    got = []
    for start, block in ((0, first), (1, second)):
        pairs = []
        for low in range(start, count - 1, 2):
            pairs += [(low, low + 1), (low + 1, low)]
        got.append(lax.ppermute(block, axis, pairs))
    return got


def steps(
    velocity,
    stress,
    lame_first,
    modulus,
    buoyancy,
    zone,
    eligible,
    cohesion,
    friction,
    source_cell,
    source_moment,
):
    shape = Shape(*zone.shape)
    rows_x, rows_y, depth = zone.shape
    whole_s, whole_v = vmem((6, shape.rows, depth)), vmem((3, shape.rows, depth))
    whole_b, whole_h = vmem((shape.rows, depth)), vmem((3, shape.rows, depth))
    y_buffers = {first: vmem((y_count(first), rows_x, depth)) for first in (True, False)}
    x_buffer = vmem((x_count(shape), 8, depth))
    early_buffer = vmem((len(early_slots(shape)), 8, depth))
    whole_r = vmem((5, (rows_x + 2 * BESIDE) * rows_y, depth))

    deep = (4, rows_x - 4)
    next_inner = (6, rows_x - 6)
    bands = range(0, rows_y, 8)

    def own_forces(lanes, s, v, b, x):
        for t in bands:
            push_velocity(shape, lanes, s, v, b, aligned(shape, x, t))

    def load(
        v_in, s_in, b_in, lame_in, shear_in, zone_in, able_in,
        s, v, b, h, first, second, x_first, x_second, floats, ints, sems, edge_sems,
    ):
        groups, edges = [], []
        for g, x in enumerate(range(0, rows_x, 8)):
            group = []
            for i, (source, ref) in enumerate(((s_in, s), (v_in, v), (b_in, b))):
                part = source.at[:, pl.ds(x, 8)] if i < 2 else source.at[pl.ds(x, 8)]
                place = own_cells(shape, ref, x, 8)
                group.append(pltpu.make_async_copy(part, place, sems.at[g, i]))
                group[-1].start()
            groups.append(group)
        for i, source in enumerate((lame_in, shear_in, zone_in, able_in)):
            ref = floats.at[i] if i < 2 else ints.at[i - 2]
            for side, x in enumerate((rows_x - BESIDE, 0)):
                part = source.at[pl.ds(x, BESIDE)]
                edges.append(pltpu.make_async_copy(part, ref.at[side], edge_sems.at[i, side]))
                edges[-1].start()

        def raw(c, side, x, t):
            if c < 2:
                return floats[c, side, x, pl.ds(t, 8), :]
            return ints[c - 2, side, x, pl.ds(t, 8), :].astype(jnp.float32)

        zero = jnp.zeros((8, depth), jnp.float32)
        for x in range(-2, rows_x + 3):
            for c in (XY, YY, YZ):
                s[c, pl.ds(shape.row(x, -RIM), 8), :] = zero
        for x in range(-2, rows_x + 2):
            for t in bands:
                for c in range(3):
                    h[c, pl.ds(shape.row(x, t), 8), :] = zero
        for x in (-2, -1, rows_x, rows_x + 1):
            for t in bands:
                for c in range(6):
                    s[c, pl.ds(shape.row(x, t), 8), :] = zero
        lanes = Lanes(depth)
        done = 0
        for g, group in enumerate(groups):
            for copy in group:
                copy.wait()
            stop = rows_x if g == len(groups) - 1 else 8 * g + 6
            layers(done, stop, lambda x: own_forces(lanes, s, v, b, x), stop - done)
            done = stop
        send_y(shape, s, v, b, first, second)
        for copy in edges:
            copy.wait()
        send_early(shape, s, b, raw, x_first, x_second)

    s, v, b, h, first, second, x_first, x_second = call(
        load,
        [velocity, stress, buoyancy, lame_first, modulus, zone, eligible],
        [in_hbm] * 7,
        [whole_s, whole_v, whole_b, whole_h] + [y_buffers[True]] * 2 + [early_buffer] * 2,
        [in_vmem] * 8,
        10000000,
        scratch=[
            pltpu.VMEM((2, 2, BESIDE, rows_y, depth), jnp.float32),
            pltpu.VMEM((2, 2, BESIDE, rows_y, depth), jnp.int32),
            pltpu.SemaphoreType.DMA((rows_x // 8, 3)),
            pltpu.SemaphoreType.DMA((4, 2)),
        ],
    )

    def prepare(after, lame_in, shear_in, zone_in, able_in, cohesion, friction, rock, zones, able, sems):
        flat = rock.reshape(5, rows_x + 2 * BESIDE, rows_y, depth)
        pairs = [(zone_in, zones), (able_in, able)]
        pairs += [(a, flat.at[i, pl.ds(BESIDE, rows_x)]) for i, a in enumerate((lame_in, shear_in))]
        run_copies(pairs, sems)

        def layer(x):
            for t in bands:
                which, able_here = zones[x, pl.ds(t, 8), :], able[x, pl.ds(t, 8), :]
                fill_rock(shape, rock, x, t, cohesion, friction, which, able_here)

        layers(0, rows_x, layer, 4)

    early_rims = tuple(range(BESIDE + 1)), tuple(range(rows_x - BESIDE, rows_x + 1))
    early = tuple(range(5)), tuple(range(rows_x - 5, rows_x))

    def turn(s, v_in, b_in, h_in, got_a, got_b, v, b, h, out_a, out_b):
        receive_y(shape, h, v, b, got_a, got_b)
        halves = [h.at[c] for c in range(3)]
        own = [s.at[c] for c in (XY, YY, YZ)]
        for x in early[0] + early[1]:
            for t in bands:
                push_across_y(halves, v, b, shape.row(x, t))
        for x in early_rims[0] + early_rims[1]:
            push_across_y(own, v, b, shape.row(x, -RIM))
        send_x(shape, v, b, got_a, got_b, out_a, out_b)

    def interior(
        s_in, v_in, b_in, h, rock_in, early_a, early_b, cell, moment, cohesion, friction, s, v, b, rock
    ):
        lanes = Lanes(depth)
        halves = [h.at[c] for c in range(3)]
        own = [s.at[c] for c in (XY, YY, YZ)]

        def layer(x):
            for t in bands:
                push_across_y(halves, v, b, aligned(shape, x, t))

        def rim(x):
            push_across_y(own, v, b, aligned(shape, x, -RIM))

        layers(early[0][-1] + 1, early[1][0], layer, 4)
        layers(early_rims[0][-1] + 1, early_rims[1][0], rim, 4)
        inject(shape, s, cell, moment, lambda x: (x >= deep[0]) & (x < deep[1]))
        layers(*deep, lambda x: push_stress(shape, lanes, s, v, rock, x), 4)
        layers(*next_inner, lambda x: own_forces(lanes, s, v, b, x), 4)
        receive_early(shape, s, b, rock, cohesion, friction, early_a, early_b)

    def border(
        s_in, v_in, b, rock, got_a, got_b, sent_a, sent_b, cell, moment, s, v, out_a, out_b
    ):
        receive_x(shape, s, v, b, (got_a, got_b), (sent_a, sent_b))
        lanes = Lanes(depth)
        low, high = -BESIDE, rows_x + BESIDE
        near = lambda x: (x >= low) & (x < high) & ((x < deep[0]) | (x >= deep[1]))
        inject(shape, s, cell, moment, near)
        for first, stop in ((low, deep[0]), (deep[1], high)):
            for x in range(first, stop):
                push_stress(shape, lanes, s, v, rock, x)
        for first, stop in ((-2, next_inner[0]), (next_inner[1], rows_x + 2)):
            for x in range(first, stop):
                own_forces(lanes, s, v, b, x)
        send_y(shape, s, v, None, out_a, out_b)

    def finish(
        s_in, v_in, b, h_in, rock, got_a, got_b, cell, moment, s, v, h, v_out, s_out, sems
    ):
        receive_y(shape, h, v, None, got_a, got_b)
        lanes = Lanes(depth)
        halves = [h.at[c] for c in range(3)]
        own = [s.at[c] for c in (XY, YY, YZ)]

        def layer(x):
            for t in bands:
                push_across_y(halves, v, b, aligned(shape, x, t))

        layers(-2, rows_x + 2, layer, 4)
        copies = [pltpu.make_async_copy(own_cells(shape, v), v_out, sems.at[0])]
        copies[0].start()
        layers(0, rows_x + 1, lambda x: push_across_y(own, v, b, aligned(shape, x, -RIM)), 3)
        inject(shape, s, cell, moment, lambda x: (x >= 0) & (x < rows_x))
        for i, x in enumerate(range(0, rows_x, 8)):
            layers(x, x + 8, lambda x: push_stress(shape, lanes, s, v, rock, x), 8)
            part = s_out.at[:, pl.ds(x, 8)]
            copies.append(pltpu.make_async_copy(own_cells(shape, s, x, 8), part, sems.at[i + 1]))
            copies[-1].start()
        for c in copies:
            c.wait()

    cells = [source_cell, source_moment]
    first, second = swaps("gy", first, second)
    x_first, x_second = swaps("gx", x_first, x_second)
    v, b, h, sent_a, sent_b = call(
        turn,
        [s, v, b, h, first, second],
        [in_vmem] * 6,
        [whole_v, whole_b, whole_h, x_buffer, x_buffer],
        [in_vmem] * 5,
        1000000,
        aliases={1: 0, 2: 1, 3: 2},
    )
    got_a, got_b = swaps("gx", sent_a, sent_b)
    rock = call(
        prepare,
        [v, lame_first, modulus, zone, eligible, cohesion, friction],
        [in_vmem] + [in_hbm] * 4 + [in_smem] * 2,
        whole_r,
        in_vmem,
        10000000,
        scratch=[
            pltpu.VMEM((rows_x, rows_y, depth), jnp.int32),
            pltpu.VMEM((rows_x, rows_y, depth), jnp.int32),
            pltpu.SemaphoreType.DMA((4,)),
        ],
    )
    s, v, b, rock = call(
        interior,
        [s, v, b, h, rock, x_first, x_second] + cells + [cohesion, friction],
        [in_vmem] * 7 + [in_smem] * 4,
        [whole_s, whole_v, whole_b, whole_r],
        [in_vmem] * 4,
        10000000,
        aliases={0: 0, 1: 1, 2: 2, 4: 3},
    )
    s, v, first, second = call(
        border,
        [s, v, b, rock, got_a, got_b, sent_a, sent_b] + cells,
        [in_vmem] * 8 + [in_smem] * 2,
        [whole_s, whole_v, y_buffers[False], y_buffers[False]],
        [in_vmem] * 4,
        10000000,
        aliases={0: 0, 1: 1},
    )
    first, second = swaps("gy", first, second)
    outs = call(
        finish,
        [s, v, b, h, rock, first, second] + cells,
        [in_vmem] * 7 + [in_smem] * 2,
        [
            whole_s,
            whole_v,
            whole_h,
            pltpu.HBM(velocity.shape, jnp.float32),
            pltpu.HBM(stress.shape, jnp.float32),
        ],
        [in_vmem] * 3 + [in_hbm] * 2,
        10000000,
        aliases={0: 0, 1: 1, 3: 2},
        scratch=[pltpu.SemaphoreType.DMA((rows_x // 8 + 1,))],
    )
    return (outs[3], outs[4])


def solution(mesh):
    placed = (
        P(None, "gx", "gy", None),
        P(None, "gx", "gy", None),
        P("gx", "gy", None),
        P("gx", "gy", None),
        P("gx", "gy", None),
        P("gx", "gy", None),
        P("gx", "gy", None),
        P(),
        P(),
        P(),
        P(),
    )
    return jax.shard_map(
        steps,
        mesh=mesh,
        in_specs=placed,
        out_specs=(P(None, "gx", "gy", None), P(None, "gx", "gy", None)),
        check_vma=False,
    )
```

```python
import jax
import jax.numpy as jnp
from jax import lax
from jax.experimental import pallas as pl
from jax.experimental.pallas import tpu as pltpu
from jax.sharding import PartitionSpec as P


time_step = 0.1
near_weight = 9.0 / 8.0
far_weight = 1.0 / 24.0
shear_floor = 0.25

XX, YY, ZZ, XY, XZ, YZ = range(6)

LOW_X = ((XX, 1), (XY, 2), (XZ, 2))
HIGH_X = ((XX, 2), (XY, 1), (XZ, 1))
LOW_FLOW_Y = ((0, 1), (1, 2), (2, 1))
HIGH_FLOW_Y = ((0, 2), (1, 1), (2, 2))
BESIDE = 3
LOW_DEEP_X = ((0, 5), (1, 4), (2, 4))
HIGH_DEEP_X = ((0, 4), (1, 5), (2, 5))
DRIVES_X = (XX, XY, XZ)
DRIVES_Y = (XY, YY, YZ)
LOW_PUSH = ((0, 2), (1, 1), (2, 2))
HIGH_PUSH = ((0, 1), (1, 2), (2, 1))

NEAR, FAR = near_weight, far_weight
UP = {1: NEAR, 0: -NEAR, 2: -FAR, -1: FAR}
DOWN = {0: NEAR, -1: -NEAR, 1: -FAR, -2: FAR}


def crossing(table, at, sources):
    total = None
    for step, weight in table.items():
        if at + step in sources:
            term = weight * sources[at + step]()
            total = term if total is None else total + term
    return total


def crossing_x(c, x, sources):
    return crossing(UP if c == 0 else DOWN, x, sources)


def crossing_y(c, y, sources):
    return crossing(UP if c == 1 else DOWN, y, sources)


PAD_X = 8
RIM = 8


class Shape:
    def __init__(self, rows_x, rows_y, depth):
        self.rows_x, self.rows_y, self.depth = rows_x, rows_y, depth
        self.pitch = rows_y + RIM
        self.rows = (rows_x + 2 * PAD_X + 1) * self.pitch

    def row(self, x, y):
        return (x + PAD_X) * self.pitch + RIM + y


def entries(spec):
    return [(c, k) for c, depth in spec for k in range(depth)]


def edge_layers(shape):
    return (0, 1, shape.rows_x - 2, shape.rows_x - 1)


def beside_layers(shape):
    return (-2, -1, shape.rows_x, shape.rows_x + 1)


def by_parity(axis, body, *swapped):
    odd = lax.axis_index(axis) % 2

    @pl.when(odd == 0)
    def _():
        body(*[r for first, second in swapped for r in (second, first)])

    @pl.when(odd == 1)
    def _():
        body(*[r for first, second in swapped for r in (first, second)])


def y_faces(shape):
    rows = shape.rows_y
    above = (LOW_PUSH, LOW_FLOW_Y, lambda y: y - rows, lambda y: y + rows)
    below = (HIGH_PUSH, HIGH_FLOW_Y, lambda y: y + rows, lambda y: y - rows)
    return above, below


def pushed(spec, shape):
    low = spec is LOW_PUSH
    return [(c, k if low else shape.rows_y - 1 - k) for c, k in entries(spec)]


def rim_rows(spec, shape):
    low = spec is LOW_FLOW_Y
    return [(c, -1 - k if low else shape.rows_y + k) for c, k in entries(spec)]


def side_rows(spec, shape):
    return [-1, -2] if spec is LOW_FLOW_Y else [shape.rows_y, shape.rows_y + 1]


def send_y(shape, stress, flow, buoyancy, first, second, groups, singles=True):
    rows_y = shape.rows_y

    def fill(out, push, flow_spec, to_other, to_own):
        face = [y for y in (0, 1, rows_y - 2, rows_y - 1) if to_other(y) in (-2, -1, rows_y, rows_y + 1)]

        def force(c, y, read):
            sources = {to_other(o): (lambda o=o: read(DRIVES_Y[c], o)) for o in face}
            return crossing_y(c, y, sources)

        for x in groups:

            def read(c, y):
                return stress[c, pl.ds(shape.row(x, y), 8, stride=shape.pitch), :]

            slot = 0
            for c, y in pushed(push, shape):
                out[slot, pl.ds(x, 8), :] = force(c, y, read)
                slot += 1
            whole = [(flow.at[c], to_own(y)) for c, y in rim_rows(flow_spec, shape)]
            if buoyancy is not None:
                whole += [(buoyancy, to_own(y)) for y in side_rows(flow_spec, shape)]
            for ref, y in whole:
                out[slot, pl.ds(x, 8), :] = ref[pl.ds(shape.row(x, y), 8, stride=shape.pitch), :]
                slot += 1
        if not singles:
            return
        last = out.at[out.shape[0] - 1]
        for i, x in enumerate(edge_layers(shape) if buoyancy is not None else beside_layers(shape)):

            def single(c, y):
                return stress[c, pl.ds(shape.row(x, y), 1), :]

            if buoyancy is not None:
                rows = [single(DRIVES_X[c], to_own(y)) for c, y in rim_rows(flow_spec, shape)]
            else:
                rows = [force(c, y, single) for c, y in pushed(push, shape)]
            for j, row in enumerate(rows):
                last[pl.ds(8 * i + j, 1), :] = row

    def body(below, above):
        for out, face in zip((above, below), y_faces(shape)):
            fill(out, *face)

    by_parity("gy", body, (first, second))


def receive_y(shape, force, flow, buoyancy, first, second, begun=False):
    def take(got, push, flow_spec):
        slot = 0
        whole = [(force.at[c], y, False) for c, y in pushed(push, shape)]
        whole += [(flow.at[c], y, begun) for c, y in rim_rows(flow_spec, shape)]
        if buoyancy is not None:
            whole += [(buoyancy, y, False) for y in side_rows(flow_spec, shape)]
        for slot, (ref, y, add) in enumerate(whole):
            for x in range(0, shape.rows_x, 8):
                place = pl.ds(shape.row(x, y), 8, stride=shape.pitch)
                value = got[slot, pl.ds(x, 8), :]
                ref[place, :] = ref[place, :] + value if add else value
        if buoyancy is None:
            for i, x in enumerate(beside_layers(shape)):
                for j, (c, y) in enumerate(pushed(push, shape)):
                    single = got[got.shape[0] - 1, pl.ds(8 * i + j, 1), :]
                    force[c, pl.ds(shape.row(x, y), 1), :] = single

    def body(below, above):
        take(below, LOW_PUSH, LOW_FLOW_Y)
        take(above, HIGH_PUSH, HIGH_FLOW_Y)

    by_parity("gy", body, (first, second))


def y_count(first_round):
    most = max(
        len(entries(push)) + len(entries(flow_spec))
        for push, flow_spec in ((LOW_PUSH, LOW_FLOW_Y), (HIGH_PUSH, HIGH_FLOW_Y))
    )
    return most + 1 + (2 if first_round else 0)


def early_slots(shape, side):
    bands = range(0, shape.rows_y, 8)
    deep = (LOW_DEEP_X, HIGH_DEEP_X)[side]
    keys = [("s", c, k, t) for c in range(6) for k in range(BESIDE) for t in bands]
    keys += [("r", c, k, t) for c in range(4) for k in range(BESIDE) for t in bands]
    keys += [("b", 0, k, t) for k in range(2) for t in bands]
    keys += [("v", c, k, t) for c, k in entries(deep) for t in bands]
    return {key: i for i, key in enumerate(keys)}


def early_count(shape):
    return max(len(early_slots(shape, side)) for side in (0, 1))


def send_early(shape, stress, flow, buoyancy, raw, first, second):
    def fill(out, side, place):
        for (kind, c, k, t), slot in early_slots(shape, side).items():
            x = place(k)
            if kind == "r":
                at = x - (shape.rows_x - BESIDE if side == 0 else 0)
                out[slot] = raw(c, side, at, t)
            else:
                ref = buoyancy if kind == "b" else (stress if kind == "s" else flow).at[c]
                out[slot] = tile(ref, shape.row(x, t))

    def body(below, above):
        fill(above, 0, lambda k: shape.rows_x - 1 - k)
        fill(below, 1, lambda k: k)

    by_parity("gx", body, (first, second))


def receive_early(shape, stress, flow, buoyancy, rock, cohesion, friction, first, second):
    def take(got, side, place):
        slots = early_slots(shape, side)
        for (kind, c, k, t), slot in slots.items():
            x = place(k)
            if kind == "s":
                stress[c, pl.ds(shape.row(x, t), 8), :] = got[slot]
            elif kind == "b":
                buoyancy[pl.ds(shape.row(x, t), 8), :] = got[slot]
            elif kind == "v":
                flow[c, pl.ds(shape.row(x, t), 8), :] = got[slot]
            elif c == 0:
                raw = [got[slots["r", i, k, t]] for i in range(4)]
                fill_rock(shape, rock, x, t, cohesion, friction, *raw)

    def body(below, above):
        take(below, 0, lambda k: -1 - k)
        take(above, 1, lambda k: shape.rows_x + k)

    by_parity("gx", body, (first, second))
    for t in range(0, shape.rows_y, 8):
        for c in range(3):
            there = {
                x: (lambda x=x: tile(stress.at[DRIVES_X[c]], shape.row(x, t)))
                for x in edge_layers(shape) + beside_layers(shape)
            }
            inside = {x: there[x] for x in edge_layers(shape)}
            outside = {x: there[x] for x in beside_layers(shape)}
            for targets, sources in ((inside, outside), (outside, inside)):
                for x in targets:
                    force = crossing_x(c, x, sources)
                    if force is not None:
                        row = shape.row(x, t)
                        flow[c, pl.ds(row, 8), :] += time_step * tile(buoyancy, row) * force


def fill_rock(shape, rock, x, t, cohesion, friction, first, shear, which, able):
    hold = jnp.full((8, shape.depth), cohesion[0], jnp.float32)
    rub = jnp.full((8, shape.depth), friction[0], jnp.float32)
    for k in range(1, cohesion.shape[0]):
        hit = which == k
        hold = jnp.where(hit, cohesion[k], hold)
        rub = jnp.where(hit, friction[k], rub)
    own = pl.multiple_of((x + BESIDE) * shape.rows_y + t, 8)
    rock[0, pl.ds(own, 8), :] = first
    rock[1, pl.ds(own, 8), :] = shear
    rock[2, pl.ds(own, 8), :] = hold * jnp.sqrt(1.0 - rub * rub)
    rock[3, pl.ds(own, 8), :] = rub
    rock[4, pl.ds(own, 8), :] = jnp.where(able == 1, 1.0, 0.0)


def late_rows(shape, side):
    spec, deep = ((LOW_X, LOW_DEEP_X), (HIGH_X, HIGH_DEEP_X))[side]
    reached = pushed(LOW_PUSH, shape) + pushed(HIGH_PUSH, shape)
    rims = rim_rows(LOW_FLOW_Y, shape) + rim_rows(HIGH_FLOW_Y, shape)
    keys = [("d", c, k, y) for c, k in entries(deep) for which, y in reached if which == c]
    keys += [("v", c, k, y) for k in range(BESIDE) for c, y in rims]
    sides = side_rows(LOW_FLOW_Y, shape) + side_rows(HIGH_FLOW_Y, shape)
    keys += [("b", 0, k, y) for k in range(2) for y in sides]
    depths = dict(spec)
    keys += [("s", c, k, y) for c, y in rims for k in range(depths[DRIVES_X[c]])]
    return {key: i for i, key in enumerate(keys)}


def late_count(shape):
    return -(-max(len(late_rows(shape, side)) for side in (0, 1)) // 8) * 8


def send_late(shape, force, flow, buoyancy, got_first, got_second, first, second):
    layer_at = {x: i for i, x in enumerate(edge_layers(shape))}

    def fill(out, side, place, got_below, got_above):
        singles = {}
        for got, spec in ((got_below, LOW_FLOW_Y), (got_above, HIGH_FLOW_Y)):
            for j, key in enumerate(rim_rows(spec, shape)):
                singles[key] = (got, j)
        for (kind, c, k, y), at in late_rows(shape, side).items():
            x = place(k)
            if kind == "s":
                got, j = singles[c, y]
                row = got[got.shape[0] - 1, pl.ds(8 * layer_at[x] + j, 1), :]
            else:
                ref = {"d": force, "v": flow}[kind].at[c] if kind != "b" else buoyancy
                row = ref[pl.ds(shape.row(x, y), 1), :]
            out[pl.ds(at, 1), :] = row

    def with_singles(got_below, got_above):
        def body(below, above):
            fill(above, 0, lambda k: shape.rows_x - 1 - k, got_below, got_above)
            fill(below, 1, lambda k: k, got_below, got_above)

        by_parity("gx", body, (first, second))

    by_parity("gy", with_singles, (got_first, got_second))


def receive_late(shape, flow, buoyancy, got, sent):
    rows_x = shape.rows_x

    def add(c, x, y, value):
        flow[c, pl.ds(shape.row(x, y), 1), :] += value

    def body(below, above, sent_below, sent_above):
        def read(sides):
            return {
                (kind, c, place(k), y): (lambda ref=ref, at=at: ref[pl.ds(at, 1), :])
                for ref, side, place in sides
                for (kind, c, k, y), at in late_rows(shape, side).items()
            }

        came = read(((below, 0, lambda k: -1 - k), (above, 1, lambda k: rows_x + k)))
        went = read(((sent_above, 0, lambda k: rows_x - 1 - k), (sent_below, 1, lambda k: k)))

        def rims(of, c, y):
            return {x: f for (kind, which, x, at), f in of.items() if (kind, which, at) == ("s", c, y)}

        for (kind, c, x, y), value in came.items():
            if kind == "d":
                add(c, x, y, value())
        for c, y in rim_rows(LOW_FLOW_Y, shape) + rim_rows(HIGH_FLOW_Y, shape):
            halo, own = rims(came, c, y), rims(went, c, y)
            for x in edge_layers(shape):
                force = crossing_x(c, x, halo)
                if force is not None:
                    scale = time_step * buoyancy[pl.ds(shape.row(x, y), 1), :]
                    add(c, x, y, scale * force)
            for x in [d for k in range(BESIDE) for d in (-1 - k, rows_x + k)]:
                value = came["v", c, x, y]()
                force = crossing_x(c, x, own)
                if force is not None:
                    value = value + time_step * came["b", 0, x, y]() * force
                flow[c, pl.ds(shape.row(x, y), 1), :] = value

    by_parity("gx", body, got, sent)


class Lanes:
    def __init__(self, depth):
        self.depth = depth
        lane = lax.broadcasted_iota(jnp.int32, (8, depth), 1)
        zero = jnp.zeros((8, depth), jnp.float32)
        near = jnp.full((8, depth), near_weight, jnp.float32)
        far = jnp.full((8, depth), far_weight, jnp.float32)
        self.f_up = jnp.where(lane < depth - 1, near, zero)
        self.f_up2 = jnp.where(lane < depth - 2, far, zero)
        self.f_down = jnp.where(lane > 0, far, zero)
        self.b_down = jnp.where(lane > 0, near, zero)
        self.b_down2 = jnp.where(lane > 1, far, zero)
        self.b_up = jnp.where(lane < depth - 1, far, zero)

    def forward(self, f):
        up, up2, down = (pltpu.roll(f, s % self.depth, 1) for s in (-1, -2, 1))
        return (self.f_up * up - near_weight * f) - (self.f_up2 * up2 - self.f_down * down)

    def backward(self, f):
        up, down, down2 = (pltpu.roll(f, s % self.depth, 1) for s in (-1, 1, 2))
        return (near_weight * f - self.b_down * down) - (self.b_up * up - self.b_down2 * down2)


def forward(ref, row, step):
    a, b, c, d = (ref[pl.ds(row + k * step, 8), :] for k in (-1, 0, 1, 2))
    return near_weight * (c - b) - far_weight * (d - a)


def backward(ref, row, step):
    a, b, c, d = (ref[pl.ds(row + k * step, 8), :] for k in (-2, -1, 0, 1))
    return near_weight * (c - b) - far_weight * (d - a)


def tile(ref, row):
    return ref[pl.ds(row, 8), :]


def push_velocity(shape, lanes, stress, flow, buoyancy, row, along="xyz"):
    sx, sy = shape.pitch, 1
    xx, yy, zz, xy, xz, yz = (stress.at[c] for c in range(6))
    parts = {
        "x": lambda: (forward(xx, row, sx), backward(xy, row, sx), backward(xz, row, sx)),
        "y": lambda: (backward(xy, row, sy), forward(yy, row, sy), backward(yz, row, sy)),
        "z": lambda: (
            lanes.backward(tile(xz, row)),
            lanes.backward(tile(yz, row)),
            lanes.forward(tile(zz, row)),
        ),
    }
    force = parts[along[0]]()
    for axis in along[1:]:
        force = [f + g for f, g in zip(force, parts[axis]())]
    scale = time_step * tile(buoyancy, row)
    for c in range(3):
        flow[c, pl.ds(row, 8), :] += scale * force[c]


def across_y(stress, buoyancy, row):
    xy, yy, yz = (stress.at[c] for c in DRIVES_Y)
    scale = time_step * tile(buoyancy, row)
    forces = (backward(xy, row, 1), forward(yy, row, 1), backward(yz, row, 1))
    return [scale * f for f in forces]


def layers(first, stop, body, unroll):
    def run(x, carry):
        body(x)
        return carry

    lax.fori_loop(first, stop, run, 0, unroll=unroll)


def aligned(shape, x, y):
    return pl.multiple_of((x + PAD_X) * shape.pitch + RIM + y, 8)


def inject(shape, stress, source_cell, source_moment, wanted):
    rows_x, rows_y, depth = shape.rows_x, shape.rows_y, shape.depth
    total_y = rows_y * lax.axis_size("gy")
    start_x = lax.axis_index("gx") * rows_x
    start_y = lax.axis_index("gy") * rows_y
    sub = lax.broadcasted_iota(jnp.int32, (8, depth), 0)
    lane = lax.broadcasted_iota(jnp.int32, (8, depth), 1)
    for s in range(source_cell.shape[0]):
        cell = source_cell[s]
        line = lax.div(cell, depth)
        x = lax.div(line, total_y) - start_x
        y = lax.rem(line, total_y) - start_y
        z = lax.rem(cell, depth)

        @pl.when(wanted(x) & (y >= 0) & (y < rows_y))
        def _(x=x, y=y, z=z, s=s):
            band = lax.div(y, 8) * 8
            row = aligned(shape, x, band)
            here = (sub == y - band) & (lane == z)
            for c in range(6):
                amount = time_step * source_moment[c, s]
                stress[c, pl.ds(row, 8), :] += jnp.where(here, amount, 0.0)


def push_stress(shape, lanes, stress, flow, rock, x):
    sx, sy = shape.pitch, 1
    vx, vy, vz = (flow.at[c] for c in range(3))

    for t in range(0, shape.rows_y, 8):
        row = aligned(shape, x, t)
        own = pl.multiple_of((x + BESIDE) * shape.rows_y + t, 8)
        first = time_step * rock[0, pl.ds(own, 8), :]
        shear = time_step * rock[1, pl.ds(own, 8), :]
        strain_x = backward(vx, row, sx)
        strain_y = backward(vy, row, sy)
        here_z = tile(vz, row)
        strain_z = lanes.backward(here_z)
        volume = first * (strain_x + strain_y + strain_z)
        twice = 2.0 * shear
        xx = tile(stress.at[XX], row) + (volume + twice * strain_x)
        yy = tile(stress.at[YY], row) + (volume + twice * strain_y)
        zz = tile(stress.at[ZZ], row) + (volume + twice * strain_z)
        xy = tile(stress.at[XY], row) + shear * (forward(vx, row, sy) + forward(vy, row, sx))
        xz = tile(stress.at[XZ], row) + shear * (
            lanes.forward(tile(vx, row)) + forward(vz, row, sx)
        )
        yz = tile(stress.at[YZ], row) + shear * (
            lanes.forward(tile(vy, row)) + forward(vz, row, sy)
        )
        pressure = (xx + yy + zz) * (1.0 / 3.0)
        dx, dy, dz = xx - pressure, yy - pressure, zz - pressure
        second = 0.5 * (dx * dx + dy * dy + dz * dz) + xy * xy + xz * xz + yz * yz
        strength = jnp.maximum(
            rock[2, pl.ds(own, 8), :] - pressure * rock[3, pl.ds(own, 8), :], 0.0
        )
        ratio = strength * lax.rsqrt(jnp.maximum(second, shear_floor * shear_floor))
        factor = jnp.where(rock[4, pl.ds(own, 8), :] > 0.5, jnp.minimum(ratio, 1.0), 1.0)
        stress[XX, pl.ds(row, 8), :] = pressure + factor * dx
        stress[YY, pl.ds(row, 8), :] = pressure + factor * dy
        stress[ZZ, pl.ds(row, 8), :] = pressure + factor * dz
        stress[XY, pl.ds(row, 8), :] = factor * xy
        stress[XZ, pl.ds(row, 8), :] = factor * xz
        stress[YZ, pl.ds(row, 8), :] = factor * yz


def own_cells(shape, ref, first=0, count=None):
    lead = ref.shape[:-2]
    view = ref.reshape(*lead, shape.rows_x + 2 * PAD_X + 1, shape.pitch, shape.depth)
    count = shape.rows_x - first if count is None else count
    return view.at[
        (slice(None),) * len(lead) + (pl.ds(PAD_X + first, count), pl.ds(RIM, shape.rows_y))
    ]


def vmem(shape):
    return pltpu.VMEM(shape, jnp.float32)


in_vmem = pl.BlockSpec(memory_space=pltpu.VMEM)
in_smem = pl.BlockSpec(memory_space=pltpu.SMEM)
in_hbm = pl.BlockSpec(memory_space=pltpu.HBM)


def call(body, ins, in_specs, out_shape, out_specs, flops, aliases=None, scratch=()):
    space = {id(in_vmem): pltpu.VMEM, id(in_hbm): pltpu.HBM}
    ins = [
        pltpu.with_memory_space_constraint(x, space[id(s)]) if id(s) in space else x
        for x, s in zip(ins, in_specs)
    ]
    return pl.pallas_call(
        body,
        in_specs=in_specs,
        out_shape=out_shape,
        out_specs=out_specs,
        input_output_aliases=aliases or {},
        scratch_shapes=scratch,
        cost_estimate=pl.CostEstimate(flops=flops, bytes_accessed=1000000, transcendentals=0),
        compiler_params=pltpu.CompilerParams(vmem_limit_bytes=16 * 1024 * 1024),
    )(*ins)


def swaps(axis, first, second):
    count = lax.axis_size(axis)
    got = []
    for start, block in ((0, first), (1, second)):
        pairs = []
        for low in range(start, count - 1, 2):
            pairs += [(low, low + 1), (low + 1, low)]
        got.append(lax.ppermute(block, axis, pairs))
    return got


def steps(
    velocity,
    stress,
    lame_first,
    modulus,
    buoyancy,
    zone,
    eligible,
    cohesion,
    friction,
    source_cell,
    source_moment,
):
    shape = Shape(*zone.shape)
    rows_x, rows_y, depth = zone.shape
    whole_s, whole_v = vmem((6, shape.rows, depth)), vmem((3, shape.rows, depth))
    whole_b, whole_h = vmem((shape.rows, depth)), vmem((3, shape.rows, depth))
    y_buffers = {first: vmem((y_count(first), rows_x, depth)) for first in (True, False)}
    late_buffer = vmem((late_count(shape), depth))
    early_buffer = vmem((early_count(shape), 8, depth))
    whole_r = vmem((5, (rows_x + 2 * BESIDE) * rows_y, depth))

    inner = (2, rows_x - 2)
    next_inner = (4, rows_x - 4)
    bands = range(0, rows_y, 8)

    def own_forces(lanes, s, v, b, x):
        for t in bands:
            push_velocity(shape, lanes, s, v, b, aligned(shape, x, t))

    def load(
        v_in, s_in, b_in, lame_in, shear_in, zone_in, able_in,
        s, v, b, h, first, second, x_first, x_second, floats, ints, sems, edge_sems,
    ):
        groups, edges = [], []
        marks = list(range(0, rows_x - 8, 8)) + [rows_x - 8, rows_x - 4, rows_x]
        for g, (x, stop) in enumerate(zip(marks, marks[1:])):
            group = []
            for i, (source, ref) in enumerate(((s_in, s), (v_in, v), (b_in, b))):
                span = pl.ds(x, stop - x)
                part = source.at[:, span] if i < 2 else source.at[span]
                place = own_cells(shape, ref, x, stop - x)
                group.append(pltpu.make_async_copy(part, place, sems.at[g, i]))
                group[-1].start()
            groups.append(group)
        for i, source in enumerate((lame_in, shear_in, zone_in, able_in)):
            ref = floats.at[i] if i < 2 else ints.at[i - 2]
            for side, x in enumerate((rows_x - BESIDE, 0)):
                part = source.at[pl.ds(x, BESIDE)]
                edges.append(pltpu.make_async_copy(part, ref.at[side], edge_sems.at[i, side]))
                edges[-1].start()

        def raw(c, side, x, t):
            if c < 2:
                return floats[c, side, x, pl.ds(t, 8), :]
            return ints[c - 2, side, x, pl.ds(t, 8), :].astype(jnp.float32)

        zero = jnp.zeros((8, depth), jnp.float32)
        for x in range(-2, rows_x + 3):
            for c in (XY, YY, YZ):
                s[c, pl.ds(shape.row(x, -RIM), 8), :] = zero
        for x in range(-2, rows_x + 2):
            for t in bands:
                for c in range(3):
                    h[c, pl.ds(shape.row(x, t), 8), :] = zero
        for x in (-2, -1, rows_x, rows_x + 1):
            for t in bands:
                for c in range(6):
                    s[c, pl.ds(shape.row(x, t), 8), :] = zero
        lanes = Lanes(depth)
        done = packed = 0
        for stop, group in zip(marks[1:], groups):
            for copy in group:
                copy.wait()
            stop = stop if stop == rows_x else stop - 2
            layers(done, stop, lambda x: own_forces(lanes, s, v, b, x), stop - done)
            done = stop
            ready = range(packed, done - 7, 8)
            if len(ready) > 0:
                send_y(shape, s, v, b, first, second, ready, done == rows_x)
                packed = ready[-1] + 8
        for copy in edges:
            copy.wait()
        send_early(shape, s, v, b, raw, x_first, x_second)

    s, v, b, h, first, second, x_first, x_second = call(
        load,
        [velocity, stress, buoyancy, lame_first, modulus, zone, eligible],
        [in_hbm] * 7,
        [whole_s, whole_v, whole_b, whole_h] + [y_buffers[True]] * 2 + [early_buffer] * 2,
        [in_vmem] * 8,
        10000000,
        scratch=[
            pltpu.VMEM((2, 2, BESIDE, rows_y, depth), jnp.float32),
            pltpu.VMEM((2, 2, BESIDE, rows_y, depth), jnp.int32),
            pltpu.SemaphoreType.DMA((rows_x // 8 + 1, 3)),
            pltpu.SemaphoreType.DMA((4, 2)),
        ],
    )

    def prepare(after, lame_in, shear_in, zone_in, able_in, cohesion, friction, rock):
        def layer(x):
            for t in bands:
                raw = [r[x, pl.ds(t, 8), :] for r in (lame_in, shear_in, zone_in, able_in)]
                fill_rock(shape, rock, x, t, cohesion, friction, *raw)

        layers(0, rows_x, layer, 8)

    early_rims = tuple(range(BESIDE + 1)), tuple(range(rows_x - BESIDE, rows_x + 1))
    early = tuple(range(5)), tuple(range(rows_x - 5, rows_x))

    def push_rim(s, v, b, x):
        for c, value in enumerate(across_y(s, b, aligned(shape, x, -RIM))):
            v[c, pl.ds(aligned(shape, x, -RIM), 8), :] += value

    def push_rows(v, b, h, x, keep=False):
        for t in bands:
            row = aligned(shape, x, t)
            scale = time_step * tile(b, row)
            for c in range(3):
                gain = scale * tile(h.at[c], row)
                v[c, pl.ds(row, 8), :] += gain
                if keep:
                    h[c, pl.ds(row, 8), :] = gain

    def turn(s, v_in, b_in, h_in, got_a, got_b, v, b, h, out_a, out_b):
        receive_y(shape, h, v, b, got_a, got_b)
        for x in early[0] + early[1]:
            push_rows(v, b, h, x, keep=True)
        for x in early_rims[0] + early_rims[1]:
            push_rim(s, v, b, x)
        send_late(shape, h, v, b, got_a, got_b, out_a, out_b)

    def interior(
        s_in, v_in, b_in, h, rock_in, early_a, early_b, cell, moment, cohesion, friction, s, v, b, rock
    ):
        lanes = Lanes(depth)
        layers(early[0][-1] + 1, early[1][0], lambda x: push_rows(v, b, h, x), 4)
        layers(early_rims[0][-1] + 1, early_rims[1][0], lambda x: push_rim(s, v, b, x), 4)
        receive_early(shape, s, v, b, rock, cohesion, friction, early_a, early_b)
        inject(shape, s, cell, moment, lambda x: (x >= -BESIDE) & (x < rows_x + BESIDE))
        layers(*inner, lambda x: push_stress(shape, lanes, s, v, rock, x), 4)
        layers(*next_inner, lambda x: own_forces(lanes, s, v, b, x), 4)

    def border(s_in, v_in, b, rock, got_a, got_b, sent_a, sent_b, s, v, out_a, out_b):
        receive_late(shape, v, b, (got_a, got_b), (sent_a, sent_b))
        lanes = Lanes(depth)
        for first, stop in ((-BESIDE, inner[0]), (inner[1], rows_x + BESIDE)):
            for x in range(first, stop):
                push_stress(shape, lanes, s, v, rock, x)
        for first, stop in ((-2, next_inner[0]), (next_inner[1], rows_x + 2)):
            for x in range(first, stop):
                own_forces(lanes, s, v, b, x)
        send_y(shape, s, v, None, out_a, out_b, range(0, rows_x, 8))

    def between(s_in, v_in, b, cell, moment, s, v):
        def rim(x):
            for c, value in enumerate(across_y(s, b, aligned(shape, x, -RIM))):
                v[c, pl.ds(aligned(shape, x, -RIM), 8), :] = value

        layers(0, rows_x + 1, rim, 3)
        inject(shape, s, cell, moment, lambda x: (x >= 0) & (x < rows_x))

    def finish(s_in, v_in, b, h_in, rock, got_a, got_b, s, v, h, v_out, s_out, sems):
        receive_y(shape, h, v, None, got_a, got_b, begun=True)
        lanes = Lanes(depth)
        layers(-2, rows_x + 2, lambda x: push_rows(v, b, h, x), 4)
        copies = [pltpu.make_async_copy(own_cells(shape, v), v_out, sems.at[0])]
        copies[0].start()
        for i, x in enumerate(range(0, rows_x, 8)):
            layers(x, x + 8, lambda x: push_stress(shape, lanes, s, v, rock, x), 8)
            part = s_out.at[:, pl.ds(x, 8)]
            copies.append(pltpu.make_async_copy(own_cells(shape, s, x, 8), part, sems.at[i + 1]))
            copies[-1].start()
        for c in copies:
            c.wait()

    cells = [source_cell, source_moment]
    first, second = swaps("gy", first, second)
    x_first, x_second = swaps("gx", x_first, x_second)
    v, b, h, sent_a, sent_b = call(
        turn,
        [s, v, b, h, first, second],
        [in_vmem] * 6,
        [whole_v, whole_b, whole_h, late_buffer, late_buffer],
        [in_vmem] * 5,
        1000000,
        aliases={1: 0, 2: 1, 3: 2},
    )
    got_a, got_b = swaps("gx", sent_a, sent_b)
    rock = call(
        prepare,
        [v, lame_first, modulus, zone, eligible, cohesion, friction],
        [in_vmem] * 5 + [in_smem] * 2,
        whole_r,
        in_vmem,
        10000000,
    )
    s, v, b, rock = call(
        interior,
        [s, v, b, h, rock, x_first, x_second] + cells + [cohesion, friction],
        [in_vmem] * 7 + [in_smem] * 4,
        [whole_s, whole_v, whole_b, whole_r],
        [in_vmem] * 4,
        10000000,
        aliases={0: 0, 1: 1, 2: 2, 4: 3},
    )
    s, v, first, second = call(
        border,
        [s, v, b, rock, got_a, got_b, sent_a, sent_b],
        [in_vmem] * 8,
        [whole_s, whole_v, y_buffers[False], y_buffers[False]],
        [in_vmem] * 4,
        10000000,
        aliases={0: 0, 1: 1},
    )
    first, second = swaps("gy", first, second)
    s, v = call(
        between,
        [s, v, b] + cells,
        [in_vmem] * 3 + [in_smem] * 2,
        [whole_s, whole_v],
        [in_vmem] * 2,
        10000000,
        aliases={0: 0, 1: 1},
    )
    outs = call(
        finish,
        [s, v, b, h, rock, first, second],
        [in_vmem] * 7,
        [
            whole_s,
            whole_v,
            whole_h,
            pltpu.HBM(velocity.shape, jnp.float32),
            pltpu.HBM(stress.shape, jnp.float32),
        ],
        [in_vmem] * 3 + [in_hbm] * 2,
        10000000,
        aliases={0: 0, 1: 1, 3: 2},
        scratch=[pltpu.SemaphoreType.DMA((rows_x // 8 + 1,))],
    )
    return (outs[3], outs[4])


def solution(mesh):
    placed = (
        P(None, "gx", "gy", None),
        P(None, "gx", "gy", None),
        P("gx", "gy", None),
        P("gx", "gy", None),
        P("gx", "gy", None),
        P("gx", "gy", None),
        P("gx", "gy", None),
        P(),
        P(),
        P(),
        P(),
    )
    return jax.shard_map(
        steps,
        mesh=mesh,
        in_specs=placed,
        out_specs=(P(None, "gx", "gy", None), P(None, "gx", "gy", None)),
        check_vma=False,
    )
```

```python
import jax
import jax.numpy as jnp
from jax import lax
from jax.experimental import pallas as pl
from jax.experimental.pallas import tpu as pltpu
from jax.sharding import PartitionSpec as P


time_step = 0.1
near_weight = 9.0 / 8.0
far_weight = 1.0 / 24.0
shear_floor = 0.25

XX, YY, ZZ, XY, XZ, YZ = range(6)

LOW_X = ((XX, 1), (XY, 2), (XZ, 2))
HIGH_X = ((XX, 2), (XY, 1), (XZ, 1))
LOW_FLOW_Y = ((0, 1), (1, 2), (2, 1))
HIGH_FLOW_Y = ((0, 2), (1, 1), (2, 2))
BESIDE = 3
LOW_DEEP_X = ((0, 5), (1, 4), (2, 4))
HIGH_DEEP_X = ((0, 4), (1, 5), (2, 5))
DRIVES_X = (XX, XY, XZ)
DRIVES_Y = (XY, YY, YZ)
LOW_PUSH = ((0, 2), (1, 1), (2, 2))
HIGH_PUSH = ((0, 1), (1, 2), (2, 1))

NEAR, FAR = near_weight, far_weight
UP = {1: NEAR, 0: -NEAR, 2: -FAR, -1: FAR}
DOWN = {0: NEAR, -1: -NEAR, 1: -FAR, -2: FAR}


def crossing(table, at, sources):
    total = None
    for step, weight in table.items():
        if at + step in sources:
            term = weight * sources[at + step]()
            total = term if total is None else total + term
    return total


def crossing_x(c, x, sources):
    return crossing(UP if c == 0 else DOWN, x, sources)


def crossing_y(c, y, sources):
    return crossing(UP if c == 1 else DOWN, y, sources)


PAD_X = 8
RIM = 8


class Shape:
    def __init__(self, rows_x, rows_y, depth):
        self.rows_x, self.rows_y, self.depth = rows_x, rows_y, depth
        self.pitch = rows_y + RIM
        self.rows = (rows_x + 2 * PAD_X + 1) * self.pitch

    def row(self, x, y):
        return (x + PAD_X) * self.pitch + RIM + y


def entries(spec):
    return [(c, k) for c, depth in spec for k in range(depth)]


def edge_layers(shape):
    return (0, 1, shape.rows_x - 2, shape.rows_x - 1)


def beside_layers(shape):
    return (-2, -1, shape.rows_x, shape.rows_x + 1)


def by_parity(axis, body, *swapped):
    odd = lax.axis_index(axis) % 2

    @pl.when(odd == 0)
    def _():
        body(*[r for first, second in swapped for r in (second, first)])

    @pl.when(odd == 1)
    def _():
        body(*[r for first, second in swapped for r in (first, second)])


def y_faces(shape):
    rows = shape.rows_y
    above = (LOW_PUSH, LOW_FLOW_Y, lambda y: y - rows, lambda y: y + rows)
    below = (HIGH_PUSH, HIGH_FLOW_Y, lambda y: y + rows, lambda y: y - rows)
    return above, below


def pushed(spec, shape):
    low = spec is LOW_PUSH
    return [(c, k if low else shape.rows_y - 1 - k) for c, k in entries(spec)]


def rim_rows(spec, shape):
    low = spec is LOW_FLOW_Y
    return [(c, -1 - k if low else shape.rows_y + k) for c, k in entries(spec)]


def side_rows(spec, shape):
    return [-1, -2] if spec is LOW_FLOW_Y else [shape.rows_y, shape.rows_y + 1]


def send_y(shape, stress, flow, buoyancy, first, second, groups, singles=True):
    rows_y = shape.rows_y

    def fill(out, push, flow_spec, to_other, to_own):
        face = [y for y in (0, 1, rows_y - 2, rows_y - 1) if to_other(y) in (-2, -1, rows_y, rows_y + 1)]

        def force(c, y, read):
            sources = {to_other(o): (lambda o=o: read(DRIVES_Y[c], o)) for o in face}
            return crossing_y(c, y, sources)

        for x in groups:

            def read(c, y):
                return stress[c, pl.ds(shape.row(x, y), 8, stride=shape.pitch), :]

            slot = 0
            for c, y in pushed(push, shape):
                out[slot, pl.ds(x, 8), :] = force(c, y, read)
                slot += 1
            whole = [(flow.at[c], to_own(y)) for c, y in rim_rows(flow_spec, shape)]
            if buoyancy is not None:
                whole += [(buoyancy, to_own(y)) for y in side_rows(flow_spec, shape)]
            for ref, y in whole:
                out[slot, pl.ds(x, 8), :] = ref[pl.ds(shape.row(x, y), 8, stride=shape.pitch), :]
                slot += 1
        if not singles:
            return
        last = out.at[out.shape[0] - 1]
        for i, x in enumerate(edge_layers(shape) if buoyancy is not None else beside_layers(shape)):

            def single(c, y):
                return stress[c, pl.ds(shape.row(x, y), 1), :]

            if buoyancy is not None:
                rows = [single(DRIVES_X[c], to_own(y)) for c, y in rim_rows(flow_spec, shape)]
            else:
                rows = [force(c, y, single) for c, y in pushed(push, shape)]
            for j, row in enumerate(rows):
                last[pl.ds(8 * i + j, 1), :] = row

    def body(below, above):
        for out, face in zip((above, below), y_faces(shape)):
            fill(out, *face)

    by_parity("gy", body, (first, second))


def receive_y(shape, force, flow, buoyancy, first, second, begun=False):
    def take(got, push, flow_spec):
        slot = 0
        whole = [(force.at[c], y, False) for c, y in pushed(push, shape)]
        whole += [(flow.at[c], y, begun) for c, y in rim_rows(flow_spec, shape)]
        if buoyancy is not None:
            whole += [(buoyancy, y, False) for y in side_rows(flow_spec, shape)]
        for slot, (ref, y, add) in enumerate(whole):
            for x in range(0, shape.rows_x, 8):
                place = pl.ds(shape.row(x, y), 8, stride=shape.pitch)
                value = got[slot, pl.ds(x, 8), :]
                ref[place, :] = ref[place, :] + value if add else value
        if buoyancy is None:
            for i, x in enumerate(beside_layers(shape)):
                for j, (c, y) in enumerate(pushed(push, shape)):
                    single = got[got.shape[0] - 1, pl.ds(8 * i + j, 1), :]
                    force[c, pl.ds(shape.row(x, y), 1), :] = single

    def body(below, above):
        take(below, LOW_PUSH, LOW_FLOW_Y)
        take(above, HIGH_PUSH, HIGH_FLOW_Y)

    by_parity("gy", body, (first, second))


def y_count(first_round):
    most = max(
        len(entries(push)) + len(entries(flow_spec))
        for push, flow_spec in ((LOW_PUSH, LOW_FLOW_Y), (HIGH_PUSH, HIGH_FLOW_Y))
    )
    return most + 1 + (2 if first_round else 0)


def early_slots(shape):
    bands = range(0, shape.rows_y, 8)
    keys = [("s", c, k, t) for c in range(6) for k in range(BESIDE) for t in bands]
    keys += [("r", c, k, t) for c in range(4) for k in range(BESIDE) for t in bands]
    keys += [("b", 0, k, t) for k in range(2) for t in bands]
    return {key: i for i, key in enumerate(keys)}


def send_early(shape, stress, buoyancy, raw, first, second):
    def fill(out, side, place):
        for (kind, c, k, t), slot in early_slots(shape).items():
            x = place(k)
            if kind == "r":
                at = x - (shape.rows_x - BESIDE if side == 0 else 0)
                out[slot] = raw(c, side, at, t)
            else:
                ref = buoyancy if kind == "b" else stress.at[c]
                out[slot] = tile(ref, shape.row(x, t))

    def body(below, above):
        fill(above, 0, lambda k: shape.rows_x - 1 - k)
        fill(below, 1, lambda k: k)

    by_parity("gx", body, (first, second))


def receive_early(shape, stress, flow, buoyancy, rock, table, first, second):
    zones = [(table[0, k], table[1, k]) for k in range(table.shape[1])]

    def take(got, place):
        slots = early_slots(shape)
        for (kind, c, k, t), slot in slots.items():
            x = place(k)
            if kind == "s":
                stress[c, pl.ds(shape.row(x, t), 8), :] = got[slot]
            elif kind == "b":
                buoyancy[pl.ds(shape.row(x, t), 8), :] = got[slot]
            elif c == 0:
                raw = [got[slots["r", i, k, t]] for i in range(4)]
                fill_rock(shape, rock, x, t, zones, *raw)

    def body(below, above):
        take(below, lambda k: -1 - k)
        take(above, lambda k: shape.rows_x + k)

    by_parity("gx", body, (first, second))
    for t in range(0, shape.rows_y, 8):
        for c in range(3):
            there = {
                x: (lambda x=x: tile(stress.at[DRIVES_X[c]], shape.row(x, t)))
                for x in edge_layers(shape) + beside_layers(shape)
            }
            inside = {x: there[x] for x in edge_layers(shape)}
            outside = {x: there[x] for x in beside_layers(shape)}
            for targets, sources in ((inside, outside), (outside, inside)):
                for x in targets:
                    force = crossing_x(c, x, sources)
                    row = shape.row(x, t)
                    if force is not None:
                        force = time_step * tile(buoyancy, row) * force
                        if x in inside:
                            force = flow[c, pl.ds(row, 8), :] + force
                        flow[c, pl.ds(row, 8), :] = force


def fill_rock(shape, rock, x, t, zones, first, shear, which, able):
    hold, rub = zones[0]
    for k, (cohesion, friction) in enumerate(zones):
        hit = which == k
        hold = jnp.where(hit, cohesion, hold)
        rub = jnp.where(hit, friction, rub)
    own = pl.multiple_of((x + BESIDE) * shape.rows_y + t, 8)
    rock[0, pl.ds(own, 8), :] = time_step * first
    rock[1, pl.ds(own, 8), :] = time_step * shear
    rock[2, pl.ds(own, 8), :] = hold * jnp.sqrt(1.0 - rub * rub)
    rock[3, pl.ds(own, 8), :] = rub
    rock[4, pl.ds(own, 8), :] = jnp.where(able == 1, 1.0, 0.0)


def late_rows(shape, side):
    spec, deep = ((LOW_X, LOW_DEEP_X), (HIGH_X, HIGH_DEEP_X))[side]
    rims = rim_rows(LOW_FLOW_Y, shape) + rim_rows(HIGH_FLOW_Y, shape)
    keys = [("d", c, k, y) for c, k in entries(deep) for y in range(shape.rows_y)]
    keys += [("v", c, k, y) for k in range(BESIDE) for c, y in rims]
    sides = side_rows(LOW_FLOW_Y, shape) + side_rows(HIGH_FLOW_Y, shape)
    keys += [("b", 0, k, y) for k in range(2) for y in sides]
    depths = dict(spec)
    keys += [("s", c, k, y) for c, y in rims for k in range(depths[DRIVES_X[c]])]
    return {key: i for i, key in enumerate(keys)}


def late_count(shape):
    return -(-max(len(late_rows(shape, side)) for side in (0, 1)) // 8) * 8


def send_late(shape, flow, buoyancy, got_first, got_second, first, second):
    layer_at = {x: i for i, x in enumerate(edge_layers(shape))}

    def fill(out, side, place, got_below, got_above):
        singles = {}
        for got, spec in ((got_below, LOW_FLOW_Y), (got_above, HIGH_FLOW_Y)):
            for j, key in enumerate(rim_rows(spec, shape)):
                singles[key] = (got, j)
        for (kind, c, k, y), at in late_rows(shape, side).items():
            x = place(k)
            if kind == "d":
                if y % 8 == 0:
                    out[pl.ds(at, 8), :] = tile(flow.at[c], shape.row(x, y))
                continue
            if kind == "s":
                got, j = singles[c, y]
                row = got[got.shape[0] - 1, pl.ds(8 * layer_at[x] + j, 1), :]
            else:
                ref = flow.at[c] if kind == "v" else buoyancy
                row = ref[pl.ds(shape.row(x, y), 1), :]
            out[pl.ds(at, 1), :] = row

    def with_singles(got_below, got_above):
        def body(below, above):
            fill(above, 0, lambda k: shape.rows_x - 1 - k, got_below, got_above)
            fill(below, 1, lambda k: k, got_below, got_above)

        by_parity("gx", body, (first, second))

    by_parity("gy", with_singles, (got_first, got_second))


def receive_late(shape, flow, buoyancy, got, sent):
    rows_x = shape.rows_x

    def add(c, x, y, value):
        flow[c, pl.ds(shape.row(x, y), 1), :] += value

    def body(below, above, sent_below, sent_above):
        def read(sides):
            return {
                (kind, c, place(k), y): (
                    lambda ref=ref, at=at, n=8 if kind == "d" else 1: ref[pl.ds(at, n), :]
                )
                for ref, side, place in sides
                for (kind, c, k, y), at in late_rows(shape, side).items()
            }

        came = read(((below, 0, lambda k: -1 - k), (above, 1, lambda k: rows_x + k)))
        went = read(((sent_above, 0, lambda k: rows_x - 1 - k), (sent_below, 1, lambda k: k)))

        def rims(of, c, y):
            return {x: f for (kind, which, x, at), f in of.items() if (kind, which, at) == ("s", c, y)}

        met = {
            (c, x)
            for c in range(3)
            for x in beside_layers(shape)
            if crossing_x(c, x, {e: lambda: 0.0 for e in edge_layers(shape)}) is not None
        }
        for (kind, c, x, y), value in came.items():
            if kind == "d" and y % 8 == 0:
                place = pl.ds(shape.row(x, y), 8)
                flow[c, place, :] = flow[c, place, :] + value() if (c, x) in met else value()
        for c, y in rim_rows(LOW_FLOW_Y, shape) + rim_rows(HIGH_FLOW_Y, shape):
            halo, own = rims(came, c, y), rims(went, c, y)
            for x in edge_layers(shape):
                force = crossing_x(c, x, halo)
                if force is not None:
                    scale = time_step * buoyancy[pl.ds(shape.row(x, y), 1), :]
                    add(c, x, y, scale * force)
            for x in [d for k in range(BESIDE) for d in (-1 - k, rows_x + k)]:
                value = came["v", c, x, y]()
                force = crossing_x(c, x, own)
                if force is not None:
                    value = value + time_step * came["b", 0, x, y]() * force
                flow[c, pl.ds(shape.row(x, y), 1), :] = value

    by_parity("gx", body, got, sent)


class Lanes:
    def __init__(self, depth):
        self.depth = depth
        lane = lax.broadcasted_iota(jnp.int32, (8, depth), 1)
        zero = jnp.zeros((8, depth), jnp.float32)
        near = jnp.full((8, depth), near_weight, jnp.float32)
        far = jnp.full((8, depth), far_weight, jnp.float32)
        self.f_up = jnp.where(lane < depth - 1, near, zero)
        self.f_up2 = jnp.where(lane < depth - 2, far, zero)
        self.f_down = jnp.where(lane > 0, far, zero)
        self.b_down = jnp.where(lane > 0, near, zero)
        self.b_down2 = jnp.where(lane > 1, far, zero)
        self.b_up = jnp.where(lane < depth - 1, far, zero)

    def forward(self, f):
        up, up2, down = (pltpu.roll(f, s % self.depth, 1) for s in (-1, -2, 1))
        return (self.f_up * up - near_weight * f) - (self.f_up2 * up2 - self.f_down * down)

    def backward(self, f):
        up, down, down2 = (pltpu.roll(f, s % self.depth, 1) for s in (-1, 1, 2))
        return (near_weight * f - self.b_down * down) - (self.b_up * up - self.b_down2 * down2)


def forward(ref, row, step):
    a, b, c, d = (ref[pl.ds(row + k * step, 8), :] for k in (-1, 0, 1, 2))
    return near_weight * (c - b) - far_weight * (d - a)


def backward(ref, row, step):
    a, b, c, d = (ref[pl.ds(row + k * step, 8), :] for k in (-2, -1, 0, 1))
    return near_weight * (c - b) - far_weight * (d - a)


def tile(ref, row):
    return ref[pl.ds(row, 8), :]


def push_velocity(shape, lanes, stress, flow, buoyancy, row, along="xyz"):
    sx, sy = shape.pitch, 1
    xx, yy, zz, xy, xz, yz = (stress.at[c] for c in range(6))
    parts = {
        "x": lambda: (forward(xx, row, sx), backward(xy, row, sx), backward(xz, row, sx)),
        "y": lambda: (backward(xy, row, sy), forward(yy, row, sy), backward(yz, row, sy)),
        "z": lambda: (
            lanes.backward(tile(xz, row)),
            lanes.backward(tile(yz, row)),
            lanes.forward(tile(zz, row)),
        ),
    }
    force = parts[along[0]]()
    for axis in along[1:]:
        force = [f + g for f, g in zip(force, parts[axis]())]
    scale = time_step * tile(buoyancy, row)
    for c in range(3):
        flow[c, pl.ds(row, 8), :] += scale * force[c]


def across_y(stress, buoyancy, row):
    xy, yy, yz = (stress.at[c] for c in DRIVES_Y)
    scale = time_step * tile(buoyancy, row)
    forces = (backward(xy, row, 1), forward(yy, row, 1), backward(yz, row, 1))
    return [scale * f for f in forces]


def layers(first, stop, body, unroll):
    def run(x, carry):
        body(x)
        return carry

    lax.fori_loop(first, stop, run, 0, unroll=unroll)


def aligned(shape, x, y):
    return pl.multiple_of((x + PAD_X) * shape.pitch + RIM + y, 8)


INJECTION = 5


def inject(shape, rock, source_cell, source_moment):
    rows_x, rows_y, depth = shape.rows_x, shape.rows_y, shape.depth
    total_y = rows_y * lax.axis_size("gy")
    start_x = lax.axis_index("gx") * rows_x - BESIDE
    start_y = lax.axis_index("gy") * rows_y
    sub = lax.broadcasted_iota(jnp.int32, (8, depth), 0)
    lane = lax.broadcasted_iota(jnp.int32, (8, depth), 1)
    unread = (rows_x + 2 * BESIDE) * rows_y
    for s in range(source_cell.shape[0]):
        cell = source_cell[s]
        line = lax.div(cell, depth)
        x = lax.div(line, total_y) - start_x
        y = lax.rem(line, total_y) - start_y
        z = lax.rem(cell, depth)
        here = (x >= 0) & (x < rows_x + 2 * BESIDE) & (y >= 0) & (y < rows_y)
        band = lax.div(jnp.where(here, y, 0), 8) * 8
        row = pl.multiple_of(jnp.where(here, x * rows_y + band, unread), 8)
        spot = (sub == y - band) & (lane == z)
        for c in range(6):
            amount = time_step * source_moment[c, s]
            rock[INJECTION + c, pl.ds(row, 8), :] += jnp.where(spot, amount, 0.0)


def push_stress(shape, lanes, stress, flow, rock, x):
    sx, sy = shape.pitch, 1
    vx, vy, vz = (flow.at[c] for c in range(3))

    for t in range(0, shape.rows_y, 8):
        row = aligned(shape, x, t)
        own = pl.multiple_of((x + BESIDE) * shape.rows_y + t, 8)
        first = rock[0, pl.ds(own, 8), :]
        shear = rock[1, pl.ds(own, 8), :]
        base = [
            tile(stress.at[c], row) + rock[INJECTION + c, pl.ds(own, 8), :] for c in range(6)
        ]
        strain_x = backward(vx, row, sx)
        strain_y = backward(vy, row, sy)
        here_z = tile(vz, row)
        strain_z = lanes.backward(here_z)
        volume = first * (strain_x + strain_y + strain_z)
        twice = 2.0 * shear
        xx = base[XX] + (volume + twice * strain_x)
        yy = base[YY] + (volume + twice * strain_y)
        zz = base[ZZ] + (volume + twice * strain_z)
        xy = base[XY] + shear * (forward(vx, row, sy) + forward(vy, row, sx))
        xz = base[XZ] + shear * (
            lanes.forward(tile(vx, row)) + forward(vz, row, sx)
        )
        yz = base[YZ] + shear * (
            lanes.forward(tile(vy, row)) + forward(vz, row, sy)
        )
        pressure = (xx + yy + zz) * (1.0 / 3.0)
        dx, dy, dz = xx - pressure, yy - pressure, zz - pressure
        second = 0.5 * (dx * dx + dy * dy + dz * dz) + xy * xy + xz * xz + yz * yz
        strength = jnp.maximum(
            rock[2, pl.ds(own, 8), :] - pressure * rock[3, pl.ds(own, 8), :], 0.0
        )
        ratio = strength * lax.rsqrt(jnp.maximum(second, shear_floor * shear_floor))
        factor = jnp.where(rock[4, pl.ds(own, 8), :] > 0.5, jnp.minimum(ratio, 1.0), 1.0)
        stress[XX, pl.ds(row, 8), :] = pressure + factor * dx
        stress[YY, pl.ds(row, 8), :] = pressure + factor * dy
        stress[ZZ, pl.ds(row, 8), :] = pressure + factor * dz
        stress[XY, pl.ds(row, 8), :] = factor * xy
        stress[XZ, pl.ds(row, 8), :] = factor * xz
        stress[YZ, pl.ds(row, 8), :] = factor * yz


def own_cells(shape, ref, first=0, count=None):
    lead = ref.shape[:-2]
    view = ref.reshape(*lead, shape.rows_x + 2 * PAD_X + 1, shape.pitch, shape.depth)
    count = shape.rows_x - first if count is None else count
    return view.at[
        (slice(None),) * len(lead) + (pl.ds(PAD_X + first, count), pl.ds(RIM, shape.rows_y))
    ]


def vmem(shape):
    return pltpu.VMEM(shape, jnp.float32)


in_vmem = pl.BlockSpec(memory_space=pltpu.VMEM)
in_smem = pl.BlockSpec(memory_space=pltpu.SMEM)
in_hbm = pl.BlockSpec(memory_space=pltpu.HBM)


def call(body, ins, in_specs, out_shape, out_specs, flops, aliases=None, scratch=()):
    space = {id(in_vmem): pltpu.VMEM, id(in_hbm): pltpu.HBM}
    ins = [
        pltpu.with_memory_space_constraint(x, space[id(s)]) if id(s) in space else x
        for x, s in zip(ins, in_specs)
    ]
    return pl.pallas_call(
        body,
        in_specs=in_specs,
        out_shape=out_shape,
        out_specs=out_specs,
        input_output_aliases=aliases or {},
        scratch_shapes=scratch,
        cost_estimate=pl.CostEstimate(flops=flops, bytes_accessed=1000000, transcendentals=0),
        compiler_params=pltpu.CompilerParams(vmem_limit_bytes=16 * 1024 * 1024),
    )(*ins)


def swaps(axis, first, second):
    count = lax.axis_size(axis)
    got = []
    for start, block in ((0, first), (1, second)):
        pairs = []
        for low in range(start, count - 1, 2):
            pairs += [(low, low + 1), (low + 1, low)]
        got.append(lax.ppermute(block, axis, pairs))
    return got


def steps(
    velocity,
    stress,
    lame_first,
    modulus,
    buoyancy,
    zone,
    eligible,
    cohesion,
    friction,
    source_cell,
    source_moment,
):
    shape = Shape(*zone.shape)
    rows_x, rows_y, depth = zone.shape
    whole_s, whole_v = vmem((6, shape.rows, depth)), vmem((3, shape.rows, depth))
    whole_b, whole_h = vmem((shape.rows, depth)), vmem((3, shape.rows, depth))
    y_buffers = {first: vmem((y_count(first), rows_x, depth)) for first in (True, False)}
    late_buffer = vmem((late_count(shape), depth))
    early_buffer = vmem((len(early_slots(shape)), 8, depth))
    whole_r = vmem((INJECTION + 6, (rows_x + 2 * BESIDE) * rows_y + 8, depth))

    inner = (4, rows_x - 4)
    next_inner = (6, rows_x - 6)
    bands = range(0, rows_y, 8)

    def own_forces(lanes, s, v, b, x):
        for t in bands:
            push_velocity(shape, lanes, s, v, b, aligned(shape, x, t))

    def load(
        v_in, s_in, b_in, lame_in, shear_in, zone_in, able_in,
        s, v, b, h, first, second, floats, ints, sems, edge_sems,
    ):
        groups, edges = [], []
        marks = list(range(0, rows_x - 8, 8)) + [rows_x - 8, rows_x - 4, rows_x]
        for g, (x, stop) in enumerate(zip(marks, marks[1:])):
            group = []
            for i, (source, ref) in enumerate(((s_in, s), (v_in, v), (b_in, b))):
                span = pl.ds(x, stop - x)
                part = source.at[:, span] if i < 2 else source.at[span]
                place = own_cells(shape, ref, x, stop - x)
                group.append(pltpu.make_async_copy(part, place, sems.at[g, i]))
                group[-1].start()
            groups.append(group)
        for i, source in enumerate((lame_in, shear_in, zone_in, able_in)):
            ref = floats.at[i] if i < 2 else ints.at[i - 2]
            for side, x in enumerate((rows_x - BESIDE, 0)):
                part = source.at[pl.ds(x, BESIDE)]
                edges.append(pltpu.make_async_copy(part, ref.at[side], edge_sems.at[i, side]))
                edges[-1].start()

        zero = jnp.zeros((8, depth), jnp.float32)
        for x in range(-2, rows_x + 3):
            for c in (XY, YY, YZ):
                s[c, pl.ds(shape.row(x, -RIM), 8), :] = zero
        for x in range(-2, rows_x + 2):
            for t in bands:
                for c in range(3):
                    h[c, pl.ds(shape.row(x, t), 8), :] = zero
        for x in (-2, -1, rows_x, rows_x + 1):
            for t in bands:
                for c in range(6):
                    s[c, pl.ds(shape.row(x, t), 8), :] = zero
        lanes = Lanes(depth)
        done = packed = 0
        for stop, group in zip(marks[1:], groups):
            for copy in group:
                copy.wait()
            stop = stop if stop == rows_x else stop - 2
            layers(done, stop, lambda x: own_forces(lanes, s, v, b, x), stop - done)
            done = stop
            ready = range(packed, done - 7, 8)
            if len(ready) > 0:
                send_y(shape, s, v, b, first, second, ready, done == rows_x)
                packed = ready[-1] + 8
        for copy in edges:
            copy.wait()

    edge = (2, 2, BESIDE, rows_y, depth)
    s, v, b, h, first, second, floats, ints = call(
        load,
        [velocity, stress, buoyancy, lame_first, modulus, zone, eligible],
        [in_hbm] * 7,
        [whole_s, whole_v, whole_b, whole_h, y_buffers[True], y_buffers[True], vmem(edge)]
        + [pltpu.VMEM(edge, jnp.int32)],
        [in_vmem] * 8,
        10000000,
        scratch=[
            pltpu.SemaphoreType.DMA((rows_x // 8 + 1, 3)),
            pltpu.SemaphoreType.DMA((4, 2)),
        ],
    )

    def pack(s, b, floats, ints, x_first, x_second):
        def raw(c, side, x, t):
            if c < 2:
                return floats[c, side, x, pl.ds(t, 8), :]
            return ints[c - 2, side, x, pl.ds(t, 8), :].astype(jnp.float32)

        send_early(shape, s, b, raw, x_first, x_second)

    x_first, x_second = call(
        pack, [s, b, floats, ints], [in_vmem] * 4, [early_buffer] * 2, [in_vmem] * 2, 1000000
    )

    def prepare(
        after, lame_in, shear_in, zone_in, able_in, cohesion, friction, cell, moment, rock, table
    ):
        zones = [
            [jnp.full((8, depth), r[k], jnp.float32) for r in (cohesion, friction)]
            for k in range(cohesion.shape[0])
        ]
        for k, both in enumerate(zones):
            for i, value in enumerate(both):
                table[i, k] = value
        zero = jnp.zeros((8, depth), jnp.float32)
        for c in range(INJECTION, INJECTION + 6):
            for row in range(0, rock.shape[1], 8):
                rock[c, pl.ds(row, 8), :] = zero

        def layer(x):
            for t in bands:
                raw = [r[x, pl.ds(t, 8), :] for r in (lame_in, shear_in, zone_in, able_in)]
                fill_rock(shape, rock, x, t, zones, *raw)

        layers(0, rows_x, layer, 8)
        inject(shape, rock, cell, moment)

    early_rims = tuple(range(BESIDE + 1)), tuple(range(rows_x - BESIDE, rows_x + 1))
    early = tuple(range(5)), tuple(range(rows_x - 5, rows_x))

    def push_rim(s, v, b, x):
        for c, value in enumerate(across_y(s, b, aligned(shape, x, -RIM))):
            v[c, pl.ds(aligned(shape, x, -RIM), 8), :] += value

    def push_rows(v, b, h, x):
        for t in bands:
            row = aligned(shape, x, t)
            scale = time_step * tile(b, row)
            for c in range(3):
                v[c, pl.ds(row, 8), :] += scale * tile(h.at[c], row)

    def turn(s, v_in, b_in, h_in, got_a, got_b, v, b, h, out_a, out_b):
        receive_y(shape, h, v, b, got_a, got_b)
        for x in early[0] + early[1]:
            push_rows(v, b, h, x)
        for x in early_rims[0] + early_rims[1]:
            push_rim(s, v, b, x)
        send_late(shape, v, b, got_a, got_b, out_a, out_b)

    def interior(s_in, v_in, b, h, rock, s, v):
        lanes = Lanes(depth)
        layers(early[0][-1] + 1, early[1][0], lambda x: push_rows(v, b, h, x), 4)
        layers(early_rims[0][-1] + 1, early_rims[1][0], lambda x: push_rim(s, v, b, x), 4)
        layers(*inner, lambda x: push_stress(shape, lanes, s, v, rock, x), 4)
        layers(*next_inner, lambda x: own_forces(lanes, s, v, b, x), 4)

    def beside(s_in, v_in, b_in, rock_in, table, early_a, early_b, s, v, b, rock):
        receive_early(shape, s, v, b, rock, table, early_a, early_b)

    def border(s_in, v_in, b, rock, got_a, got_b, sent_a, sent_b, s, v, out_a, out_b):
        receive_late(shape, v, b, (got_a, got_b), (sent_a, sent_b))
        lanes = Lanes(depth)
        for first, stop in ((-BESIDE, inner[0]), (inner[1], rows_x + BESIDE)):
            for x in range(first, stop):
                push_stress(shape, lanes, s, v, rock, x)
        for first, stop in ((-2, next_inner[0]), (next_inner[1], rows_x + 2)):
            for x in range(first, stop):
                own_forces(lanes, s, v, b, x)
        send_y(shape, s, v, None, out_a, out_b, range(0, rows_x, 8))

    def between(s, v_in, b, v):
        def rim(x):
            for c, value in enumerate(across_y(s, b, aligned(shape, x, -RIM))):
                v[c, pl.ds(aligned(shape, x, -RIM), 8), :] = value

        layers(0, rows_x + 1, rim, 3)

    def finish(s_in, v_in, b, h_in, rock, got_a, got_b, s, v, h, v_out, s_out, sems):
        receive_y(shape, h, v, None, got_a, got_b, begun=True)
        lanes = Lanes(depth)
        layers(-2, rows_x + 2, lambda x: push_rows(v, b, h, x), 4)
        copies = [pltpu.make_async_copy(own_cells(shape, v), v_out, sems.at[0])]
        copies[0].start()
        for i, x in enumerate(range(0, rows_x, 8)):
            layers(x, x + 8, lambda x: push_stress(shape, lanes, s, v, rock, x), 8)
            part = s_out.at[:, pl.ds(x, 8)]
            copies.append(pltpu.make_async_copy(own_cells(shape, s, x, 8), part, sems.at[i + 1]))
            copies[-1].start()
        for c in copies:
            c.wait()

    first, second = swaps("gy", first, second)
    x_first, x_second = swaps("gx", x_first, x_second)
    v, b, h, sent_a, sent_b = call(
        turn,
        [s, v, b, h, first, second],
        [in_vmem] * 6,
        [whole_v, whole_b, whole_h, late_buffer, late_buffer],
        [in_vmem] * 5,
        1000000,
        aliases={1: 0, 2: 1, 3: 2},
    )
    got_a, got_b = swaps("gx", sent_a, sent_b)
    rock, table = call(
        prepare,
        [b, lame_first, modulus, zone, eligible]
        + [cohesion, friction, source_cell, source_moment],
        [in_vmem] * 5 + [in_smem] * 4,
        [whole_r, vmem((2, cohesion.shape[0], 8, depth))],
        [in_vmem] * 2,
        10000000,
    )
    s, v = call(
        interior,
        [s, v, b, h, rock],
        [in_vmem] * 5,
        [whole_s, whole_v],
        [in_vmem] * 2,
        10000000,
        aliases={0: 0, 1: 1},
    )
    s, v, b, rock = call(
        beside,
        [s, v, b, rock, table, x_first, x_second],
        [in_vmem] * 7,
        [whole_s, whole_v, whole_b, whole_r],
        [in_vmem] * 4,
        10000000,
        aliases={0: 0, 1: 1, 2: 2, 3: 3},
    )
    s, v, first, second = call(
        border,
        [s, v, b, rock, got_a, got_b, sent_a, sent_b],
        [in_vmem] * 8,
        [whole_s, whole_v, y_buffers[False], y_buffers[False]],
        [in_vmem] * 4,
        10000000,
        aliases={0: 0, 1: 1},
    )
    first, second = swaps("gy", first, second)
    v = call(between, [s, v, b], [in_vmem] * 3, whole_v, in_vmem, 10000000, aliases={1: 0})
    outs = call(
        finish,
        [s, v, b, h, rock, first, second],
        [in_vmem] * 7,
        [
            whole_s,
            whole_v,
            whole_h,
            pltpu.HBM(velocity.shape, jnp.float32),
            pltpu.HBM(stress.shape, jnp.float32),
        ],
        [in_vmem] * 3 + [in_hbm] * 2,
        10000000,
        aliases={0: 0, 1: 1, 3: 2},
        scratch=[pltpu.SemaphoreType.DMA((rows_x // 8 + 1,))],
    )
    return (outs[3], outs[4])


def solution(mesh):
    placed = (
        P(None, "gx", "gy", None),
        P(None, "gx", "gy", None),
        P("gx", "gy", None),
        P("gx", "gy", None),
        P("gx", "gy", None),
        P("gx", "gy", None),
        P("gx", "gy", None),
        P(),
        P(),
        P(),
        P(),
    )
    return jax.shard_map(
        steps,
        mesh=mesh,
        in_specs=placed,
        out_specs=(P(None, "gx", "gy", None), P(None, "gx", "gy", None)),
        check_vma=False,
    )
```

```python
import jax
import jax.numpy as jnp
from jax import lax
from jax.experimental import pallas as pl
from jax.experimental.pallas import tpu as pltpu
from jax.sharding import PartitionSpec as P


time_step = 0.1
near_weight = 9.0 / 8.0
far_weight = 1.0 / 24.0
shear_floor = 0.25

XX, YY, ZZ, XY, XZ, YZ = range(6)

LOW_X = ((XX, 1), (XY, 2), (XZ, 2))
HIGH_X = ((XX, 2), (XY, 1), (XZ, 1))
LOW_FLOW_Y = ((0, 1), (1, 2), (2, 1))
HIGH_FLOW_Y = ((0, 2), (1, 1), (2, 2))
BESIDE = 3
LOW_DEEP_X = ((0, 5), (1, 4), (2, 4))
HIGH_DEEP_X = ((0, 4), (1, 5), (2, 5))
DRIVES_X = (XX, XY, XZ)
DRIVES_Y = (XY, YY, YZ)
LOW_PUSH = ((0, 2), (1, 1), (2, 2))
HIGH_PUSH = ((0, 1), (1, 2), (2, 1))

NEAR, FAR = near_weight, far_weight
UP = {1: NEAR, 0: -NEAR, 2: -FAR, -1: FAR}
DOWN = {0: NEAR, -1: -NEAR, 1: -FAR, -2: FAR}


def crossing(table, at, sources):
    total = None
    for step, weight in table.items():
        if at + step in sources:
            term = weight * sources[at + step]()
            total = term if total is None else total + term
    return total


def crossing_x(c, x, sources):
    return crossing(UP if c == 0 else DOWN, x, sources)


def crossing_y(c, y, sources):
    return crossing(UP if c == 1 else DOWN, y, sources)


PAD_X = 8
RIM = 8


class Shape:
    def __init__(self, rows_x, rows_y, depth):
        self.rows_x, self.rows_y, self.depth = rows_x, rows_y, depth
        self.pitch = rows_y + RIM
        self.rows = (rows_x + 2 * PAD_X + 1) * self.pitch

    def row(self, x, y):
        return (x + PAD_X) * self.pitch + RIM + y


def entries(spec):
    return [(c, k) for c, depth in spec for k in range(depth)]


def edge_layers(shape):
    return (0, 1, shape.rows_x - 2, shape.rows_x - 1)


def beside_layers(shape):
    return (-2, -1, shape.rows_x, shape.rows_x + 1)


def by_parity(axis, body, *swapped):
    odd = lax.axis_index(axis) % 2

    @pl.when(odd == 0)
    def _():
        body(*[r for first, second in swapped for r in (second, first)])

    @pl.when(odd == 1)
    def _():
        body(*[r for first, second in swapped for r in (first, second)])


def y_faces(shape):
    rows = shape.rows_y
    above = (LOW_PUSH, LOW_FLOW_Y, lambda y: y - rows, lambda y: y + rows)
    below = (HIGH_PUSH, HIGH_FLOW_Y, lambda y: y + rows, lambda y: y - rows)
    return above, below


def pushed(spec, shape):
    low = spec is LOW_PUSH
    return [(c, k if low else shape.rows_y - 1 - k) for c, k in entries(spec)]


def rim_rows(spec, shape):
    low = spec is LOW_FLOW_Y
    return [(c, -1 - k if low else shape.rows_y + k) for c, k in entries(spec)]


def side_rows(spec, shape):
    return [-1, -2] if spec is LOW_FLOW_Y else [shape.rows_y, shape.rows_y + 1]


def send_y(shape, stress, flow, buoyancy, first, second, groups, singles=True):
    rows_y = shape.rows_y

    def fill(out, push, flow_spec, to_other, to_own):
        face = [y for y in (0, 1, rows_y - 2, rows_y - 1) if to_other(y) in (-2, -1, rows_y, rows_y + 1)]

        def force(c, y, read):
            sources = {to_other(o): (lambda o=o: read(DRIVES_Y[c], o)) for o in face}
            return crossing_y(c, y, sources)

        for x in groups:

            def read(c, y):
                return stress[c, pl.ds(shape.row(x, y), 8, stride=shape.pitch), :]

            slot = 0
            for c, y in pushed(push, shape):
                out[slot, pl.ds(x, 8), :] = force(c, y, read)
                slot += 1
            whole = [(flow.at[c], to_own(y)) for c, y in rim_rows(flow_spec, shape)]
            if buoyancy is not None:
                whole += [(buoyancy, to_own(y)) for y in side_rows(flow_spec, shape)]
            for ref, y in whole:
                out[slot, pl.ds(x, 8), :] = ref[pl.ds(shape.row(x, y), 8, stride=shape.pitch), :]
                slot += 1
        if not singles:
            return
        last = out.at[out.shape[0] - 1]
        for i, x in enumerate(edge_layers(shape) if buoyancy is not None else beside_layers(shape)):

            def single(c, y):
                return stress[c, pl.ds(shape.row(x, y), 1), :]

            if buoyancy is not None:
                rows = [single(DRIVES_X[c], to_own(y)) for c, y in rim_rows(flow_spec, shape)]
            else:
                rows = [force(c, y, single) for c, y in pushed(push, shape)]
            for j, row in enumerate(rows):
                last[pl.ds(8 * i + j, 1), :] = row

    def body(below, above):
        for out, face in zip((above, below), y_faces(shape)):
            fill(out, *face)

    by_parity("gy", body, (first, second))


def receive_y(shape, force, flow, buoyancy, first, second, begun=False):
    def take(got, push, flow_spec):
        slot = 0
        whole = [(force.at[c], y, False) for c, y in pushed(push, shape)]
        whole += [(flow.at[c], y, begun) for c, y in rim_rows(flow_spec, shape)]
        if buoyancy is not None:
            whole += [(buoyancy, y, False) for y in side_rows(flow_spec, shape)]
        for slot, (ref, y, add) in enumerate(whole):
            for x in range(0, shape.rows_x, 8):
                place = pl.ds(shape.row(x, y), 8, stride=shape.pitch)
                value = got[slot, pl.ds(x, 8), :]
                ref[place, :] = ref[place, :] + value if add else value
        if buoyancy is None:
            for i, x in enumerate(beside_layers(shape)):
                for j, (c, y) in enumerate(pushed(push, shape)):
                    single = got[got.shape[0] - 1, pl.ds(8 * i + j, 1), :]
                    force[c, pl.ds(shape.row(x, y), 1), :] = single

    def body(below, above):
        take(below, LOW_PUSH, LOW_FLOW_Y)
        take(above, HIGH_PUSH, HIGH_FLOW_Y)

    by_parity("gy", body, (first, second))


def y_count(first_round):
    most = max(
        len(entries(push)) + len(entries(flow_spec))
        for push, flow_spec in ((LOW_PUSH, LOW_FLOW_Y), (HIGH_PUSH, HIGH_FLOW_Y))
    )
    return most + 1 + (2 if first_round else 0)


def early_slots(shape):
    bands = range(0, shape.rows_y, 8)
    keys = [("s", c, k, t) for c in range(6) for k in range(BESIDE) for t in bands]
    keys += [("r", c, k, t) for c in range(4) for k in range(BESIDE) for t in bands]
    keys += [("b", 0, k, t) for k in range(2) for t in bands]
    return {key: i for i, key in enumerate(keys)}


def send_early(shape, stress, buoyancy, raw, first, second):
    def fill(out, side, place):
        for (kind, c, k, t), slot in early_slots(shape).items():
            x = place(k)
            if kind == "r":
                at = x - (shape.rows_x - BESIDE if side == 0 else 0)
                out[slot] = raw(c, side, at, t)
            else:
                ref = buoyancy if kind == "b" else stress.at[c]
                out[slot] = tile(ref, shape.row(x, t))

    def body(below, above):
        fill(above, 0, lambda k: shape.rows_x - 1 - k)
        fill(below, 1, lambda k: k)

    by_parity("gx", body, (first, second))


def receive_early(shape, stress, flow, buoyancy, rock, table, first, second):
    zones = [(table[0, k], table[1, k]) for k in range(table.shape[1])]

    def take(got, place):
        slots = early_slots(shape)
        for (kind, c, k, t), slot in slots.items():
            x = place(k)
            if kind == "s":
                stress[c, pl.ds(shape.row(x, t), 8), :] = got[slot]
            elif kind == "b":
                buoyancy[pl.ds(shape.row(x, t), 8), :] = got[slot]
            elif c == 0:
                raw = [got[slots["r", i, k, t]] for i in range(4)]
                fill_rock(shape, rock, x, t, zones, *raw)

    def body(below, above):
        take(below, lambda k: -1 - k)
        take(above, lambda k: shape.rows_x + k)

    by_parity("gx", body, (first, second))
    for t in range(0, shape.rows_y, 8):
        for c in range(3):
            there = {
                x: (lambda x=x: tile(stress.at[DRIVES_X[c]], shape.row(x, t)))
                for x in edge_layers(shape) + beside_layers(shape)
            }
            inside = {x: there[x] for x in edge_layers(shape)}
            outside = {x: there[x] for x in beside_layers(shape)}
            for targets, sources in ((inside, outside), (outside, inside)):
                for x in targets:
                    force = crossing_x(c, x, sources)
                    row = shape.row(x, t)
                    if force is not None:
                        force = time_step * tile(buoyancy, row) * force
                        if x in inside:
                            force = flow[c, pl.ds(row, 8), :] + force
                        flow[c, pl.ds(row, 8), :] = force


def fill_rock(shape, rock, x, t, zones, first, shear, which, able):
    hold, rub = zones[0]
    for k, (cohesion, friction) in enumerate(zones):
        hit = which == k
        hold = jnp.where(hit, cohesion, hold)
        rub = jnp.where(hit, friction, rub)
    own = pl.multiple_of((x + BESIDE) * shape.rows_y + t, 8)
    rock[0, pl.ds(own, 8), :] = time_step * first
    rock[1, pl.ds(own, 8), :] = time_step * shear
    rock[2, pl.ds(own, 8), :] = hold * jnp.sqrt(1.0 - rub * rub)
    rock[3, pl.ds(own, 8), :] = rub
    rock[4, pl.ds(own, 8), :] = jnp.where(able == 1, 1.0, 0.0)


def late_rows(shape, side):
    spec, deep = ((LOW_X, LOW_DEEP_X), (HIGH_X, HIGH_DEEP_X))[side]
    rims = rim_rows(LOW_FLOW_Y, shape) + rim_rows(HIGH_FLOW_Y, shape)
    keys = [("d", c, k, y) for c, k in entries(deep) for y in range(shape.rows_y)]
    keys += [("v", c, k, y) for k in range(BESIDE) for c, y in rims]
    sides = side_rows(LOW_FLOW_Y, shape) + side_rows(HIGH_FLOW_Y, shape)
    keys += [("b", 0, k, y) for k in range(2) for y in sides]
    depths = dict(spec)
    keys += [("s", c, k, y) for c, y in rims for k in range(depths[DRIVES_X[c]])]
    return {key: i for i, key in enumerate(keys)}


def late_count(shape):
    return -(-max(len(late_rows(shape, side)) for side in (0, 1)) // 8) * 8


def send_late(shape, flow, buoyancy, got_first, got_second, first, second):
    layer_at = {x: i for i, x in enumerate(edge_layers(shape))}

    def fill(out, side, place, got_below, got_above):
        singles = {}
        for got, spec in ((got_below, LOW_FLOW_Y), (got_above, HIGH_FLOW_Y)):
            for j, key in enumerate(rim_rows(spec, shape)):
                singles[key] = (got, j)
        for (kind, c, k, y), at in late_rows(shape, side).items():
            x = place(k)
            if kind == "d":
                if y % 8 == 0:
                    out[pl.ds(at, 8), :] = tile(flow.at[c], shape.row(x, y))
                continue
            if kind == "s":
                got, j = singles[c, y]
                row = got[got.shape[0] - 1, pl.ds(8 * layer_at[x] + j, 1), :]
            else:
                ref = flow.at[c] if kind == "v" else buoyancy
                row = ref[pl.ds(shape.row(x, y), 1), :]
            out[pl.ds(at, 1), :] = row

    def with_singles(got_below, got_above):
        def body(below, above):
            fill(above, 0, lambda k: shape.rows_x - 1 - k, got_below, got_above)
            fill(below, 1, lambda k: k, got_below, got_above)

        by_parity("gx", body, (first, second))

    by_parity("gy", with_singles, (got_first, got_second))


def receive_late(shape, flow, buoyancy, got, sent):
    rows_x = shape.rows_x

    def add(c, x, y, value):
        flow[c, pl.ds(shape.row(x, y), 1), :] += value

    def body(below, above, sent_below, sent_above):
        def read(sides):
            return {
                (kind, c, place(k), y): (
                    lambda ref=ref, at=at, n=8 if kind == "d" else 1: ref[pl.ds(at, n), :]
                )
                for ref, side, place in sides
                for (kind, c, k, y), at in late_rows(shape, side).items()
            }

        came = read(((below, 0, lambda k: -1 - k), (above, 1, lambda k: rows_x + k)))
        went = read(((sent_above, 0, lambda k: rows_x - 1 - k), (sent_below, 1, lambda k: k)))

        def rims(of, c, y):
            return {x: f for (kind, which, x, at), f in of.items() if (kind, which, at) == ("s", c, y)}

        met = {
            (c, x)
            for c in range(3)
            for x in beside_layers(shape)
            if crossing_x(c, x, {e: lambda: 0.0 for e in edge_layers(shape)}) is not None
        }
        for (kind, c, x, y), value in came.items():
            if kind == "d" and y % 8 == 0:
                place = pl.ds(shape.row(x, y), 8)
                flow[c, place, :] = flow[c, place, :] + value() if (c, x) in met else value()
        for c, y in rim_rows(LOW_FLOW_Y, shape) + rim_rows(HIGH_FLOW_Y, shape):
            halo, own = rims(came, c, y), rims(went, c, y)
            for x in edge_layers(shape):
                force = crossing_x(c, x, halo)
                if force is not None:
                    scale = time_step * buoyancy[pl.ds(shape.row(x, y), 1), :]
                    add(c, x, y, scale * force)
            for x in [d for k in range(BESIDE) for d in (-1 - k, rows_x + k)]:
                value = came["v", c, x, y]()
                force = crossing_x(c, x, own)
                if force is not None:
                    value = value + time_step * came["b", 0, x, y]() * force
                flow[c, pl.ds(shape.row(x, y), 1), :] = value

    by_parity("gx", body, got, sent)


class Lanes:
    def __init__(self, depth):
        self.depth = depth
        lane = lax.broadcasted_iota(jnp.int32, (8, depth), 1)
        zero = jnp.zeros((8, depth), jnp.float32)
        near = jnp.full((8, depth), near_weight, jnp.float32)
        far = jnp.full((8, depth), far_weight, jnp.float32)
        self.f_up = jnp.where(lane < depth - 1, near, zero)
        self.f_up2 = jnp.where(lane < depth - 2, far, zero)
        self.f_down = jnp.where(lane > 0, far, zero)
        self.b_down = jnp.where(lane > 0, near, zero)
        self.b_down2 = jnp.where(lane > 1, far, zero)
        self.b_up = jnp.where(lane < depth - 1, far, zero)

    def forward(self, f):
        up, up2, down = (pltpu.roll(f, s % self.depth, 1) for s in (-1, -2, 1))
        return (self.f_up * up - near_weight * f) - (self.f_up2 * up2 - self.f_down * down)

    def backward(self, f):
        up, down, down2 = (pltpu.roll(f, s % self.depth, 1) for s in (-1, 1, 2))
        return (near_weight * f - self.b_down * down) - (self.b_up * up - self.b_down2 * down2)


def forward(ref, row, step):
    a, b, c, d = (ref[pl.ds(row + k * step, 8), :] for k in (-1, 0, 1, 2))
    return near_weight * (c - b) - far_weight * (d - a)


def backward(ref, row, step):
    a, b, c, d = (ref[pl.ds(row + k * step, 8), :] for k in (-2, -1, 0, 1))
    return near_weight * (c - b) - far_weight * (d - a)


def tile(ref, row):
    return ref[pl.ds(row, 8), :]


def push_velocity(shape, lanes, stress, flow, buoyancy, row, along="xyz"):
    sx, sy = shape.pitch, 1
    xx, yy, zz, xy, xz, yz = (stress.at[c] for c in range(6))
    parts = {
        "x": lambda: (forward(xx, row, sx), backward(xy, row, sx), backward(xz, row, sx)),
        "y": lambda: (backward(xy, row, sy), forward(yy, row, sy), backward(yz, row, sy)),
        "z": lambda: (
            lanes.backward(tile(xz, row)),
            lanes.backward(tile(yz, row)),
            lanes.forward(tile(zz, row)),
        ),
    }
    force = parts[along[0]]()
    for axis in along[1:]:
        force = [f + g for f, g in zip(force, parts[axis]())]
    scale = time_step * tile(buoyancy, row)
    for c in range(3):
        flow[c, pl.ds(row, 8), :] += scale * force[c]


def across_y(stress, buoyancy, row):
    xy, yy, yz = (stress.at[c] for c in DRIVES_Y)
    scale = time_step * tile(buoyancy, row)
    forces = (backward(xy, row, 1), forward(yy, row, 1), backward(yz, row, 1))
    return [scale * f for f in forces]


def layers(first, stop, body, unroll):
    def run(x, carry):
        body(x)
        return carry

    lax.fori_loop(first, stop, run, 0, unroll=unroll)


def aligned(shape, x, y):
    return pl.multiple_of((x + PAD_X) * shape.pitch + RIM + y, 8)


INJECTION = 5


def inject(shape, rock, source_cell, source_moment):
    rows_x, rows_y, depth = shape.rows_x, shape.rows_y, shape.depth
    total_y = rows_y * lax.axis_size("gy")
    start_x = lax.axis_index("gx") * rows_x - BESIDE
    start_y = lax.axis_index("gy") * rows_y
    sub = lax.broadcasted_iota(jnp.int32, (8, depth), 0)
    lane = lax.broadcasted_iota(jnp.int32, (8, depth), 1)
    unread = (rows_x + 2 * BESIDE) * rows_y
    for s in range(source_cell.shape[0]):
        cell = source_cell[s]
        line = lax.div(cell, depth)
        x = lax.div(line, total_y) - start_x
        y = lax.rem(line, total_y) - start_y
        z = lax.rem(cell, depth)
        here = (x >= 0) & (x < rows_x + 2 * BESIDE) & (y >= 0) & (y < rows_y)
        band = lax.div(jnp.where(here, y, 0), 8) * 8
        row = pl.multiple_of(jnp.where(here, x * rows_y + band, unread), 8)
        spot = (sub == y - band) & (lane == z)
        for c in range(6):
            amount = time_step * source_moment[c, s]
            rock[INJECTION + c, pl.ds(row, 8), :] += jnp.where(spot, amount, 0.0)


def push_stress(shape, lanes, stress, flow, rock, x):
    sx, sy = shape.pitch, 1
    vx, vy, vz = (flow.at[c] for c in range(3))

    for t in range(0, shape.rows_y, 8):
        row = aligned(shape, x, t)
        own = pl.multiple_of((x + BESIDE) * shape.rows_y + t, 8)
        first = rock[0, pl.ds(own, 8), :]
        shear = rock[1, pl.ds(own, 8), :]
        base = [
            tile(stress.at[c], row) + rock[INJECTION + c, pl.ds(own, 8), :] for c in range(6)
        ]
        strain_x = backward(vx, row, sx)
        strain_y = backward(vy, row, sy)
        here_z = tile(vz, row)
        strain_z = lanes.backward(here_z)
        volume = first * (strain_x + strain_y + strain_z)
        twice = 2.0 * shear
        xx = base[XX] + (volume + twice * strain_x)
        yy = base[YY] + (volume + twice * strain_y)
        zz = base[ZZ] + (volume + twice * strain_z)
        xy = base[XY] + shear * (forward(vx, row, sy) + forward(vy, row, sx))
        xz = base[XZ] + shear * (
            lanes.forward(tile(vx, row)) + forward(vz, row, sx)
        )
        yz = base[YZ] + shear * (
            lanes.forward(tile(vy, row)) + forward(vz, row, sy)
        )
        pressure = (xx + yy + zz) * (1.0 / 3.0)
        dx, dy, dz = xx - pressure, yy - pressure, zz - pressure
        second = 0.5 * (dx * dx + dy * dy + dz * dz) + xy * xy + xz * xz + yz * yz
        strength = jnp.maximum(
            rock[2, pl.ds(own, 8), :] - pressure * rock[3, pl.ds(own, 8), :], 0.0
        )
        ratio = strength * lax.rsqrt(jnp.maximum(second, shear_floor * shear_floor))
        factor = jnp.where(rock[4, pl.ds(own, 8), :] > 0.5, jnp.minimum(ratio, 1.0), 1.0)
        stress[XX, pl.ds(row, 8), :] = pressure + factor * dx
        stress[YY, pl.ds(row, 8), :] = pressure + factor * dy
        stress[ZZ, pl.ds(row, 8), :] = pressure + factor * dz
        stress[XY, pl.ds(row, 8), :] = factor * xy
        stress[XZ, pl.ds(row, 8), :] = factor * xz
        stress[YZ, pl.ds(row, 8), :] = factor * yz


def own_cells(shape, ref, first=0, count=None):
    lead = ref.shape[:-2]
    view = ref.reshape(*lead, shape.rows_x + 2 * PAD_X + 1, shape.pitch, shape.depth)
    count = shape.rows_x - first if count is None else count
    return view.at[
        (slice(None),) * len(lead) + (pl.ds(PAD_X + first, count), pl.ds(RIM, shape.rows_y))
    ]


def vmem(shape):
    return pltpu.VMEM(shape, jnp.float32)


in_vmem = pl.BlockSpec(memory_space=pltpu.VMEM)
in_smem = pl.BlockSpec(memory_space=pltpu.SMEM)
in_hbm = pl.BlockSpec(memory_space=pltpu.HBM)


def call(body, ins, in_specs, out_shape, out_specs, flops, aliases=None, scratch=()):
    space = {id(in_vmem): pltpu.VMEM, id(in_hbm): pltpu.HBM}
    ins = [
        pltpu.with_memory_space_constraint(x, space[id(s)]) if id(s) in space else x
        for x, s in zip(ins, in_specs)
    ]
    return pl.pallas_call(
        body,
        in_specs=in_specs,
        out_shape=out_shape,
        out_specs=out_specs,
        input_output_aliases=aliases or {},
        scratch_shapes=scratch,
        cost_estimate=pl.CostEstimate(flops=flops, bytes_accessed=1000000, transcendentals=0),
        compiler_params=pltpu.CompilerParams(vmem_limit_bytes=16 * 1024 * 1024),
    )(*ins)


def swaps(axis, first, second):
    count = lax.axis_size(axis)
    got = []
    for start, block in ((0, first), (1, second)):
        pairs = []
        for low in range(start, count - 1, 2):
            pairs += [(low, low + 1), (low + 1, low)]
        got.append(lax.ppermute(block, axis, pairs))
    return got


def steps(
    velocity,
    stress,
    lame_first,
    modulus,
    buoyancy,
    zone,
    eligible,
    cohesion,
    friction,
    source_cell,
    source_moment,
):
    shape = Shape(*zone.shape)
    rows_x, rows_y, depth = zone.shape
    whole_s, whole_v = vmem((6, shape.rows, depth)), vmem((3, shape.rows, depth))
    whole_b, whole_h = vmem((shape.rows, depth)), vmem((3, shape.rows, depth))
    y_buffers = {first: vmem((y_count(first), rows_x, depth)) for first in (True, False)}
    late_buffer = vmem((late_count(shape), depth))
    early_buffer = vmem((len(early_slots(shape)), 8, depth))
    whole_r = vmem((INJECTION + 6, (rows_x + 2 * BESIDE) * rows_y + 8, depth))

    inner = (4, rows_x - 4)
    next_inner = (6, rows_x - 6)
    bands = range(0, rows_y, 8)

    def own_forces(lanes, s, v, b, x):
        for t in bands:
            push_velocity(shape, lanes, s, v, b, aligned(shape, x, t))

    def load(
        v_in, s_in, b_in, lame_in, shear_in, zone_in, able_in,
        s, v, b, h, first, second, floats, ints, sems, edge_sems,
    ):
        groups, edges = [], []
        marks = list(range(0, rows_x - 8, 8)) + [rows_x - 8, rows_x - 4, rows_x]
        for g, (x, stop) in enumerate(zip(marks, marks[1:])):
            group = []
            for i, (source, ref) in enumerate(((s_in, s), (v_in, v), (b_in, b))):
                span = pl.ds(x, stop - x)
                part = source.at[:, span] if i < 2 else source.at[span]
                place = own_cells(shape, ref, x, stop - x)
                group.append(pltpu.make_async_copy(part, place, sems.at[g, i]))
                group[-1].start()
            groups.append(group)
        for i, source in enumerate((lame_in, shear_in, zone_in, able_in)):
            ref = floats.at[i] if i < 2 else ints.at[i - 2]
            for side, x in enumerate((rows_x - BESIDE, 0)):
                part = source.at[pl.ds(x, BESIDE)]
                edges.append(pltpu.make_async_copy(part, ref.at[side], edge_sems.at[i, side]))
                edges[-1].start()

        zero = jnp.zeros((8, depth), jnp.float32)
        for x in range(-2, rows_x + 3):
            for c in (XY, YY, YZ):
                s[c, pl.ds(shape.row(x, -RIM), 8), :] = zero
        for x in range(-2, rows_x + 2):
            for t in bands:
                for c in range(3):
                    h[c, pl.ds(shape.row(x, t), 8), :] = zero
        for x in (-2, -1, rows_x, rows_x + 1):
            for t in bands:
                for c in range(6):
                    s[c, pl.ds(shape.row(x, t), 8), :] = zero
        lanes = Lanes(depth)
        done = packed = 0
        for stop, group in zip(marks[1:], groups):
            for copy in group:
                copy.wait()
            stop = stop if stop == rows_x else stop - 2
            layers(done, stop, lambda x: own_forces(lanes, s, v, b, x), stop - done)
            done = stop
            ready = range(packed, done - 7, 8)
            if len(ready) > 0:
                send_y(shape, s, v, b, first, second, ready, done == rows_x)
                packed = ready[-1] + 8
        for copy in edges:
            copy.wait()

    edge = (2, 2, BESIDE, rows_y, depth)
    s, v, b, h, first, second, floats, ints = call(
        load,
        [velocity, stress, buoyancy, lame_first, modulus, zone, eligible],
        [in_hbm] * 7,
        [whole_s, whole_v, whole_b, whole_h, y_buffers[True], y_buffers[True], vmem(edge)]
        + [pltpu.VMEM(edge, jnp.int32)],
        [in_vmem] * 8,
        10000000,
        scratch=[
            pltpu.SemaphoreType.DMA((rows_x // 8 + 1, 3)),
            pltpu.SemaphoreType.DMA((4, 2)),
        ],
    )

    def pack(s, b, floats, ints, x_first, x_second):
        def raw(c, side, x, t):
            if c < 2:
                return floats[c, side, x, pl.ds(t, 8), :]
            return ints[c - 2, side, x, pl.ds(t, 8), :].astype(jnp.float32)

        send_early(shape, s, b, raw, x_first, x_second)

    x_first, x_second = call(
        pack, [s, b, floats, ints], [in_vmem] * 4, [early_buffer] * 2, [in_vmem] * 2, 1000000
    )

    def prepare(
        after, lame_in, shear_in, zone_in, able_in, cohesion, friction, cell, moment, rock, table
    ):
        zones = [
            [jnp.full((8, depth), r[k], jnp.float32) for r in (cohesion, friction)]
            for k in range(cohesion.shape[0])
        ]
        for k, both in enumerate(zones):
            for i, value in enumerate(both):
                table[i, k] = value
        zero = jnp.zeros((8, depth), jnp.float32)
        for c in range(INJECTION, INJECTION + 6):
            for row in range(0, rock.shape[1], 8):
                rock[c, pl.ds(row, 8), :] = zero

        def layer(x):
            for t in bands:
                raw = [r[x, pl.ds(t, 8), :] for r in (lame_in, shear_in, zone_in, able_in)]
                fill_rock(shape, rock, x, t, zones, *raw)

        layers(0, rows_x, layer, 8)
        inject(shape, rock, cell, moment)

    early_rims = tuple(range(BESIDE + 1)), tuple(range(rows_x - BESIDE, rows_x + 1))
    early = tuple(range(5)), tuple(range(rows_x - 5, rows_x))

    def push_rim(s, v, b, x):
        for c, value in enumerate(across_y(s, b, aligned(shape, x, -RIM))):
            v[c, pl.ds(aligned(shape, x, -RIM), 8), :] += value

    def push_rows(v, b, h, x):
        for t in bands:
            row = aligned(shape, x, t)
            scale = time_step * tile(b, row)
            for c in range(3):
                v[c, pl.ds(row, 8), :] += scale * tile(h.at[c], row)

    def turn(s, v_in, b_in, h_in, got_a, got_b, v, b, h, out_a, out_b):
        receive_y(shape, h, v, b, got_a, got_b)
        for x in early[0] + early[1]:
            push_rows(v, b, h, x)
        for x in early_rims[0] + early_rims[1]:
            push_rim(s, v, b, x)
        send_late(shape, v, b, got_a, got_b, out_a, out_b)

    def interior(s_in, v_in, b, h, rock, s, v):
        lanes = Lanes(depth)
        layers(early[0][-1] + 1, early[1][0], lambda x: push_rows(v, b, h, x), 4)
        layers(early_rims[0][-1] + 1, early_rims[1][0], lambda x: push_rim(s, v, b, x), 4)
        layers(*inner, lambda x: push_stress(shape, lanes, s, v, rock, x), 4)
        layers(*next_inner, lambda x: own_forces(lanes, s, v, b, x), 4)

    def beside(s_in, v_in, b_in, rock_in, table, early_a, early_b, s, v, b, rock):
        receive_early(shape, s, v, b, rock, table, early_a, early_b)

    def border(s_in, v_in, b, rock, got_a, got_b, sent_a, sent_b, s, v, out_a, out_b):
        receive_late(shape, v, b, (got_a, got_b), (sent_a, sent_b))
        lanes = Lanes(depth)
        for first, stop in ((-BESIDE, inner[0]), (inner[1], rows_x + BESIDE)):
            for x in range(first, stop):
                push_stress(shape, lanes, s, v, rock, x)
        for first, stop in ((-2, next_inner[0]), (next_inner[1], rows_x + 2)):
            for x in range(first, stop):
                own_forces(lanes, s, v, b, x)
        send_y(shape, s, v, None, out_a, out_b, range(0, rows_x, 8))

    def between(s, v_in, b, v):
        def rim(x):
            for c, value in enumerate(across_y(s, b, aligned(shape, x, -RIM))):
                v[c, pl.ds(aligned(shape, x, -RIM), 8), :] = value

        layers(0, rows_x + 1, rim, 3)

    def finish(s_in, v_in, b, h_in, rock, got_a, got_b, s, v, h, v_out, s_out, sems):
        receive_y(shape, h, v, None, got_a, got_b, begun=True)
        lanes = Lanes(depth)
        layers(-2, rows_x + 2, lambda x: push_rows(v, b, h, x), 4)
        copies = [pltpu.make_async_copy(own_cells(shape, v), v_out, sems.at[0])]
        copies[0].start()
        marks = list(range(0, rows_x - 8, 8)) + [rows_x - 8, rows_x - 4, rows_x]
        for i, (x, stop) in enumerate(zip(marks, marks[1:])):
            n = stop - x
            layers(x, stop, lambda x: push_stress(shape, lanes, s, v, rock, x), n)
            part = s_out.at[:, pl.ds(x, n)]
            copies.append(pltpu.make_async_copy(own_cells(shape, s, x, n), part, sems.at[i + 1]))
            copies[-1].start()
        for c in copies:
            c.wait()

    first, second = swaps("gy", first, second)
    x_first, x_second = swaps("gx", x_first, x_second)
    v, b, h, sent_a, sent_b = call(
        turn,
        [s, v, b, h, first, second],
        [in_vmem] * 6,
        [whole_v, whole_b, whole_h, late_buffer, late_buffer],
        [in_vmem] * 5,
        1000000,
        aliases={1: 0, 2: 1, 3: 2},
    )
    got_a, got_b = swaps("gx", sent_a, sent_b)
    rock, table = call(
        prepare,
        [b, lame_first, modulus, zone, eligible]
        + [cohesion, friction, source_cell, source_moment],
        [in_vmem] * 5 + [in_smem] * 4,
        [whole_r, vmem((2, cohesion.shape[0], 8, depth))],
        [in_vmem] * 2,
        10000000,
    )
    s, v = call(
        interior,
        [s, v, b, h, rock],
        [in_vmem] * 5,
        [whole_s, whole_v],
        [in_vmem] * 2,
        10000000,
        aliases={0: 0, 1: 1},
    )
    s, v, b, rock = call(
        beside,
        [s, v, b, rock, table, x_first, x_second],
        [in_vmem] * 7,
        [whole_s, whole_v, whole_b, whole_r],
        [in_vmem] * 4,
        10000000,
        aliases={0: 0, 1: 1, 2: 2, 3: 3},
    )
    s, v, first, second = call(
        border,
        [s, v, b, rock, got_a, got_b, sent_a, sent_b],
        [in_vmem] * 8,
        [whole_s, whole_v, y_buffers[False], y_buffers[False]],
        [in_vmem] * 4,
        10000000,
        aliases={0: 0, 1: 1},
    )
    first, second = swaps("gy", first, second)
    v = call(between, [s, v, b], [in_vmem] * 3, whole_v, in_vmem, 10000000, aliases={1: 0})
    outs = call(
        finish,
        [s, v, b, h, rock, first, second],
        [in_vmem] * 7,
        [
            whole_s,
            whole_v,
            whole_h,
            pltpu.HBM(velocity.shape, jnp.float32),
            pltpu.HBM(stress.shape, jnp.float32),
        ],
        [in_vmem] * 3 + [in_hbm] * 2,
        10000000,
        aliases={0: 0, 1: 1, 3: 2},
        scratch=[pltpu.SemaphoreType.DMA((rows_x // 8 + 2,))],
    )
    return (outs[3], outs[4])


def solution(mesh):
    placed = (
        P(None, "gx", "gy", None),
        P(None, "gx", "gy", None),
        P("gx", "gy", None),
        P("gx", "gy", None),
        P("gx", "gy", None),
        P("gx", "gy", None),
        P("gx", "gy", None),
        P(),
        P(),
        P(),
        P(),
    )
    return jax.shard_map(
        steps,
        mesh=mesh,
        in_specs=placed,
        out_specs=(P(None, "gx", "gy", None), P(None, "gx", "gy", None)),
        check_vma=False,
    )
```
